32 devices in a mesh: grid: 8 (over y, x, core), atom: 4 (over z).
Axes of the slice: x: 2, y: 2, z: 4, core: 2. Of those that a mesh axis runs over, the one named last changes fastest.
Arguments:
- basis_values: bfloat16 [64, 128, 512], P(('grid', 'atom')), may hold values from -8 to 8
- block_lists: int32 [64, 4], P('grid'), may hold values from 0 to 95, as said below
- orbitals: bfloat16 [12288, 4096], P('grid', 'atom'), may hold values from -0.00390625 to 0.00390625
- point_weights: float32 [8192], P(('grid', 'atom')), may hold values from 0.1 to 1
- point_atoms: int32 [8192], P(('grid', 'atom')), may hold values from 0 to 127, as said below
- embed_scale: float32 [256], replicated, may hold values from -4 to 4
- embed_shift: float32 [256], replicated, may hold values from -3 to 3
- message_weight: bfloat16 [2, 256, 256], replicated, may hold values from -0.375 to 0.375
- atom_weight: bfloat16 [2, 256, 256], replicated, may hold values from -0.375 to 0.375
- head_weight: float32 [256], replicated, may hold values from -0.375 to 0.375
Outputs:
- fock_orbitals: float32 [12288, 4096], P('grid', 'atom')
- potential: float32 [8192], P(('grid', 'atom'))
The draws below stay inside these ranges and needn't reach their ends.
Inputs may be any that keep to these rules, and one draw needn't show every extreme that they name: `block_lists`: each row names 4 different blocks; a batch b of group g = b // 8 names only blocks (g - 1) * 12 to (g + 2) * 12 - 1. `point_atoms`: the 256 points of one device name atom centres of one run of max(8, 1) consecutive centres, counted round.
All inputs are finite; a program needn't handle non-finite values.
Results may differ from the reference program's by a relative error of at most 0.04.
Values may be sent and summed in bfloat16 or wider, within the bound.
A program may use at most 128 MiB of HBM per device.

```python
import math
import jax
import jax.numpy as jnp
from jax import lax

BLK = 128
NBLK = 96
NLIST = 4
BPTS = 128
NOCC = 4096
FEAT = 256
LAYERS = 2
PT_DEV = 256
ATOM_DEV = 32
NB = 12288
NATOM = 128
POINTS = 8192
NBATCH = 64
N_GRID = 8


def draw_basis_values(key, part):
    owners = POINTS // PT_DEV
    per_owner = PT_DEV // BPTS
    key_scale = jax.random.fold_in(key, 21)
    key_entry = jax.random.fold_in(key, 22)
    exponent = jax.random.uniform(key_scale, (owners,), jnp.float32, -2.0, 1.5)
    owner_scale = jnp.repeat(jnp.exp(exponent), per_owner, total_repeat_length=NBATCH)
    entries = jax.random.normal(key_entry, (NBATCH, BPTS, NLIST * BLK), jnp.float32)
    batch_scale = jnp.ones((NBATCH,), jnp.float32)
    values = entries * (owner_scale * batch_scale)[:, None, None]
    return jnp.clip(values, -8.0, 8.0).astype(jnp.bfloat16)


def draw_block_lists(key, part):
    per_group = NBATCH // N_GRID
    owned = NBLK // N_GRID
    span = 3 * owned
    group = jnp.arange(NBATCH, dtype=jnp.int32) // per_group
    base = (group - 1) * owned
    offsets = jnp.arange(span, dtype=jnp.int32)
    positions = base[:, None] + offsets[None, :]
    outside = jnp.logical_or(positions < 0, positions >= NBLK).astype(jnp.int32)
    scores = jax.random.randint(key, (NBATCH, span), 0, 1048576, dtype=jnp.int32) * span + offsets[None, :]
    scores = scores + outside * 67108864
    order = jnp.argsort(scores, axis=1, stable=True).astype(jnp.int32)
    return base[:, None] + order[:, :NLIST]


def draw_point_atoms(key, part):
    key_start = jax.random.fold_in(key, 11)
    key_first = jax.random.fold_in(key, 12)
    key_second = jax.random.fold_in(key, 13)
    owners = POINTS // PT_DEV
    window = max(ATOM_DEV // 4, 1)
    starts = jax.random.randint(key_start, (owners,), 0, NATOM, dtype=jnp.int32)
    first = jax.random.randint(key_first, (owners, PT_DEV), 0, window, dtype=jnp.int32)
    second = jax.random.randint(key_second, (owners, PT_DEV), 0, window, dtype=jnp.int32)
    picked = jnp.minimum(first, second)
    return ((starts[:, None] + picked) % NATOM).reshape(-1).astype(jnp.int32)


def steps_of(own_key, shape, split, low, high):
    factor_of, own = 1.0, jax.random.fold_in(own_key, 6)
    for position, shards_of in split:
        heights = jnp.exp(jax.random.uniform(jax.random.fold_in(own, position), (shards_of,), jnp.float32, low / len(split), high / len(split)))
        factor_of = factor_of * jnp.repeat(heights, shape[position] // shards_of).reshape([-1 if axis == position else 1 for axis in range(len(shape))])
    return factor_of


def gaussian(own_key, dims, scale, most, shards=(), kind=jnp.bfloat16):
    result = jax.random.normal(own_key, dims, jnp.float32) * scale
    if len(shards) > 0:
        result = steps_of(own_key, dims, shards, -0.22, 0.18) * result
    return jnp.clip(result, min=-most, max=most).astype(kind)


def setup_inputs(seed: int = 0) -> dict:
    keys = jax.random.split(jax.random.key(seed), 11)
    return {
        "basis_values": draw_basis_values(jax.random.fold_in(keys[10], 71), 0),
        "block_lists": draw_block_lists(jax.random.fold_in(keys[10], 71), 0),
        "orbitals": gaussian(keys[2], (NB, NOCC), (NLIST * BLK * NOCC) ** -0.5, 0.00390625, ((0, 8), (1, 4))),
        "point_weights": jnp.clip(jnp.exp(math.log(1.0) - 2.3025851 * jax.random.uniform(keys[3], (POINTS,), jnp.float32) ** steps_of(keys[3], (POINTS,), ((0, 32),), -0.2, 0.2)), 0.1, 1.0),
        "point_atoms": draw_point_atoms(jax.random.fold_in(keys[10], 71), 0),
        "embed_scale": gaussian(keys[5], (FEAT,), 1.0, 4.0, (), jnp.float32),
        "embed_shift": gaussian(keys[6], (FEAT,), 0.7, 3.0, (), jnp.float32),
        "message_weight": gaussian(keys[7], (LAYERS, FEAT, FEAT), FEAT ** -0.5, 0.375),
        "atom_weight": gaussian(keys[8], (LAYERS, FEAT, FEAT), FEAT ** -0.5, 0.375),
        "head_weight": gaussian(keys[9], (FEAT,), FEAT ** -0.5, 0.375, (), jnp.float32),
    }


def orbital_values(values, lists, orbitals):
    blocks = orbitals.reshape(NBLK, BLK, NOCC)
    chosen = blocks[lists].reshape(lists.shape[0], NLIST * BLK, NOCC)
    psi = jnp.einsum("bpk,bko->bpo", values.astype(jnp.float32), chosen.astype(jnp.float32))
    return psi.astype(jnp.bfloat16)


def reference(basis_values, block_lists, orbitals, point_weights, point_atoms, embed_scale, embed_shift, message_weight, atom_weight, head_weight):
    grouped_values = basis_values.reshape(N_GRID, -1, BPTS, NLIST * BLK)
    grouped_lists = block_lists.reshape(N_GRID, -1, NLIST)

    def group_density(items):
        psi = orbital_values(items[0], items[1], orbitals)
        return 2.0 * jnp.sum(jnp.square(psi.astype(jnp.float32)), axis=2)

    density = lax.map(group_density, (grouped_values, grouped_lists)).reshape(-1)
    radius = jnp.cbrt(density)
    hidden = jax.nn.silu(radius[:, None] * embed_scale[None, :] + embed_shift[None, :])
    mass = jax.ops.segment_sum(point_weights, point_atoms, num_segments=NATOM)
    for layer in range(LAYERS):
        message = jax.nn.silu(jnp.dot(hidden.astype(jnp.bfloat16), message_weight[layer], preferred_element_type=jnp.float32))
        weighted = (point_weights[:, None] * message).astype(jnp.bfloat16)
        rows = jax.ops.segment_sum(weighted.astype(jnp.float32), point_atoms, num_segments=NATOM)
        mean = rows / (1.0 + mass[:, None])
        update = jax.nn.silu(jnp.dot(mean.astype(jnp.bfloat16), atom_weight[layer], preferred_element_type=jnp.float32)).astype(jnp.bfloat16)
        hidden = hidden + message * update[point_atoms].astype(jnp.float32)
    score = jnp.dot(hidden, head_weight, precision=lax.Precision.HIGHEST)
    potential = radius * (1.0 + jnp.tanh(score))
    scaled = (point_weights * potential).reshape(N_GRID, -1, BPTS)

    def group_fock(total, items):
        values, lists, scale = items
        psi = orbital_values(values, lists, orbitals)
        weighted_psi = (scale[:, :, None] * psi.astype(jnp.float32)).astype(jnp.bfloat16)
        terms = jnp.einsum("bpk,bpo->bko", values.astype(jnp.float32), weighted_psi.astype(jnp.float32))
        terms = terms.reshape(-1, BLK, NOCC)
        partial_value = jnp.zeros((NBLK, BLK, NOCC), jnp.float32).at[lists.reshape(-1)].add(terms)
        rounded = lax.optimization_barrier(partial_value.astype(jnp.bfloat16)).astype(jnp.float32)
        return total + rounded, None

    start = jnp.zeros((NBLK, BLK, NOCC), jnp.float32)
    total, unused = lax.scan(group_fock, start, (grouped_values, grouped_lists, scaled))
    return total.reshape(NB, NOCC), potential
```

```python
import functools
import jax
import jax.numpy as jnp
from jax import lax
from jax.experimental import pallas as pl
from jax.experimental.pallas import tpu as pltpu
from jax.sharding import PartitionSpec as P

ATOM_DEV = 32
RUN = max(ATOM_DEV // 4, 1)
LANES = 128
VMEM = pl.BlockSpec(memory_space=pltpu.VMEM)
HBM = pl.BlockSpec(memory_space=pltpu.HBM)
MESH = pl.DeviceIdType.MESH
TILE = 256


def wait_bytes(ref, sem):
    pltpu.make_async_copy(ref, ref, sem).wait()


def meet_all(shape):
    n_grid, n_atom = shape
    n = n_grid * n_atom
    me = lax.axis_index("grid") * n_atom + lax.axis_index("atom")
    barrier = pltpu.get_barrier_semaphore()

    @pl.loop(1, n)
    def _(d):
        t = lax.rem(me + d, n)
        pl.semaphore_signal(
            barrier, inc=1, device_id=(t // n_atom, lax.rem(t, n_atom)), device_id_type=MESH
        )

    pl.semaphore_wait(barrier, n - 1)


def to_columns(rows):
    parts = [
        jnp.transpose(jnp.broadcast_to(rows[i : i + 1, :], (LANES, LANES)))
        for i in range(rows.shape[0])
    ]
    return jnp.concatenate(parts, axis=0)


def to_rows(columns):
    parts = []
    for i in range(columns.shape[0] // LANES):
        piece = jnp.broadcast_to(columns[i * LANES : (i + 1) * LANES, :], (LANES, LANES))
        parts.append(jnp.transpose(piece)[0:1, :])
    return jnp.concatenate(parts, axis=0)


def wrapped(values, total):
    values = jnp.where(values < 0.0, values + total, values)
    return jnp.where(values >= total, values - total, values)


def exchange_kernel(
    shape, layers, own, piece, names, atoms, weights, scale, shift, mw_in, aw_in, head,
    pot, near, psi, basis_t, all_names,
    rows, basis, lists, acc, part_out, part_in, relay, mw, aw, dens, dens_buf,
    info, info_buf, rows_out, rows_buf, scaled_out, scaled_buf,
    load, list_sem, name_sent, name_got, v_sent, v_got, z_sent, chip_sent,
    part_sent, part_got, psi_sent, psi_got, passed, relay_sent, sent, got,
):
    n_grid, n_atom = shape
    n = n_grid * n_atom
    grid, atom = lax.axis_index("grid"), lax.axis_index("atom")
    me = grid * n_atom + atom
    last, middle = n_grid - 1, n_grid // 2
    side = lax.rem(grid, 2)
    outer, inner = 2 * side, 2 - 2 * side
    og, ig = grid - 1 + 2 * side, grid + 1 - 2 * side
    has_outer = jnp.logical_and(og >= 0, og < n_grid)
    at_split = jnp.logical_or(grid == middle - 1, grid == middle)
    whole = jnp.logical_and(has_outer, jnp.logical_not(at_split))
    relays = jnp.logical_or(grid == 0, grid == last)
    relay_to = jnp.where(grid == middle, 0, last)
    forward_to = jnp.where(grid == 0, middle - 1, middle)

    nb, points, depth = piece.shape
    owned, width, columns = own.shape
    picks = depth // width
    tile = min(columns, TILE)
    relayed = nb // 2
    direct = nb - relayed

    def remote(source, target, send_sem, recv_sem, to):
        pltpu.make_async_remote_copy(
            src_ref=source,
            dst_ref=target,
            send_sem=send_sem,
            recv_sem=recv_sem,
            device_id=to,
            device_id_type=MESH,
        ).start()

    def to_all(source, held, k):
        @pl.loop(1, n)
        def _(d):
            t = lax.rem(me + d, n)
            remote(
                source, held.at[me], sent.at[k], got.at[k],
                (t // n_atom, lax.rem(t, n_atom)),
            )

    def wait_all(held, sem, count):
        wait_bytes(held.at[pl.ds(0, count)], sem)

    def visit(t):
        reach = jnp.minimum(atom, n_atom - 1 - atom)
        close = jnp.where(lax.rem(t, 2) == 1, atom - (t + 1) // 2, atom + t // 2)
        far = jnp.where(reach == atom, t, n_atom - 1 - t)
        return jnp.where(t <= 2 * reach, close, far)

    loads = [
        pltpu.make_async_copy(own, rows.at[pl.ds(1, owned)], load.at[0]),
        pltpu.make_async_copy(mw_in, mw, load.at[1]),
        pltpu.make_async_copy(aw_in, aw, load.at[2]),
    ]
    for copy in loads:
        copy.start()
    meet_all(shape)

    @pl.when(has_outer)
    def _():
        remote(names, all_names.at[inner], name_sent.at[0], name_got.at[inner], (og, atom))
        remote(piece, basis.at[inner, atom], v_sent.at[0], v_got.at[inner, atom], (og, atom))

    remote(names, all_names.at[outer], name_sent.at[1], name_got.at[outer], (ig, atom))
    remote(piece, basis.at[outer, atom], v_sent.at[1], v_got.at[outer, atom], (ig, atom))

    @pl.when(atom < n_atom - 1)
    def _():
        remote(
            piece, basis.at[1, atom], z_sent.at[0, 0, atom], v_got.at[1, atom], (grid, atom + 1)
        )

    @pl.when(atom > 0)
    def _():
        remote(
            piece, basis.at[1, atom], z_sent.at[0, 1, atom], v_got.at[1, atom], (grid, atom - 1)
        )

    total = float(ATOM_DEV * n_atom)
    named = atoms[...].astype(jnp.float32)
    lead = named[0:1, 0:1]
    shifted = wrapped(named - lead + total / 2, total) - total / 2
    least = jnp.min(jnp.min(shifted, axis=1, keepdims=True), axis=0, keepdims=True)
    start = wrapped(lead + least, total)
    place = shifted - least
    lane = lax.broadcasted_iota(jnp.int32, (1, LANES), 1)
    mine = jnp.where(lane < RUN, wrapped(start + lane.astype(jnp.float32), total), -1.0)
    run = lax.broadcasted_iota(jnp.int32, (RUN, LANES), 0).astype(jnp.float32)
    mass = jnp.zeros((RUN, 1), jnp.float32)
    for i in range(nb):
        here = jnp.where(place[i : i + 1, :] == run, weights[i : i + 1, :], 0.0)
        mass = mass + jnp.sum(here, axis=1, keepdims=True)
    info[...] = jnp.where(
        lax.broadcasted_iota(jnp.int32, (RUN, LANES), 1) < LANES // 2,
        wrapped(start + run, total),
        mass,
    )
    to_all(info, info_buf, 1)
    info_buf[me] = info[...]

    basis[1, atom] = piece[...]
    all_names[1] = names[...]
    for edge in (0, owned + 1):
        rows[edge] = jnp.zeros((width, columns), rows.dtype)

    @pl.when(jnp.logical_not(has_outer))
    def _():
        all_names[outer] = jnp.full_like(names, -1)
        part_in[0] = jnp.zeros(part_in.shape[1:], part_in.dtype)

    @pl.when(has_outer)
    def _():
        wait_bytes(names, name_got.at[outer])

    wait_bytes(names, name_got.at[inner])
    copy = pltpu.make_async_copy(all_names, lists, list_sem.at[0])
    copy.start()
    copy.wait()
    loads[0].wait()
    first = grid * owned

    def product(slot, q, i, keep):
        chosen = []
        for j in range(picks):
            block = lists[slot, q * nb + i, j] - first + 1
            chosen.append(jnp.minimum(jnp.maximum(block, 0), owned + 1))
        values = basis[slot, q, i]
        for c in range(columns // tile):
            at = pl.ds(c * tile, tile)
            held = jnp.concatenate(
                [rows[k, :, at] for k in chosen], axis=0
            )
            keep(at, jnp.dot(values, held, preferred_element_type=jnp.float32))

    def outward(phase, q, i, source, target, sent_sem, got_sem):
        @pl.when(whole)
        def _():
            remote(source, target, sent_sem, got_sem, (og, atom))

        if i < direct:

            @pl.when(at_split)
            def _():
                remote(source, target, sent_sem, got_sem, (og, atom))
        else:

            @pl.when(at_split)
            def _():
                remote(
                    source, relay.at[phase, q, i - direct], sent_sem, passed.at[phase, q],
                    (relay_to, atom),
                )

    def forward(phase, r):
        q = visit(r)

        @pl.when(relays)
        def _():
            held = relay.at[phase, q]
            wait_bytes(held, passed.at[phase, q])
            at = pl.ds(q * nb + direct, relayed)
            if phase == 0:
                target, got_sem = part_in.at[0, at], part_got.at[0, q]
            else:
                target, got_sem = psi.at[inner, at], psi_got.at[inner, q]
            remote(held, target, relay_sent.at[phase], got_sem, (forward_to, atom))

    def finish(q):
        wait_bytes(part_in.at[1, pl.ds(q * nb, nb)], part_got.at[1, q])

        @pl.when(has_outer)
        def _():
            wait_bytes(part_in.at[0, pl.ds(q * nb, nb)], part_got.at[0, q])

        for i in range(nb):
            b = q * nb + i
            sums = jnp.zeros((points, LANES), jnp.float32)
            for c in range(columns // LANES):
                at = pl.ds(c * LANES, LANES)
                value = (
                    acc[b, :, at]
                    + part_in[0, b, :, at].astype(jnp.float32)
                    + part_in[1, b, :, at].astype(jnp.float32)
                )
                rounded = value.astype(jnp.bfloat16)
                psi[1, b, :, at] = rounded
                sums = sums + jnp.square(rounded.astype(jnp.float32))
            dens[q, i : i + 1, :] = jnp.sum(jnp.transpose(sums), axis=0, keepdims=True)

        @pl.when(q != atom)
        def _():
            remote(dens.at[q], dens_buf.at[atom], sent.at[0], got.at[0], (grid, q))

        at = pl.ds(q * nb, nb)
        remote(psi.at[1, at], psi.at[outer, at], psi_sent.at[1], psi_got.at[outer, q], (ig, atom))

    def psi_round(r):
        q = visit(r)
        for i in range(nb):
            b = q * nb + i
            outward(
                1, q, i, psi.at[1, b], psi.at[inner, b], psi_sent.at[0], psi_got.at[inner, q]
            )

    @pl.loop(0, n_atom)
    def _(t):
        q = visit(t)

        @pl.when(t > 0)
        def _():
            wait_bytes(piece, v_got.at[1, q])
            remote(
                basis.at[1, q], basis.at[outer, q], chip_sent.at[q], v_got.at[outer, q],
                (ig, atom),
            )

        def along(stream, slot):
            for way in range(2):
                able = (
                    jnp.logical_and(q <= atom, atom < n_atom - 1)
                    if way == 0
                    else jnp.logical_and(q >= atom, atom > 0)
                )

                @pl.when(able)
                def _():
                    remote(
                        basis.at[slot, q], basis.at[slot, q], z_sent.at[stream, way, q],
                        v_got.at[slot, q], (grid, atom + 1 - 2 * way),
                    )

        @pl.when(has_outer)
        def _():
            wait_bytes(piece, v_got.at[outer, q])
            along(1, outer)

        @pl.when(t > 0)
        def _():
            along(0, 1)

        @pl.when(has_outer)
        def _():
            for i in range(nb):
                b = q * nb + i

                def keep(at, value):
                    part_out[0, b, :, at] = value.astype(jnp.bfloat16)

                product(outer, q, i, keep)
                outward(
                    0, q, i, part_out.at[0, b], part_in.at[0, b], part_sent.at[0],
                    part_got.at[0, q],
                )

        wait_bytes(piece, v_got.at[inner, q])
        for i in range(nb):
            b = q * nb + i

            def keep(at, value):
                part_out[1, b, :, at] = value.astype(jnp.bfloat16)

            product(inner, q, i, keep)
            remote(
                part_out.at[1, b], part_in.at[1, b], part_sent.at[1], part_got.at[1, q],
                (ig, atom),
            )

        for i in range(nb):
            b = q * nb + i

            def keep(at, value):
                acc[b, :, at] = value

            product(1, q, i, keep)
            for slot in range(3):
                basis_t[slot, b] = jnp.transpose(basis[slot, q, i])

        @pl.when(t >= 1)
        def _():
            forward(0, t - 1)

        @pl.when(t >= 2)
        def _():
            finish(visit(t - 2))

    stops = layers + 2

    def rounds(s, act):
        for r in range(n_atom):
            if r * stops // n_atom == s:
                act(r)

    if n_atom < 3:
        finish(visit(0))
    rounds(0, psi_round)
    if n_atom >= 3:
        finish(visit(n_atom - 2))
    forward(0, n_atom - 1)
    finish(visit(n_atom - 1))
    dens_buf[atom] = dens[atom]

    weight = to_columns(weights[...])[:, 0:1]
    spot = to_columns(place)
    hot = (spot == lax.broadcasted_iota(jnp.int32, spot.shape, 1).astype(jnp.float32)).astype(
        jnp.bfloat16
    )
    deep = lax.broadcasted_iota(jnp.int32, (LANES, LANES), 0).astype(jnp.float32)
    hot_t = jnp.concatenate([place[i : i + 1, :] == deep for i in range(nb)], axis=1).astype(
        jnp.bfloat16
    )
    loads[1].wait()
    loads[2].wait()
    halves = scale.shape[1] // LANES
    wait_all(info_buf, got.at[1], n - 1)
    facts = info_buf[...].reshape(n * RUN, LANES)
    same = (facts[:, 0:1] == mine).astype(jnp.float32)
    mass = jnp.sum(same * facts[:, LANES // 2 : LANES // 2 + 1], axis=0, keepdims=True)
    share = 1.0 / (1.0 + to_columns(mass)[:, 0:1])
    same = same.reshape(n, RUN, LANES)
    none = jnp.zeros_like(same)
    selects = []
    for h in range(halves):
        full = jnp.concatenate(
            [same if k == h else none for k in range(halves)], axis=1
        ).reshape(n * RUN * halves, LANES)
        selects.append(jnp.transpose(full).astype(jnp.bfloat16))

    wait_all(dens_buf, got.at[0], n_atom - 1)
    density = to_columns(2.0 * jnp.sum(dens_buf[...], axis=0))
    safe = jnp.where(density > 0.0, density, 1.0)
    radius = jnp.where(density > 0.0, jnp.exp(jnp.log(safe) * (1.0 / 3.0)), 0.0)[:, 0:1]
    hidden = jax.nn.silu(radius * scale[...] + shift[...])
    for layer in range(layers):
        message = jax.nn.silu(
            jnp.dot(hidden.astype(jnp.bfloat16), mw[layer], preferred_element_type=jnp.float32)
        )
        weighted = (weight * message).astype(jnp.bfloat16)
        part = jnp.dot(hot_t, weighted, preferred_element_type=jnp.float32)
        rows_out[layer] = jnp.concatenate(
            [part[0:RUN, h * LANES : (h + 1) * LANES] for h in range(halves)], axis=0
        ).astype(jnp.bfloat16)
        to_all(rows_out.at[layer], rows_buf.at[layer], 2 + layer)
        rounds(1 + layer, psi_round)
        rows_buf[layer, me] = rows_out[layer]
        wait_all(rows_buf.at[layer], got.at[2 + layer], n - 1)
        rounds(layer, functools.partial(forward, 1))
        held = rows_buf[layer].reshape(n * RUN * halves, LANES)
        summed = jnp.concatenate(
            [jnp.dot(pick, held, preferred_element_type=jnp.float32) for pick in selects], axis=1
        )
        update = jax.nn.silu(
            jnp.dot(
                (summed * share).astype(jnp.bfloat16), aw[layer],
                preferred_element_type=jnp.float32,
            )
        ).astype(jnp.bfloat16)
        picked = jnp.dot(hot, update, preferred_element_type=jnp.float32)
        hidden = hidden + message * picked
    score = jnp.sum(hidden * head[...], axis=1, keepdims=True)
    potential = radius * (1.0 + jnp.tanh(score))
    pot[...] = to_rows(potential)
    final = 2 + layers
    scaled_out[...] = to_rows(weight * potential)
    to_all(scaled_out, scaled_buf, final)
    rounds(layers + 1, psi_round)
    scaled_buf[me] = scaled_out[...]
    wait_all(scaled_buf, got.at[final], n - 1)
    rounds(layers, functools.partial(forward, 1))
    rounds(layers + 1, functools.partial(forward, 1))
    for k in range(3):
        group = jnp.clip(grid - 1 + k, 0, n_grid - 1)
        near[k * n_atom : (k + 1) * n_atom] = scaled_buf[pl.ds(group * n_atom, n_atom)]

    @pl.loop(0, n_atom)
    def _(q):
        at = pl.ds(q * nb, nb)
        wait_bytes(psi.at[inner, at], psi_got.at[inner, q])

        @pl.when(has_outer)
        def _():
            wait_bytes(psi.at[outer, at], psi_got.at[outer, q])

        @pl.when(q != atom)
        def _():
            wait_bytes(piece, chip_sent.at[q])

        for way in range(2):
            able = (
                jnp.logical_and(q <= atom, atom < n_atom - 1)
                if way == 0
                else jnp.logical_and(q >= atom, atom > 0)
            )

            @pl.when(able)
            def _():
                wait_bytes(piece, z_sent.at[0, way, q])

            @pl.when(jnp.logical_and(able, has_outer))
            def _():
                wait_bytes(piece, z_sent.at[1, way, q])

    @pl.when(has_outer)
    def _():
        wait_bytes(names, name_sent.at[0])
        wait_bytes(piece, v_sent.at[0])
        wait_bytes(part_out.at[0], part_sent.at[0])
        wait_bytes(psi.at[1], psi_sent.at[0])

    wait_bytes(names, name_sent.at[1])
    wait_bytes(piece, v_sent.at[1])
    wait_bytes(part_out.at[1], part_sent.at[1])
    wait_bytes(psi.at[1], psi_sent.at[1])

    @pl.when(relays)
    def _():
        for phase in range(2):
            wait_bytes(relay.at[phase], relay_sent.at[phase])

    wait_all(dens_buf, sent.at[0], n_atom - 1)
    wait_all(info_buf, sent.at[1], n - 1)
    for layer in range(layers):
        wait_all(rows_buf.at[layer], sent.at[2 + layer], n - 1)
    wait_all(scaled_buf, sent.at[final], n - 1)


def exchange_of(shape, own, piece, names, atoms, weights, scale, shift, mw, aw, head):
    n_grid, n_atom = shape
    n = n_grid * n_atom
    nb, points, depth = piece.shape
    count = nb * n_atom
    width, columns = own.shape[1:]
    layers, features, _ = mw.shape
    packed = RUN * (features // LANES)
    bf16, f32 = jnp.bfloat16, jnp.float32
    dma = pltpu.SemaphoreType.DMA
    grant = 2 * own.size + 14 * count * points * columns + 6 * count * depth * points
    grant += n * (packed * LANES * (2 * layers + 8) + 12 * RUN * LANES) + (6 << 20)
    given = 6 * count * points * (columns + depth)
    if grant + given > 48 << 20:
        grant = 60 << 20
    return pl.pallas_call(
        functools.partial(exchange_kernel, shape, layers),
        out_shape=(
            jax.ShapeDtypeStruct((nb, points), f32),
            jax.ShapeDtypeStruct((3 * n_atom, nb, points), f32),
            jax.ShapeDtypeStruct((3, count, points, columns), bf16),
            jax.ShapeDtypeStruct((3, count, depth, points), bf16),
            jax.ShapeDtypeStruct((3, *names.shape), names.dtype),
        ),
        in_specs=[HBM] + [VMEM] * 6 + [HBM, HBM, VMEM],
        out_specs=(VMEM,) * 5,
        scratch_shapes=[
            pltpu.VMEM((own.shape[0] + 2, width, columns), bf16),
            pltpu.VMEM((3, n_atom, nb, points, depth), bf16),
            pltpu.SMEM((3, *names.shape), names.dtype),
            pltpu.VMEM((count, points, columns), f32),
            pltpu.VMEM((2, count, points, columns), bf16),
            pltpu.VMEM((2, count, points, columns), bf16),
            pltpu.VMEM((2, n_atom, nb // 2, points, columns), bf16),
            pltpu.VMEM(mw.shape, bf16),
            pltpu.VMEM(aw.shape, bf16),
            pltpu.VMEM((n_atom, nb, points), f32),
            pltpu.VMEM((n_atom, nb, points), f32),
            pltpu.VMEM((RUN, LANES), f32),
            pltpu.VMEM((n, RUN, LANES), f32),
            pltpu.VMEM((layers, packed, LANES), bf16),
            pltpu.VMEM((layers, n, packed, LANES), bf16),
            pltpu.VMEM((nb, points), f32),
            pltpu.VMEM((n, nb, points), f32),
            dma((3,)),
            dma((1,)),
            dma((2,)),
            dma((3,)),
            dma((2,)),
            dma((3, n_atom)),
            dma((2, 2, n_atom)),
            dma((n_atom,)),
            dma((2,)),
            dma((2, n_atom)),
            dma((2,)),
            dma((3, n_atom)),
            dma((2, n_atom)),
            dma((2,)),
            dma((3 + layers,)),
            dma((3 + layers,)),
        ],
        compiler_params=pltpu.CompilerParams(
            collective_id=0, has_side_effects=True, vmem_limit_bytes=grant
        ),
        name="exchange_of",
    )(own, piece, names, atoms, weights, scale, shift, mw, aw, head)


def fock_kernel(lists, basis_t, near, psi, out, scaled):
    step = pl.program_id(0)
    groups, count, depth, points = basis_t.shape
    picks = lists.shape[1]
    width = depth // picks
    wide = out.shape[1]
    owned = out.shape[0] // width
    columns = pl.ds(pl.multiple_of(step * wide, wide), wide)

    out[...] = jnp.zeros_like(out)

    @pl.loop(0, groups * count)
    def _(s):
        k, b = s // count, lax.rem(s, count)
        for j in range(picks):
            block = lists[s, j]

            @pl.when(jnp.logical_and(block >= 0, block < owned))
            def _():
                part = slice(j * width, (j + 1) * width)

                @pl.when(step == 0)
                def _():
                    scaled[s, part, :] = (
                        basis_t[k, b, part, :].astype(jnp.float32) * near[pl.ds(s, 1), :]
                    ).astype(jnp.bfloat16)

                at = pl.ds(pl.multiple_of(block * width, width), width)
                out[at, :] += jnp.dot(
                    scaled[s, part, :], psi[k, b, :, columns], preferred_element_type=jnp.float32
                )


def fock_of(lists, basis_t, near, psi, owned):
    groups, count, depth, points = basis_t.shape
    columns = psi.shape[3]
    wide = min(columns, 256)
    grant = 2 * (9 * count * depth * points + 6 * count * points * wide + 4 * owned * wide)
    return pl.pallas_call(
        fock_kernel,
        out_shape=jax.ShapeDtypeStruct((owned, columns), jnp.float32),
        grid_spec=pltpu.PrefetchScalarGridSpec(
            num_scalar_prefetch=1,
            grid=(columns // wide,),
            in_specs=[VMEM, VMEM, VMEM],
            out_specs=pl.BlockSpec((owned, wide), lambda i, lists: (0, i)),
            scratch_shapes=[pltpu.VMEM((groups * count, depth, points), jnp.bfloat16)],
        ),
        compiler_params=pltpu.CompilerParams(vmem_limit_bytes=grant + (12 << 20)),
        name="fock_of",
    )(lists, basis_t, near, psi)


def local(
    basis_values,
    block_lists,
    orbitals,
    point_weights,
    point_atoms,
    embed_scale,
    embed_shift,
    message_weight,
    atom_weight,
    head_weight,
):
    n_grid, n_atom = lax.axis_size("grid"), lax.axis_size("atom")
    own_rows = orbitals.shape[0]
    batches, points, depth = basis_values.shape
    picks = block_lists.shape[1]
    owned = own_rows // (depth // picks)
    first = lax.axis_index("grid") * owned
    names = jnp.pad(block_lists, ((0, 0), (0, LANES - picks)))
    potential, near, psi, basis_t, names = exchange_of(
        (n_grid, n_atom),
        orbitals.reshape(owned, own_rows // owned, -1),
        basis_values,
        names,
        point_atoms.reshape(batches, points),
        point_weights.reshape(batches, points),
        embed_scale[None, :],
        embed_shift[None, :],
        message_weight,
        atom_weight,
        head_weight[None, :],
    )
    lists = names[:, :, :picks].reshape(-1, picks) - first
    fock = fock_of(lists, basis_t, near.reshape(-1, points), psi, own_rows)
    return (fock, potential.reshape(-1))


def solution(mesh):
    return jax.shard_map(
        local,
        mesh=mesh,
        in_specs=(
            P(("grid", "atom"), None, None),
            P("grid", None),
            P("grid", "atom"),
            P(("grid", "atom")),
            P(("grid", "atom")),
            P(),
            P(),
            P(),
            P(),
            P(),
        ),
        out_specs=(P("grid", "atom"), P(("grid", "atom"))),
        check_vma=False,
    )
```

```python
import functools
import jax
import jax.numpy as jnp
from jax import lax
from jax.experimental import pallas as pl
from jax.experimental.pallas import tpu as pltpu
from jax.sharding import PartitionSpec as P

ATOM_DEV = 32
RUN = max(ATOM_DEV // 4, 1)
LANES = 128
VMEM = pl.BlockSpec(memory_space=pltpu.VMEM)
HBM = pl.BlockSpec(memory_space=pltpu.HBM)
MESH = pl.DeviceIdType.MESH
TILE = 256


def wait_bytes(ref, sem):
    pltpu.make_async_copy(ref, ref, sem).wait()


def meet_all(shape):
    n_grid, n_atom = shape
    n = n_grid * n_atom
    me = lax.axis_index("grid") * n_atom + lax.axis_index("atom")
    barrier = pltpu.get_barrier_semaphore()

    @pl.loop(1, n)
    def _(d):
        t = lax.rem(me + d, n)
        pl.semaphore_signal(
            barrier, inc=1, device_id=(t // n_atom, lax.rem(t, n_atom)), device_id_type=MESH
        )

    pl.semaphore_wait(barrier, n - 1)


def to_columns(rows):
    parts = [
        jnp.transpose(jnp.broadcast_to(rows[i : i + 1, :], (LANES, LANES)))
        for i in range(rows.shape[0])
    ]
    return jnp.concatenate(parts, axis=0)


def to_rows(columns):
    parts = []
    for i in range(columns.shape[0] // LANES):
        piece = jnp.broadcast_to(columns[i * LANES : (i + 1) * LANES, :], (LANES, LANES))
        parts.append(jnp.transpose(piece)[0:1, :])
    return jnp.concatenate(parts, axis=0)


def wrapped(values, total):
    values = jnp.where(values < 0.0, values + total, values)
    return jnp.where(values >= total, values - total, values)


def exchange_kernel(
    shape, layers, own, piece, names, *rest,
):
    given, rest = rest[:7], rest[7:]
    pot, near, psi, basis_t, all_names = rest[:5]
    atoms, weights, scale, shift, mw, aw, head = rest[5:12]
    (
        rows, basis, lists, acc, part_out, part_in, relay, dens, dens_buf,
        info, info_buf, rows_out, rows_buf, scaled_out, scaled_buf,
        load, list_sem, name_sent, name_got, v_sent, v_got, z_sent, chip_sent,
        part_sent, part_got, psi_sent, psi_got, passed, relay_sent, sent, got,
    ) = rest[12:]
    n_grid, n_atom = shape
    n = n_grid * n_atom
    grid, atom = lax.axis_index("grid"), lax.axis_index("atom")
    me = grid * n_atom + atom
    last, middle = n_grid - 1, n_grid // 2
    side = lax.rem(grid, 2)
    outer, inner = 2 * side, 2 - 2 * side
    og, ig = grid - 1 + 2 * side, grid + 1 - 2 * side
    has_outer = jnp.logical_and(og >= 0, og < n_grid)
    at_split = jnp.logical_or(grid == middle - 1, grid == middle)
    whole = jnp.logical_and(has_outer, jnp.logical_not(at_split))
    relays = jnp.logical_or(grid == 0, grid == last)
    relay_to = jnp.where(grid == middle, 0, last)
    forward_to = jnp.where(grid == 0, middle - 1, middle)

    nb, points, depth = piece.shape
    owned, width, columns = own.shape
    picks = depth // width
    tile = min(columns, TILE)
    relayed = nb // 2
    direct = nb - relayed

    def remote(source, target, send_sem, recv_sem, to):
        pltpu.make_async_remote_copy(
            src_ref=source,
            dst_ref=target,
            send_sem=send_sem,
            recv_sem=recv_sem,
            device_id=to,
            device_id_type=MESH,
        ).start()

    def to_all(source, held, k):
        @pl.loop(1, n)
        def _(d):
            t = lax.rem(me + d, n)
            remote(
                source, held.at[me], sent.at[k], got.at[k],
                (t // n_atom, lax.rem(t, n_atom)),
            )

    def wait_all(held, sem, count):
        wait_bytes(held.at[pl.ds(0, count)], sem)

    def visit(t):
        reach = jnp.minimum(atom, n_atom - 1 - atom)
        close = jnp.where(lax.rem(t, 2) == 1, atom - (t + 1) // 2, atom + t // 2)
        far = jnp.where(reach == atom, t, n_atom - 1 - t)
        return jnp.where(t <= 2 * reach, close, far)

    held_here = (
        rows.at[pl.ds(1, owned)], basis.at[1, atom], all_names.at[1],
        atoms, weights, scale, shift, mw, aw, head,
    )
    loads = [
        pltpu.make_async_copy(source, target, load.at[i])
        for i, (source, target) in enumerate(zip((own, piece, names, *given), held_here))
    ]
    for copy in loads:
        copy.start()
    meet_all(shape)

    @pl.when(has_outer)
    def _():
        remote(names, all_names.at[inner], name_sent.at[0], name_got.at[inner], (og, atom))
        remote(piece, basis.at[inner, atom], v_sent.at[0], v_got.at[inner, atom], (og, atom))

    remote(names, all_names.at[outer], name_sent.at[1], name_got.at[outer], (ig, atom))
    remote(piece, basis.at[outer, atom], v_sent.at[1], v_got.at[outer, atom], (ig, atom))

    @pl.when(atom < n_atom - 1)
    def _():
        remote(
            piece, basis.at[1, atom], z_sent.at[0, 0, atom], v_got.at[1, atom], (grid, atom + 1)
        )

    @pl.when(atom > 0)
    def _():
        remote(
            piece, basis.at[1, atom], z_sent.at[0, 1, atom], v_got.at[1, atom], (grid, atom - 1)
        )

    for copy in loads[1:5]:
        copy.wait()
    total = float(ATOM_DEV * n_atom)
    named = atoms[...].astype(jnp.float32)
    lead = named[0:1, 0:1]
    shifted = wrapped(named - lead + total / 2, total) - total / 2
    least = jnp.min(jnp.min(shifted, axis=1, keepdims=True), axis=0, keepdims=True)
    start = wrapped(lead + least, total)
    place = shifted - least
    lane = lax.broadcasted_iota(jnp.int32, (1, LANES), 1)
    mine = jnp.where(lane < RUN, wrapped(start + lane.astype(jnp.float32), total), -1.0)
    run = lax.broadcasted_iota(jnp.int32, (RUN, LANES), 0).astype(jnp.float32)
    mass = jnp.zeros((RUN, 1), jnp.float32)
    for i in range(nb):
        here = jnp.where(place[i : i + 1, :] == run, weights[i : i + 1, :], 0.0)
        mass = mass + jnp.sum(here, axis=1, keepdims=True)
    info[...] = jnp.where(
        lax.broadcasted_iota(jnp.int32, (RUN, LANES), 1) < LANES // 2,
        wrapped(start + run, total),
        mass,
    )
    to_all(info, info_buf, 1)
    info_buf[me] = info[...]

    for edge in (0, owned + 1):
        rows[edge] = jnp.zeros((width, columns), rows.dtype)

    @pl.when(jnp.logical_not(has_outer))
    def _():
        all_names[outer] = jnp.full(names.shape, -1, names.dtype)
        part_in[0] = jnp.zeros(part_in.shape[1:], part_in.dtype)

    @pl.when(has_outer)
    def _():
        wait_bytes(names, name_got.at[outer])

    wait_bytes(names, name_got.at[inner])
    copy = pltpu.make_async_copy(all_names, lists, list_sem.at[0])
    copy.start()
    copy.wait()
    loads[0].wait()
    first = grid * owned

    def product(slot, q, i, keep):
        chosen = []
        for j in range(picks):
            block = lists[slot, j, q * nb + i] - first + 1
            chosen.append(jnp.minimum(jnp.maximum(block, 0), owned + 1))
        values = basis[slot, q, i]
        for c in range(columns // tile):
            at = pl.ds(c * tile, tile)
            held = jnp.concatenate(
                [rows[k, :, at] for k in chosen], axis=0
            )
            keep(at, jnp.dot(values, held, preferred_element_type=jnp.float32))

    def outward(phase, q, i, source, target, sent_sem, got_sem):
        @pl.when(whole)
        def _():
            remote(source, target, sent_sem, got_sem, (og, atom))

        if i < direct:

            @pl.when(at_split)
            def _():
                remote(source, target, sent_sem, got_sem, (og, atom))
        else:

            @pl.when(at_split)
            def _():
                remote(
                    source, relay.at[phase, q, i - direct], sent_sem, passed.at[phase, q],
                    (relay_to, atom),
                )

    def forward(phase, r):
        q = visit(r)

        @pl.when(relays)
        def _():
            held = relay.at[phase, q]
            wait_bytes(held, passed.at[phase, q])
            at = pl.ds(q * nb + direct, relayed)
            if phase == 0:
                target, got_sem = part_in.at[0, at], part_got.at[0, q]
            else:
                target, got_sem = psi.at[inner, at], psi_got.at[inner, q]
            remote(held, target, relay_sent.at[phase], got_sem, (forward_to, atom))

    def finish(q):
        wait_bytes(part_in.at[1, pl.ds(q * nb, nb)], part_got.at[1, q])

        @pl.when(has_outer)
        def _():
            wait_bytes(part_in.at[0, pl.ds(q * nb, nb)], part_got.at[0, q])

        for i in range(nb):
            b = q * nb + i
            sums = jnp.zeros((points, LANES), jnp.float32)
            for c in range(columns // LANES):
                at = pl.ds(c * LANES, LANES)
                value = (
                    acc[b, :, at]
                    + part_in[0, b, :, at].astype(jnp.float32)
                    + part_in[1, b, :, at].astype(jnp.float32)
                )
                rounded = value.astype(jnp.bfloat16)
                psi[1, b, :, at] = rounded
                sums = sums + jnp.square(rounded.astype(jnp.float32))
            dens[q, i : i + 1, :] = jnp.sum(jnp.transpose(sums), axis=0, keepdims=True)

        @pl.when(q != atom)
        def _():
            remote(dens.at[q], dens_buf.at[atom], sent.at[0], got.at[0], (grid, q))

        at = pl.ds(q * nb, nb)
        remote(psi.at[1, at], psi.at[outer, at], psi_sent.at[1], psi_got.at[outer, q], (ig, atom))

    def psi_round(r):
        q = visit(r)
        for i in range(nb):
            b = q * nb + i
            outward(
                1, q, i, psi.at[1, b], psi.at[inner, b], psi_sent.at[0], psi_got.at[inner, q]
            )

    reach = jnp.minimum(atom, n_atom - 1 - atom)

    def along(stream, slot, q):
        for way in range(2):
            able = (
                jnp.logical_and(q <= atom, atom < n_atom - 1)
                if way == 0
                else jnp.logical_and(q >= atom, atom > 0)
            )

            @pl.when(able)
            def _():
                remote(
                    basis.at[slot, q], basis.at[slot, q], z_sent.at[stream, way, q],
                    v_got.at[slot, q], (grid, atom + 1 - 2 * way),
                )

    def spread_outer(t):
        q = visit(t)

        @pl.when(has_outer)
        def _():
            wait_bytes(basis.at[outer, q], v_got.at[outer, q])
            along(1, outer, q)

    def spread_own(t):
        q = visit(t)
        wait_bytes(basis.at[1, q], v_got.at[1, q])
        along(0, 1, q)
        remote(
            basis.at[1, q], basis.at[outer, q], chip_sent.at[q], v_got.at[outer, q], (ig, atom)
        )

    spread_outer(0)

    @pl.loop(0, n_atom)
    def _(t):
        q = visit(t)
        paired = jnp.logical_and(lax.rem(t, 2) == 1, t < 2 * reach)
        fresh = jnp.logical_and(
            t > 0, jnp.logical_or(lax.rem(t, 2) == 1, t > 2 * reach)
        )

        @pl.when(fresh)
        def _():
            spread_outer(t)

        @pl.when(paired)
        def _():
            spread_outer(t + 1)

        @pl.when(fresh)
        def _():
            spread_own(t)

        @pl.when(paired)
        def _():
            spread_own(t + 1)

        @pl.when(has_outer)
        def _():
            for i in range(nb):
                b = q * nb + i

                def keep(at, value):
                    part_out[0, b, :, at] = value.astype(jnp.bfloat16)

                product(outer, q, i, keep)
                outward(
                    0, q, i, part_out.at[0, b], part_in.at[0, b], part_sent.at[0],
                    part_got.at[0, q],
                )

        wait_bytes(basis.at[inner, q], v_got.at[inner, q])
        for i in range(nb):
            b = q * nb + i

            def keep(at, value):
                part_out[1, b, :, at] = value.astype(jnp.bfloat16)

            product(inner, q, i, keep)
            remote(
                part_out.at[1, b], part_in.at[1, b], part_sent.at[1], part_got.at[1, q],
                (ig, atom),
            )

        for i in range(nb):
            b = q * nb + i

            def keep(at, value):
                acc[b, :, at] = value

            product(1, q, i, keep)
            for slot in range(3):
                basis_t[slot, b] = jnp.transpose(basis[slot, q, i])

        @pl.when(t >= 1)
        def _():
            forward(0, t - 1)

        @pl.when(t >= 2)
        def _():
            finish(visit(t - 2))

    stops = layers + 2

    def rounds(s, act):
        for r in range(n_atom):
            if r * stops // n_atom == s:
                act(r)

    if n_atom < 3:
        finish(visit(0))
    rounds(0, psi_round)
    if n_atom >= 3:
        finish(visit(n_atom - 2))
    weight = to_columns(weights[...])[:, 0:1]
    spot = to_columns(place)
    hot = (spot == lax.broadcasted_iota(jnp.int32, spot.shape, 1).astype(jnp.float32)).astype(
        jnp.bfloat16
    )
    deep = lax.broadcasted_iota(jnp.int32, (LANES, LANES), 0).astype(jnp.float32)
    hot_t = jnp.concatenate([place[i : i + 1, :] == deep for i in range(nb)], axis=1).astype(
        jnp.bfloat16
    )
    for copy in loads[5:]:
        copy.wait()
    halves = scale.shape[1] // LANES
    wait_all(info_buf, got.at[1], n - 1)
    facts = info_buf[...].reshape(n * RUN, LANES)
    same = (facts[:, 0:1] == mine).astype(jnp.float32)
    mass = jnp.sum(same * facts[:, LANES // 2 : LANES // 2 + 1], axis=0, keepdims=True)
    share = 1.0 / (1.0 + to_columns(mass)[:, 0:1])
    same = same.reshape(n, RUN, LANES)
    none = jnp.zeros_like(same)
    selects = []
    for h in range(halves):
        full = jnp.concatenate(
            [same if k == h else none for k in range(halves)], axis=1
        ).reshape(n * RUN * halves, LANES)
        selects.append(jnp.transpose(full).astype(jnp.bfloat16))

    forward(0, n_atom - 1)
    finish(visit(n_atom - 1))
    dens_buf[atom] = dens[atom]

    wait_all(dens_buf, got.at[0], n_atom - 1)
    density = to_columns(2.0 * jnp.sum(dens_buf[...], axis=0))
    safe = jnp.where(density > 0.0, density, 1.0)
    radius = jnp.where(density > 0.0, jnp.exp(jnp.log(safe) * (1.0 / 3.0)), 0.0)[:, 0:1]
    hidden = jax.nn.silu(radius * scale[...] + shift[...])
    for layer in range(layers):
        message = jax.nn.silu(
            jnp.dot(hidden.astype(jnp.bfloat16), mw[layer], preferred_element_type=jnp.float32)
        )
        weighted = (weight * message).astype(jnp.bfloat16)
        part = jnp.dot(hot_t, weighted, preferred_element_type=jnp.float32)
        rows_out[layer] = jnp.concatenate(
            [part[0:RUN, h * LANES : (h + 1) * LANES] for h in range(halves)], axis=0
        ).astype(jnp.bfloat16)
        to_all(rows_out.at[layer], rows_buf.at[layer], 2 + layer)
        rounds(1 + layer, psi_round)
        rows_buf[layer, me] = rows_out[layer]
        wait_all(rows_buf.at[layer], got.at[2 + layer], n - 1)
        rounds(layer, functools.partial(forward, 1))
        held = rows_buf[layer].reshape(n * RUN * halves, LANES)
        summed = jnp.concatenate(
            [jnp.dot(pick, held, preferred_element_type=jnp.float32) for pick in selects], axis=1
        )
        update = jax.nn.silu(
            jnp.dot(
                (summed * share).astype(jnp.bfloat16), aw[layer],
                preferred_element_type=jnp.float32,
            )
        ).astype(jnp.bfloat16)
        picked = jnp.dot(hot, update, preferred_element_type=jnp.float32)
        hidden = hidden + message * picked
    score = jnp.sum(hidden * head[...], axis=1, keepdims=True)
    potential = radius * (1.0 + jnp.tanh(score))
    pot[...] = to_rows(potential)
    final = 2 + layers
    scaled_out[...] = to_rows(weight * potential)
    to_all(scaled_out, scaled_buf, final)
    rounds(layers + 1, psi_round)
    scaled_buf[me] = scaled_out[...]
    wait_all(scaled_buf, got.at[final], n - 1)
    rounds(layers, functools.partial(forward, 1))
    rounds(layers + 1, functools.partial(forward, 1))
    for k in range(3):
        group = jnp.clip(grid - 1 + k, 0, n_grid - 1)
        near[k * n_atom : (k + 1) * n_atom] = scaled_buf[pl.ds(group * n_atom, n_atom)]

    @pl.loop(0, n_atom)
    def _(q):
        at = pl.ds(q * nb, nb)
        wait_bytes(psi.at[inner, at], psi_got.at[inner, q])

        @pl.when(has_outer)
        def _():
            wait_bytes(psi.at[outer, at], psi_got.at[outer, q])

        @pl.when(q != atom)
        def _():
            wait_bytes(basis.at[1, q], chip_sent.at[q])

        for way in range(2):
            able = (
                jnp.logical_and(q <= atom, atom < n_atom - 1)
                if way == 0
                else jnp.logical_and(q >= atom, atom > 0)
            )

            @pl.when(able)
            def _():
                wait_bytes(basis.at[1, q], z_sent.at[0, way, q])

            @pl.when(jnp.logical_and(able, has_outer))
            def _():
                wait_bytes(basis.at[1, q], z_sent.at[1, way, q])

    @pl.when(has_outer)
    def _():
        wait_bytes(names, name_sent.at[0])
        wait_bytes(piece, v_sent.at[0])
        wait_bytes(part_out.at[0], part_sent.at[0])
        wait_bytes(psi.at[1], psi_sent.at[0])

    wait_bytes(names, name_sent.at[1])
    wait_bytes(piece, v_sent.at[1])
    wait_bytes(part_out.at[1], part_sent.at[1])
    wait_bytes(psi.at[1], psi_sent.at[1])

    @pl.when(relays)
    def _():
        for phase in range(2):
            wait_bytes(relay.at[phase], relay_sent.at[phase])

    wait_all(dens_buf, sent.at[0], n_atom - 1)
    wait_all(info_buf, sent.at[1], n - 1)
    for layer in range(layers):
        wait_all(rows_buf.at[layer], sent.at[2 + layer], n - 1)
    wait_all(scaled_buf, sent.at[final], n - 1)


def exchange_of(shape, own, piece, names, atoms, weights, scale, shift, mw, aw, head):
    n_grid, n_atom = shape
    n = n_grid * n_atom
    nb, points, depth = piece.shape
    count = nb * n_atom
    width, columns = own.shape[1:]
    layers, features, _ = mw.shape
    packed = RUN * (features // LANES)
    bf16, f32 = jnp.bfloat16, jnp.float32
    dma = pltpu.SemaphoreType.DMA
    grant = 2 * own.size + 14 * count * points * columns + 6 * count * depth * points
    grant += n * (packed * LANES * (2 * layers + 8) + 12 * RUN * LANES) + (6 << 20)
    given = 6 * count * points * (columns + depth)
    if grant + given > 48 << 20:
        grant = 60 << 20
    return pl.pallas_call(
        functools.partial(exchange_kernel, shape, layers),
        out_shape=(
            jax.ShapeDtypeStruct((nb, points), f32),
            jax.ShapeDtypeStruct((3 * n_atom, nb, points), f32),
            jax.ShapeDtypeStruct((3, count, points, columns), bf16),
            jax.ShapeDtypeStruct((3, count, depth, points), bf16),
            jax.ShapeDtypeStruct((3, *names.shape), names.dtype),
        ),
        in_specs=[HBM] * 10,
        out_specs=(VMEM,) * 5,
        scratch_shapes=[
            pltpu.VMEM(a.shape, a.dtype) for a in (atoms, weights, scale, shift, mw, aw, head)
        ]
        + [
            pltpu.VMEM((own.shape[0] + 2, width, columns), bf16),
            pltpu.VMEM((3, n_atom, nb, points, depth), bf16),
            pltpu.SMEM((3, *names.shape), names.dtype),
            pltpu.VMEM((count, points, columns), f32),
            pltpu.VMEM((2, count, points, columns), bf16),
            pltpu.VMEM((2, count, points, columns), bf16),
            pltpu.VMEM((2, n_atom, nb // 2, points, columns), bf16),
            pltpu.VMEM((n_atom, nb, points), f32),
            pltpu.VMEM((n_atom, nb, points), f32),
            pltpu.VMEM((RUN, LANES), f32),
            pltpu.VMEM((n, RUN, LANES), f32),
            pltpu.VMEM((layers, packed, LANES), bf16),
            pltpu.VMEM((layers, n, packed, LANES), bf16),
            pltpu.VMEM((nb, points), f32),
            pltpu.VMEM((n, nb, points), f32),
            dma((10,)),
            dma((1,)),
            dma((2,)),
            dma((3,)),
            dma((2,)),
            dma((3, n_atom)),
            dma((2, 2, n_atom)),
            dma((n_atom,)),
            dma((2,)),
            dma((2, n_atom)),
            dma((2,)),
            dma((3, n_atom)),
            dma((2, n_atom)),
            dma((2,)),
            dma((3 + layers,)),
            dma((3 + layers,)),
        ],
        compiler_params=pltpu.CompilerParams(
            collective_id=0, has_side_effects=True, vmem_limit_bytes=grant
        ),
        name="exchange_of",
    )(
        *(
            pltpu.with_memory_space_constraint(a, pltpu.HBM)
            for a in (own, piece, names, atoms, weights, scale, shift, mw, aw, head)
        )
    )


QUAD = 4


def fock_kernel(names, basis_t, near, psi, pot, out, pot_out, filled, table, held, done):
    groups, count, depth, points = basis_t.shape
    owned, width, columns = out.shape
    picks = depth // width
    most = groups * count
    tile = min(columns, TILE)
    first = lax.axis_index("grid") * owned
    last = pltpu.make_async_copy(pot, pot_out, done.at[owned])
    last.start()

    @pl.loop(0, owned)
    def _(r):
        filled[r] = 0

    @pl.loop(0, most)
    def _(s):
        k, b = s // count, lax.rem(s, count)
        for j in range(picks):
            block = names[k, j, b] - first

            @pl.when(jnp.logical_and(block >= 0, block < owned))
            def _():
                n = filled[block]
                table[block * most + n] = s * picks + j
                filled[block] = n + 1

    @pl.loop(0, owned)
    def _(r):
        n = filled[r]

        @pl.when(n == 0)
        def _():
            held[r] = jnp.zeros((width, columns), jnp.float32)

        @pl.loop(0, (n + QUAD - 1) // QUAD)
        def _(m):
            parts, values = [], []
            for i in range(QUAD):
                at = m * QUAD + i
                entry = table[r * most + jnp.minimum(at, n - 1)]
                s, j = entry // picks, lax.rem(entry, picks)
                k, b = s // count, lax.rem(s, count)
                taken = jnp.where(at < n, 1.0, 0.0)
                part = basis_t[k, b, pl.ds(pl.multiple_of(j * width, width), width), :]
                parts.append(
                    (part.astype(jnp.float32) * (near[pl.ds(s, 1), :] * taken)).astype(
                        jnp.bfloat16
                    )
                )
                values.append((k, b))
            left = jnp.concatenate(parts, axis=1)
            for c in range(columns // tile):
                at = pl.ds(c * tile, tile)
                right = jnp.concatenate([psi[k, b, :, at] for k, b in values], axis=0)
                value = jnp.dot(left, right, preferred_element_type=jnp.float32)

                @pl.when(m == 0)
                def _():
                    held[r, :, at] = value

                @pl.when(m > 0)
                def _():
                    held[r, :, at] += value

        pltpu.make_async_copy(held.at[r], out.at[r], done.at[r]).start()

    for r in range(owned):
        pltpu.make_async_copy(held.at[r], out.at[r], done.at[r]).wait()
    last.wait()


def fock_of(names, basis_t, near, psi, pot, owned):
    groups, count, depth, points = basis_t.shape
    columns = psi.shape[3]
    width = depth // names.shape[1]
    most = groups * count
    return pl.pallas_call(
        fock_kernel,
        out_shape=(
            jax.ShapeDtypeStruct((owned, width, columns), jnp.float32),
            jax.ShapeDtypeStruct(pot.shape, pot.dtype),
        ),
        in_specs=[pl.BlockSpec(memory_space=pltpu.SMEM), VMEM, VMEM, VMEM, VMEM],
        out_specs=(HBM, HBM),
        scratch_shapes=[
            pltpu.SMEM((owned,), jnp.int32),
            pltpu.SMEM((owned * most,), jnp.int32),
            pltpu.VMEM((owned, width, columns), jnp.float32),
            pltpu.SemaphoreType.DMA((owned + 1,)),
        ],
        compiler_params=pltpu.CompilerParams(
            vmem_limit_bytes=4 * owned * width * columns + (8 << 20)
        ),
        name="fock_of",
    )(names, basis_t, near, psi, pot)


def local(
    basis_values,
    block_lists,
    orbitals,
    point_weights,
    point_atoms,
    embed_scale,
    embed_shift,
    message_weight,
    atom_weight,
    head_weight,
):
    n_grid, n_atom = lax.axis_size("grid"), lax.axis_size("atom")
    own_rows = orbitals.shape[0]
    batches, points, depth = basis_values.shape
    picks = block_lists.shape[1]
    owned = own_rows // (depth // picks)
    potential, near, psi, basis_t, names = exchange_of(
        (n_grid, n_atom),
        orbitals.reshape(owned, own_rows // owned, -1),
        basis_values,
        block_lists.T,
        point_atoms.reshape(batches, points),
        point_weights.reshape(batches, points),
        embed_scale[None, :],
        embed_shift[None, :],
        message_weight,
        atom_weight,
        head_weight[None, :],
    )
    fock, potential = fock_of(names, basis_t, near.reshape(-1, points), psi, potential, owned)
    return (fock.reshape(own_rows, -1), potential.reshape(-1))


def solution(mesh):
    return jax.shard_map(
        local,
        mesh=mesh,
        in_specs=(
            P(("grid", "atom"), None, None),
            P("grid", None),
            P("grid", "atom"),
            P(("grid", "atom")),
            P(("grid", "atom")),
            P(),
            P(),
            P(),
            P(),
            P(),
        ),
        out_specs=(P("grid", "atom"), P(("grid", "atom"))),
        check_vma=False,
    )
```

```python
import functools
import jax
import jax.numpy as jnp
from jax import lax
from jax.experimental import pallas as pl
from jax.experimental.pallas import tpu as pltpu
from jax.sharding import PartitionSpec as P

ATOM_DEV = 32
RUN = max(ATOM_DEV // 4, 1)
LANES = 128
VMEM = pl.BlockSpec(memory_space=pltpu.VMEM)
HBM = pl.BlockSpec(memory_space=pltpu.HBM)
MESH = pl.DeviceIdType.MESH
TILE = 256


def wait_bytes(ref, sem):
    pltpu.make_async_copy(ref, ref, sem).wait()


def meet_all(shape):
    n_grid, n_atom = shape
    n = n_grid * n_atom
    me = lax.axis_index("grid") * n_atom + lax.axis_index("atom")
    barrier = pltpu.get_barrier_semaphore()

    @pl.loop(1, n)
    def _(d):
        t = lax.rem(me + d, n)
        pl.semaphore_signal(
            barrier, inc=1, device_id=(t // n_atom, lax.rem(t, n_atom)), device_id_type=MESH
        )

    pl.semaphore_wait(barrier, n - 1)


def to_columns(rows):
    parts = [
        jnp.transpose(jnp.broadcast_to(rows[i : i + 1, :], (LANES, LANES)))
        for i in range(rows.shape[0])
    ]
    return jnp.concatenate(parts, axis=0)


def to_rows(columns):
    parts = []
    for i in range(columns.shape[0] // LANES):
        piece = jnp.broadcast_to(columns[i * LANES : (i + 1) * LANES, :], (LANES, LANES))
        parts.append(jnp.transpose(piece)[0:1, :])
    return jnp.concatenate(parts, axis=0)


def wrapped(values, total):
    values = jnp.where(values < 0.0, values + total, values)
    return jnp.where(values >= total, values - total, values)


def exchange_kernel(
    shape, layers, own, piece, names, *rest,
):
    given, rest = rest[:7], rest[7:]
    pot, near, psi, basis_t, all_names = rest[:5]
    atoms, weights, scale, shift, mw, aw, head = rest[5:12]
    (
        rows, basis, lists, acc, part_out, part_in, relay, dens, dens_buf,
        info, info_buf, rows_out, rows_buf, scaled_out,
        load, list_sem, name_sent, name_got, v_sent, v_got, z_sent, chip_sent,
        part_sent, part_got, psi_sent, psi_got, passed, relay_sent, sent, got,
    ) = rest[12:]
    n_grid, n_atom = shape
    n = n_grid * n_atom
    grid, atom = lax.axis_index("grid"), lax.axis_index("atom")
    me = grid * n_atom + atom
    last, middle = n_grid - 1, n_grid // 2
    side = lax.rem(grid, 2)
    outer, inner = 2 * side, 2 - 2 * side
    og, ig = grid - 1 + 2 * side, grid + 1 - 2 * side
    has_outer = jnp.logical_and(og >= 0, og < n_grid)
    at_split = jnp.logical_or(grid == middle - 1, grid == middle)
    whole = jnp.logical_and(has_outer, jnp.logical_not(at_split))
    relays = jnp.logical_or(grid == 0, grid == last)
    relay_to = jnp.where(grid == middle, 0, last)
    forward_to = jnp.where(grid == 0, middle - 1, middle)

    nb, points, depth = piece.shape
    owned, width, columns = own.shape
    picks = depth // width
    tile = min(columns, TILE)
    relayed = nb // 2
    direct = nb - relayed

    def remote(source, target, send_sem, recv_sem, to):
        pltpu.make_async_remote_copy(
            src_ref=source,
            dst_ref=target,
            send_sem=send_sem,
            recv_sem=recv_sem,
            device_id=to,
            device_id_type=MESH,
        ).start()

    def to_all(source, held, k):
        @pl.loop(1, n)
        def _(d):
            t = lax.rem(me + d, n)
            remote(
                source, held.at[me], sent.at[k], got.at[k],
                (t // n_atom, lax.rem(t, n_atom)),
            )

    def wait_all(held, sem, count):
        wait_bytes(held.at[pl.ds(0, count)], sem)

    def visit(t):
        reach = jnp.minimum(atom, n_atom - 1 - atom)
        close = jnp.where(lax.rem(t, 2) == 1, atom - (t + 1) // 2, atom + t // 2)
        far = jnp.where(reach == atom, t, n_atom - 1 - t)
        return jnp.where(t <= 2 * reach, close, far)

    held_here = (
        rows.at[pl.ds(1, owned)], basis.at[1, atom], all_names.at[1],
        atoms, weights, scale, shift, mw, aw, head,
    )
    loads = [
        pltpu.make_async_copy(source, target, load.at[i])
        for i, (source, target) in enumerate(zip((own, piece, names, *given), held_here))
    ]
    for copy in loads:
        copy.start()
    meet_all(shape)

    @pl.when(has_outer)
    def _():
        remote(names, all_names.at[inner], name_sent.at[0], name_got.at[inner], (og, atom))
        remote(piece, basis.at[inner, atom], v_sent.at[0], v_got.at[inner, atom], (og, atom))

    remote(names, all_names.at[outer], name_sent.at[1], name_got.at[outer], (ig, atom))
    remote(piece, basis.at[outer, atom], v_sent.at[1], v_got.at[outer, atom], (ig, atom))

    @pl.when(atom < n_atom - 1)
    def _():
        remote(
            piece, basis.at[1, atom], z_sent.at[0, 0, atom], v_got.at[1, atom], (grid, atom + 1)
        )

    @pl.when(atom > 0)
    def _():
        remote(
            piece, basis.at[1, atom], z_sent.at[0, 1, atom], v_got.at[1, atom], (grid, atom - 1)
        )

    for copy in loads[1:5]:
        copy.wait()
    total = float(ATOM_DEV * n_atom)
    named = atoms[...].astype(jnp.float32)
    lead = named[0:1, 0:1]
    shifted = wrapped(named - lead + total / 2, total) - total / 2
    least = jnp.min(jnp.min(shifted, axis=1, keepdims=True), axis=0, keepdims=True)
    start = wrapped(lead + least, total)
    place = shifted - least
    lane = lax.broadcasted_iota(jnp.int32, (1, LANES), 1)
    mine = jnp.where(lane < RUN, wrapped(start + lane.astype(jnp.float32), total), -1.0)
    run = lax.broadcasted_iota(jnp.int32, (RUN, LANES), 0).astype(jnp.float32)
    mass = jnp.zeros((RUN, 1), jnp.float32)
    for i in range(nb):
        here = jnp.where(place[i : i + 1, :] == run, weights[i : i + 1, :], 0.0)
        mass = mass + jnp.sum(here, axis=1, keepdims=True)
    info[...] = jnp.where(
        lax.broadcasted_iota(jnp.int32, (RUN, LANES), 1) < LANES // 2,
        wrapped(start + run, total),
        mass,
    )
    to_all(info, info_buf, 1)
    info_buf[me] = info[...]

    for edge in (0, owned + 1):
        rows[edge] = jnp.zeros((width, columns), rows.dtype)

    @pl.when(jnp.logical_not(has_outer))
    def _():
        all_names[outer] = jnp.full(names.shape, -1, names.dtype)
        part_in[0] = jnp.zeros(part_in.shape[1:], part_in.dtype)

    @pl.when(has_outer)
    def _():
        wait_bytes(names, name_got.at[outer])

    wait_bytes(names, name_got.at[inner])
    copy = pltpu.make_async_copy(all_names, lists, list_sem.at[0])
    copy.start()
    copy.wait()
    loads[0].wait()
    first = grid * owned

    def product(slot, q, i, keep):
        chosen = []
        for j in range(picks):
            block = lists[slot, j, q * nb + i] - first + 1
            chosen.append(jnp.minimum(jnp.maximum(block, 0), owned + 1))
        values = basis[slot, q, i]
        for c in range(columns // tile):
            at = pl.ds(c * tile, tile)
            held = jnp.concatenate(
                [rows[k, :, at] for k in chosen], axis=0
            )
            keep(at, jnp.dot(values, held, preferred_element_type=jnp.float32))

    def outward(phase, q, i, source, target, sent_sem, got_sem, near_by=True, far=True):
        if near_by:

            @pl.when(whole if i >= direct else has_outer)
            def _():
                remote(source, target, sent_sem, got_sem, (og, atom))

        if far and i >= direct:

            @pl.when(at_split)
            def _():
                remote(
                    source, relay.at[phase, q, i - direct], sent_sem, passed.at[phase, q],
                    (relay_to, atom),
                )

    def forward(phase, r):
        q = visit(r)

        @pl.when(relays)
        def _():
            held = relay.at[phase, q]
            wait_bytes(held, passed.at[phase, q])
            at = pl.ds(q * nb + direct, relayed)
            if phase == 0:
                target, got_sem = part_in.at[0, at], part_got.at[0, q]
            else:
                target, got_sem = psi.at[inner, at], psi_got.at[inner, q]
            remote(held, target, relay_sent.at[phase], got_sem, (forward_to, atom))

    def finish(q):
        wait_bytes(part_in.at[1, pl.ds(q * nb, nb)], part_got.at[1, q])

        @pl.when(has_outer)
        def _():
            wait_bytes(part_in.at[0, pl.ds(q * nb, nb)], part_got.at[0, q])

        for i in range(nb):
            b = q * nb + i
            sums = jnp.zeros((points, LANES), jnp.float32)
            for c in range(columns // LANES):
                at = pl.ds(c * LANES, LANES)
                value = (
                    acc[b, :, at]
                    + part_in[0, b, :, at].astype(jnp.float32)
                    + part_in[1, b, :, at].astype(jnp.float32)
                )
                rounded = value.astype(jnp.bfloat16)
                psi[1, b, :, at] = rounded
                sums = sums + jnp.square(rounded.astype(jnp.float32))
            dens[q, i : i + 1, :] = jnp.sum(jnp.transpose(sums), axis=0, keepdims=True)

        @pl.when(q != atom)
        def _():
            remote(dens.at[q], dens_buf.at[atom], sent.at[0], got.at[0], (grid, q))

        at = pl.ds(q * nb, nb)
        remote(psi.at[1, at], psi.at[outer, at], psi_sent.at[1], psi_got.at[outer, q], (ig, atom))
        psi_outward(q, near_by=False)

    def psi_outward(q, **which):
        for i in range(nb):
            b = q * nb + i
            outward(
                1, q, i, psi.at[1, b], psi.at[inner, b], psi_sent.at[0], psi_got.at[inner, q],
                **which,
            )

    def psi_round(r):
        psi_outward(visit(r), far=False)
        forward(1, r)

    reach = jnp.minimum(atom, n_atom - 1 - atom)

    def along(stream, slot, q):
        for way in range(2):
            able = (
                jnp.logical_and(q <= atom, atom < n_atom - 1)
                if way == 0
                else jnp.logical_and(q >= atom, atom > 0)
            )

            @pl.when(able)
            def _():
                remote(
                    basis.at[slot, q], basis.at[slot, q], z_sent.at[stream, way, q],
                    v_got.at[slot, q], (grid, atom + 1 - 2 * way),
                )

    def spread_outer(t):
        q = visit(t)

        @pl.when(has_outer)
        def _():
            wait_bytes(basis.at[outer, q], v_got.at[outer, q])
            along(1, outer, q)

    def spread_own(t):
        q = visit(t)
        wait_bytes(basis.at[1, q], v_got.at[1, q])
        along(0, 1, q)
        remote(
            basis.at[1, q], basis.at[outer, q], chip_sent.at[q], v_got.at[outer, q], (ig, atom)
        )

    def product_outer(q):
        @pl.when(has_outer)
        def _():
            for i in range(nb):
                b = q * nb + i

                def keep(at, value):
                    part_out[0, b, :, at] = value.astype(jnp.bfloat16)

                product(outer, q, i, keep)
                outward(
                    0, q, i, part_out.at[0, b], part_in.at[0, b], part_sent.at[0],
                    part_got.at[0, q],
                )

    def products_here(q):
        wait_bytes(basis.at[inner, q], v_got.at[inner, q])
        for i in range(nb):
            b = q * nb + i

            def keep(at, value):
                part_out[1, b, :, at] = value.astype(jnp.bfloat16)

            product(inner, q, i, keep)
            remote(
                part_out.at[1, b], part_in.at[1, b], part_sent.at[1], part_got.at[1, q],
                (ig, atom),
            )

        for i in range(nb):
            b = q * nb + i

            def keep(at, value):
                acc[b, :, at] = value

            product(1, q, i, keep)
            for slot in range(3):
                basis_t[slot, b] = jnp.transpose(basis[slot, q, i])

    spread_outer(0)

    @pl.loop(0, n_atom)
    def _(t):
        q = visit(t)
        paired = jnp.logical_and(lax.rem(t, 2) == 1, t < 2 * reach)
        fresh = jnp.logical_and(
            t > 0, jnp.logical_or(lax.rem(t, 2) == 1, t > 2 * reach)
        )

        @pl.when(fresh)
        def _():
            spread_outer(t)

        @pl.when(paired)
        def _():
            spread_outer(t + 1)

        product_outer(q)

        @pl.when(t > 0)
        def _():
            products_here(visit(t - 1))

        @pl.when(fresh)
        def _():
            spread_own(t)

        @pl.when(paired)
        def _():
            spread_own(t + 1)

        @pl.when(t >= 1)
        def _():
            forward(0, t - 1)

        @pl.when(t >= 2)
        def _():
            finish(visit(t - 2))

    stops = layers + 2

    def rounds(s, act):
        for r in range(n_atom):
            if r * stops // n_atom == s:
                act(r)

    rounds(0, psi_round)
    products_here(visit(n_atom - 1))
    finish(visit(n_atom - 2))
    weight = to_columns(weights[...])[:, 0:1]
    spot = to_columns(place)
    hot = (spot == lax.broadcasted_iota(jnp.int32, spot.shape, 1).astype(jnp.float32)).astype(
        jnp.bfloat16
    )
    deep = lax.broadcasted_iota(jnp.int32, (LANES, LANES), 0).astype(jnp.float32)
    hot_t = jnp.concatenate([place[i : i + 1, :] == deep for i in range(nb)], axis=1).astype(
        jnp.bfloat16
    )
    for copy in loads[5:]:
        copy.wait()
    halves = scale.shape[1] // LANES
    wait_all(info_buf, got.at[1], n - 1)
    facts = info_buf[...].reshape(n * RUN, LANES)
    same = (facts[:, 0:1] == mine).astype(jnp.float32)
    mass = jnp.sum(same * facts[:, LANES // 2 : LANES // 2 + 1], axis=0, keepdims=True)
    share = 1.0 / (1.0 + to_columns(mass)[:, 0:1])
    same = same.reshape(n, RUN, LANES)
    none = jnp.zeros_like(same)
    selects = []
    for h in range(halves):
        full = jnp.concatenate(
            [same if k == h else none for k in range(halves)], axis=1
        ).reshape(n * RUN * halves, LANES)
        selects.append(jnp.transpose(full).astype(jnp.bfloat16))

    forward(0, n_atom - 1)
    finish(visit(n_atom - 1))
    dens_buf[atom] = dens[atom]

    wait_all(dens_buf, got.at[0], n_atom - 1)
    density = to_columns(2.0 * jnp.sum(dens_buf[...], axis=0))
    safe = jnp.where(density > 0.0, density, 1.0)
    radius = jnp.where(density > 0.0, jnp.exp(jnp.log(safe) * (1.0 / 3.0)), 0.0)[:, 0:1]
    hidden = jax.nn.silu(radius * scale[...] + shift[...])
    for layer in range(layers):
        message = jax.nn.silu(
            jnp.dot(hidden.astype(jnp.bfloat16), mw[layer], preferred_element_type=jnp.float32)
        )
        weighted = (weight * message).astype(jnp.bfloat16)
        part = jnp.dot(hot_t, weighted, preferred_element_type=jnp.float32)
        rows_out[layer] = jnp.concatenate(
            [part[0:RUN, h * LANES : (h + 1) * LANES] for h in range(halves)], axis=0
        ).astype(jnp.bfloat16)
        to_all(rows_out.at[layer], rows_buf.at[layer], 2 + layer)
        rounds(1 + layer, psi_round)
        rows_buf[layer, me] = rows_out[layer]
        wait_all(rows_buf.at[layer], got.at[2 + layer], n - 1)
        held = rows_buf[layer].reshape(n * RUN * halves, LANES)
        summed = jnp.concatenate(
            [jnp.dot(pick, held, preferred_element_type=jnp.float32) for pick in selects], axis=1
        )
        update = jax.nn.silu(
            jnp.dot(
                (summed * share).astype(jnp.bfloat16), aw[layer],
                preferred_element_type=jnp.float32,
            )
        ).astype(jnp.bfloat16)
        picked = jnp.dot(hot, update, preferred_element_type=jnp.float32)
        hidden = hidden + message * picked
    score = jnp.sum(hidden * head[...], axis=1, keepdims=True)
    potential = radius * (1.0 + jnp.tanh(score))
    pot[...] = to_rows(potential)
    final = 2 + layers
    scaled_out[...] = to_rows(weight * potential)

    @pl.loop(1, n_atom)
    def _(d):
        remote(
            scaled_out, near.at[n_atom + atom], sent.at[final], got.at[final],
            (grid, lax.rem(atom + d, n_atom)),
        )

    @pl.when(has_outer)
    def _():
        @pl.loop(0, n_atom)
        def _(d):
            remote(
                scaled_out, near.at[inner * n_atom + atom], sent.at[final + 1],
                got.at[final + 1 + side], (og, d),
            )

    @pl.loop(0, n_atom)
    def _(d):
        remote(
            scaled_out, near.at[outer * n_atom + atom], sent.at[final + 2],
            got.at[final + 2 - side], (ig, d),
        )

    rounds(layers + 1, psi_round)
    near[n_atom + atom] = scaled_out[...]
    wait_all(near, got.at[final], n_atom - 1)

    @pl.when(has_outer)
    def _():
        wait_all(near, got.at[final + 2 - side], n_atom)

    wait_all(near, got.at[final + 1 + side], n_atom)

    @pl.loop(0, n_atom)
    def _(q):
        at = pl.ds(q * nb, nb)
        wait_bytes(psi.at[inner, at], psi_got.at[inner, q])

        @pl.when(has_outer)
        def _():
            wait_bytes(psi.at[outer, at], psi_got.at[outer, q])

        @pl.when(q != atom)
        def _():
            wait_bytes(basis.at[1, q], chip_sent.at[q])

        for way in range(2):
            able = (
                jnp.logical_and(q <= atom, atom < n_atom - 1)
                if way == 0
                else jnp.logical_and(q >= atom, atom > 0)
            )

            @pl.when(able)
            def _():
                wait_bytes(basis.at[1, q], z_sent.at[0, way, q])

            @pl.when(jnp.logical_and(able, has_outer))
            def _():
                wait_bytes(basis.at[1, q], z_sent.at[1, way, q])

    @pl.when(has_outer)
    def _():
        wait_bytes(names, name_sent.at[0])
        wait_bytes(piece, v_sent.at[0])
        wait_bytes(part_out.at[0], part_sent.at[0])
        wait_bytes(psi.at[1], psi_sent.at[0])

    wait_bytes(names, name_sent.at[1])
    wait_bytes(piece, v_sent.at[1])
    wait_bytes(part_out.at[1], part_sent.at[1])
    wait_bytes(psi.at[1], psi_sent.at[1])

    @pl.when(relays)
    def _():
        for phase in range(2):
            wait_bytes(relay.at[phase], relay_sent.at[phase])

    wait_all(dens_buf, sent.at[0], n_atom - 1)
    wait_all(info_buf, sent.at[1], n - 1)
    for layer in range(layers):
        wait_all(rows_buf.at[layer], sent.at[2 + layer], n - 1)
    wait_all(near, sent.at[final], n_atom - 1)
    wait_all(near, sent.at[final + 2], n_atom)

    @pl.when(has_outer)
    def _():
        wait_all(near, sent.at[final + 1], n_atom)


def exchange_of(shape, own, piece, names, atoms, weights, scale, shift, mw, aw, head):
    n_grid, n_atom = shape
    n = n_grid * n_atom
    nb, points, depth = piece.shape
    count = nb * n_atom
    width, columns = own.shape[1:]
    layers, features, _ = mw.shape
    packed = RUN * (features // LANES)
    bf16, f32 = jnp.bfloat16, jnp.float32
    dma = pltpu.SemaphoreType.DMA
    grant = 2 * own.size + 14 * count * points * columns + 6 * count * depth * points
    grant += n * (packed * LANES * (2 * layers + 8) + 12 * RUN * LANES) + (6 << 20)
    given = 6 * count * points * (columns + depth)
    if grant + given > 48 << 20:
        grant = 60 << 20
    return pl.pallas_call(
        functools.partial(exchange_kernel, shape, layers),
        out_shape=(
            jax.ShapeDtypeStruct((nb, points), f32),
            jax.ShapeDtypeStruct((3 * n_atom, nb, points), f32),
            jax.ShapeDtypeStruct((3, count, points, columns), bf16),
            jax.ShapeDtypeStruct((3, count, depth, points), bf16),
            jax.ShapeDtypeStruct((3, *names.shape), names.dtype),
        ),
        in_specs=[HBM] * 10,
        out_specs=(VMEM,) * 5,
        scratch_shapes=[
            pltpu.VMEM(a.shape, a.dtype) for a in (atoms, weights, scale, shift, mw, aw, head)
        ]
        + [
            pltpu.VMEM((own.shape[0] + 2, width, columns), bf16),
            pltpu.VMEM((3, n_atom, nb, points, depth), bf16),
            pltpu.SMEM((3, *names.shape), names.dtype),
            pltpu.VMEM((count, points, columns), f32),
            pltpu.VMEM((2, count, points, columns), bf16),
            pltpu.VMEM((2, count, points, columns), bf16),
            pltpu.VMEM((2, n_atom, nb // 2, points, columns), bf16),
            pltpu.VMEM((n_atom, nb, points), f32),
            pltpu.VMEM((n_atom, nb, points), f32),
            pltpu.VMEM((RUN, LANES), f32),
            pltpu.VMEM((n, RUN, LANES), f32),
            pltpu.VMEM((layers, packed, LANES), bf16),
            pltpu.VMEM((layers, n, packed, LANES), bf16),
            pltpu.VMEM((nb, points), f32),
            dma((10,)),
            dma((1,)),
            dma((2,)),
            dma((3,)),
            dma((2,)),
            dma((3, n_atom)),
            dma((2, 2, n_atom)),
            dma((n_atom,)),
            dma((2,)),
            dma((2, n_atom)),
            dma((2,)),
            dma((3, n_atom)),
            dma((2, n_atom)),
            dma((2,)),
            dma((5 + layers,)),
            dma((5 + layers,)),
        ],
        compiler_params=pltpu.CompilerParams(
            collective_id=0, has_side_effects=True, vmem_limit_bytes=grant
        ),
        name="exchange_of",
    )(
        *(
            pltpu.with_memory_space_constraint(a, pltpu.HBM)
            for a in (own, piece, names, atoms, weights, scale, shift, mw, aw, head)
        )
    )


QUAD = 4


def fock_kernel(names, basis_t, near, psi, pot, out, pot_out, filled, table, held, done):
    groups, count, depth, points = basis_t.shape
    owned, width, columns = out.shape
    picks = depth // width
    most = groups * count
    tile = min(columns, TILE)
    first = lax.axis_index("grid") * owned
    last = pltpu.make_async_copy(pot, pot_out, done.at[owned])
    last.start()

    @pl.loop(0, owned)
    def _(r):
        filled[r] = 0

    @pl.loop(0, most)
    def _(s):
        k, b = s // count, lax.rem(s, count)
        for j in range(picks):
            block = names[k, j, b] - first

            @pl.when(jnp.logical_and(block >= 0, block < owned))
            def _():
                n = filled[block]
                table[block * most + n] = s * picks + j
                filled[block] = n + 1

    @pl.loop(0, owned)
    def _(r):
        n = filled[r]

        @pl.when(n == 0)
        def _():
            held[r] = jnp.zeros((width, columns), jnp.float32)

        @pl.loop(0, (n + QUAD - 1) // QUAD)
        def _(m):
            parts, values = [], []
            for i in range(QUAD):
                at = m * QUAD + i
                entry = table[r * most + jnp.minimum(at, n - 1)]
                s, j = entry // picks, lax.rem(entry, picks)
                k, b = s // count, lax.rem(s, count)
                taken = jnp.where(at < n, 1.0, 0.0)
                part = basis_t[k, b, pl.ds(pl.multiple_of(j * width, width), width), :]
                parts.append(
                    (part.astype(jnp.float32) * (near[pl.ds(s, 1), :] * taken)).astype(
                        jnp.bfloat16
                    )
                )
                values.append((k, b))
            left = jnp.concatenate(parts, axis=1)
            for c in range(columns // tile):
                at = pl.ds(c * tile, tile)
                right = jnp.concatenate([psi[k, b, :, at] for k, b in values], axis=0)
                value = jnp.dot(left, right, preferred_element_type=jnp.float32)

                @pl.when(m == 0)
                def _():
                    held[r, :, at] = value

                @pl.when(m > 0)
                def _():
                    held[r, :, at] += value

        pltpu.make_async_copy(held.at[r], out.at[r], done.at[r]).start()

    for r in range(owned):
        pltpu.make_async_copy(held.at[r], out.at[r], done.at[r]).wait()
    last.wait()


def fock_of(names, basis_t, near, psi, pot, owned):
    groups, count, depth, points = basis_t.shape
    columns = psi.shape[3]
    width = depth // names.shape[1]
    most = groups * count
    return pl.pallas_call(
        fock_kernel,
        out_shape=(
            jax.ShapeDtypeStruct((owned, width, columns), jnp.float32),
            jax.ShapeDtypeStruct(pot.shape, pot.dtype),
        ),
        in_specs=[pl.BlockSpec(memory_space=pltpu.SMEM), VMEM, VMEM, VMEM, VMEM],
        out_specs=(HBM, HBM),
        scratch_shapes=[
            pltpu.SMEM((owned,), jnp.int32),
            pltpu.SMEM((owned * most,), jnp.int32),
            pltpu.VMEM((owned, width, columns), jnp.float32),
            pltpu.SemaphoreType.DMA((owned + 1,)),
        ],
        compiler_params=pltpu.CompilerParams(
            vmem_limit_bytes=4 * owned * width * columns + (8 << 20)
        ),
        name="fock_of",
    )(names, basis_t, near, psi, pot)


def local(
    basis_values,
    block_lists,
    orbitals,
    point_weights,
    point_atoms,
    embed_scale,
    embed_shift,
    message_weight,
    atom_weight,
    head_weight,
):
    n_grid, n_atom = lax.axis_size("grid"), lax.axis_size("atom")
    own_rows = orbitals.shape[0]
    batches, points, depth = basis_values.shape
    picks = block_lists.shape[1]
    owned = own_rows // (depth // picks)
    potential, near, psi, basis_t, names = exchange_of(
        (n_grid, n_atom),
        orbitals.reshape(owned, own_rows // owned, -1),
        basis_values,
        block_lists.T,
        point_atoms.reshape(batches, points),
        point_weights.reshape(batches, points),
        embed_scale[None, :],
        embed_shift[None, :],
        message_weight,
        atom_weight,
        head_weight[None, :],
    )
    fock, potential = fock_of(names, basis_t, near.reshape(-1, points), psi, potential, owned)
    return (fock.reshape(own_rows, -1), potential.reshape(-1))


def solution(mesh):
    return jax.shard_map(
        local,
        mesh=mesh,
        in_specs=(
            P(("grid", "atom"), None, None),
            P("grid", None),
            P("grid", "atom"),
            P(("grid", "atom")),
            P(("grid", "atom")),
            P(),
            P(),
            P(),
            P(),
            P(),
        ),
        out_specs=(P("grid", "atom"), P(("grid", "atom"))),
        check_vma=False,
    )
```

```python
import functools
import jax
import jax.numpy as jnp
from jax import lax
from jax.experimental import pallas as pl
from jax.experimental.pallas import tpu as pltpu
from jax.sharding import PartitionSpec as P

ATOM_DEV = 32
RUN = max(ATOM_DEV // 4, 1)
LANES = 128
VMEM = pl.BlockSpec(memory_space=pltpu.VMEM)
HBM = pl.BlockSpec(memory_space=pltpu.HBM)
MESH = pl.DeviceIdType.MESH
TILE = 256


def wait_bytes(ref, sem):
    pltpu.make_async_copy(ref, ref, sem).wait()


def meet_all(shape):
    n_grid, n_atom = shape
    n = n_grid * n_atom
    me = lax.axis_index("grid") * n_atom + lax.axis_index("atom")
    barrier = pltpu.get_barrier_semaphore()

    @pl.loop(1, n)
    def _(d):
        t = lax.rem(me + d, n)
        pl.semaphore_signal(
            barrier, inc=1, device_id=(t // n_atom, lax.rem(t, n_atom)), device_id_type=MESH
        )

    pl.semaphore_wait(barrier, n - 1)


def to_columns(rows):
    parts = [
        jnp.transpose(jnp.broadcast_to(rows[i : i + 1, :], (LANES, LANES)))
        for i in range(rows.shape[0])
    ]
    return jnp.concatenate(parts, axis=0)


def to_rows(columns):
    parts = []
    for i in range(columns.shape[0] // LANES):
        piece = jnp.broadcast_to(columns[i * LANES : (i + 1) * LANES, :], (LANES, LANES))
        parts.append(jnp.transpose(piece)[0:1, :])
    return jnp.concatenate(parts, axis=0)


def wrapped(values, total):
    values = jnp.where(values < 0.0, values + total, values)
    return jnp.where(values >= total, values - total, values)


def exchange_kernel(
    shape, layers, own, piece, names, *rest,
):
    given, rest = rest[:7], rest[7:]
    pot, near, psi, basis_t, all_names = rest[:5]
    atoms, weights, scale, shift, mw, aw, head = rest[5:12]
    (
        rows, basis, lists, acc, part_out, part_in, relay, dens, dens_buf,
        info, info_buf, rows_out, rows_buf, scaled_out,
        load, list_sem, name_sent, name_got, v_sent, v_got, z_sent, chip_sent,
        part_sent, part_got, psi_sent, psi_got, passed, relay_sent, sent, got,
    ) = rest[12:]
    n_grid, n_atom = shape
    n = n_grid * n_atom
    grid, atom = lax.axis_index("grid"), lax.axis_index("atom")
    me = grid * n_atom + atom
    last, middle = n_grid - 1, n_grid // 2
    side = lax.rem(grid, 2)
    outer, inner = 2 * side, 2 - 2 * side
    og, ig = grid - 1 + 2 * side, grid + 1 - 2 * side
    has_outer = jnp.logical_and(og >= 0, og < n_grid)
    at_split = jnp.logical_or(grid == middle - 1, grid == middle)
    whole = jnp.logical_and(has_outer, jnp.logical_not(at_split))
    relays = jnp.logical_or(grid == 0, grid == last)
    relay_to = jnp.where(grid == middle, 0, last)
    forward_to = jnp.where(grid == 0, middle - 1, middle)

    nb, points, depth = piece.shape
    owned, width, columns = own.shape
    picks = depth // width
    tile = min(columns, TILE)
    relayed = nb // 2
    direct = nb - relayed

    def remote(source, target, send_sem, recv_sem, to):
        pltpu.make_async_remote_copy(
            src_ref=source,
            dst_ref=target,
            send_sem=send_sem,
            recv_sem=recv_sem,
            device_id=to,
            device_id_type=MESH,
        ).start()

    def to_all(source, held, k):
        @pl.loop(1, n)
        def _(d):
            t = lax.rem(me + d, n)
            remote(
                source, held.at[me], sent.at[k], got.at[k],
                (t // n_atom, lax.rem(t, n_atom)),
            )

    def wait_all(held, sem, count):
        wait_bytes(held.at[pl.ds(0, count)], sem)

    def visit(t):
        reach = jnp.minimum(atom, n_atom - 1 - atom)
        close = jnp.where(lax.rem(t, 2) == 1, atom - (t + 1) // 2, atom + t // 2)
        far = jnp.where(reach == atom, t, n_atom - 1 - t)
        return jnp.where(t <= 2 * reach, close, far)

    held_here = (
        rows.at[pl.ds(1, owned)], basis.at[1, atom], all_names.at[1],
        atoms, weights, scale, shift, mw, aw, head,
    )
    loads = [
        pltpu.make_async_copy(source, target, load.at[i])
        for i, (source, target) in enumerate(zip((own, piece, names, *given), held_here))
    ]
    for copy in loads:
        copy.start()
    meet_all(shape)

    @pl.when(has_outer)
    def _():
        remote(names, all_names.at[inner], name_sent.at[0], name_got.at[inner], (og, atom))
        remote(piece, basis.at[inner, atom], v_sent.at[0], v_got.at[inner, atom], (og, atom))

    remote(names, all_names.at[outer], name_sent.at[1], name_got.at[outer], (ig, atom))
    remote(piece, basis.at[outer, atom], v_sent.at[1], v_got.at[outer, atom], (ig, atom))

    @pl.when(atom < n_atom - 1)
    def _():
        remote(
            piece, basis.at[1, atom], z_sent.at[0, 0, atom], v_got.at[1, atom], (grid, atom + 1)
        )

    @pl.when(atom > 0)
    def _():
        remote(
            piece, basis.at[1, atom], z_sent.at[0, 1, atom], v_got.at[1, atom], (grid, atom - 1)
        )

    for copy in loads[1:5]:
        copy.wait()
    total = float(ATOM_DEV * n_atom)
    named = atoms[...].astype(jnp.float32)
    lead = named[0:1, 0:1]
    shifted = wrapped(named - lead + total / 2, total) - total / 2
    least = jnp.min(jnp.min(shifted, axis=1, keepdims=True), axis=0, keepdims=True)
    start = wrapped(lead + least, total)
    place = shifted - least
    lane = lax.broadcasted_iota(jnp.int32, (1, LANES), 1)
    mine = jnp.where(lane < RUN, wrapped(start + lane.astype(jnp.float32), total), -1.0)
    run = lax.broadcasted_iota(jnp.int32, (RUN, LANES), 0).astype(jnp.float32)
    mass = jnp.zeros((RUN, 1), jnp.float32)
    for i in range(nb):
        here = jnp.where(place[i : i + 1, :] == run, weights[i : i + 1, :], 0.0)
        mass = mass + jnp.sum(here, axis=1, keepdims=True)
    info[...] = jnp.where(
        lax.broadcasted_iota(jnp.int32, (RUN, LANES), 1) < LANES // 2,
        wrapped(start + run, total),
        mass,
    )
    to_all(info, info_buf, 1)
    info_buf[me] = info[...]

    for edge in (0, owned + 1):
        rows[edge] = jnp.zeros((width, columns), rows.dtype)

    @pl.when(jnp.logical_not(has_outer))
    def _():
        all_names[outer] = jnp.full(names.shape, -1, names.dtype)
        part_in[0] = jnp.zeros(part_in.shape[1:], part_in.dtype)

    @pl.when(has_outer)
    def _():
        wait_bytes(names, name_got.at[outer])

    wait_bytes(names, name_got.at[inner])
    copy = pltpu.make_async_copy(all_names, lists, list_sem.at[0])
    copy.start()
    copy.wait()
    loads[0].wait()
    first = grid * owned

    def product(slot, q, i, keep):
        chosen = []
        for j in range(picks):
            block = lists[slot, j, q * nb + i] - first + 1
            chosen.append(jnp.minimum(jnp.maximum(block, 0), owned + 1))
        values = basis[slot, q, i]
        for c in range(columns // tile):
            at = pl.ds(c * tile, tile)
            held = jnp.concatenate(
                [rows[k, :, at] for k in chosen], axis=0
            )
            keep(at, jnp.dot(values, held, preferred_element_type=jnp.float32))

    def outward(phase, q, i, source, target, sent_sem, got_sem, near_by=True, far=True):
        if near_by:

            @pl.when(whole if i >= direct else has_outer)
            def _():
                remote(source, target, sent_sem, got_sem, (og, atom))

        if far and i >= direct:

            @pl.when(at_split)
            def _():
                remote(
                    source, relay.at[phase, q, i - direct], sent_sem, passed.at[phase, q],
                    (relay_to, atom),
                )

    def forward(phase, r):
        q = visit(r)

        @pl.when(relays)
        def _():
            held = relay.at[phase, q]
            wait_bytes(held, passed.at[phase, q])
            at = pl.ds(q * nb + direct, relayed)
            if phase == 0:
                target, got_sem = part_in.at[0, at], part_got.at[0, q]
            else:
                target, got_sem = psi.at[inner, at], psi_got.at[inner, q]
            remote(held, target, relay_sent.at[phase], got_sem, (forward_to, atom))

    def finish(q):
        wait_bytes(part_in.at[1, pl.ds(q * nb, nb)], part_got.at[1, q])

        @pl.when(has_outer)
        def _():
            wait_bytes(part_in.at[0, pl.ds(q * nb, nb)], part_got.at[0, q])

        for i in range(nb):
            b = q * nb + i
            sums = jnp.zeros((points, LANES), jnp.float32)
            for c in range(columns // LANES):
                at = pl.ds(c * LANES, LANES)
                value = (
                    acc[b, :, at]
                    + part_in[0, b, :, at].astype(jnp.float32)
                    + part_in[1, b, :, at].astype(jnp.float32)
                )
                rounded = value.astype(jnp.bfloat16)
                psi[1, b, :, at] = rounded
                sums = sums + jnp.square(rounded.astype(jnp.float32))
            dens[q, i : i + 1, :] = jnp.sum(jnp.transpose(sums), axis=0, keepdims=True)

        @pl.when(q != atom)
        def _():
            remote(dens.at[q], dens_buf.at[atom], sent.at[0], got.at[0], (grid, q))

        at = pl.ds(q * nb, nb)
        remote(psi.at[1, at], psi.at[outer, at], psi_sent.at[1], psi_got.at[outer, q], (ig, atom))
        psi_outward(q, near_by=False)

    def psi_outward(q, **which):
        for i in range(nb):
            b = q * nb + i
            outward(
                1, q, i, psi.at[1, b], psi.at[inner, b], psi_sent.at[0], psi_got.at[inner, q],
                **which,
            )

    def psi_round(r):
        psi_outward(visit(r), far=False)
        forward(1, r)

    reach = jnp.minimum(atom, n_atom - 1 - atom)

    def along(stream, slot, q):
        for way in range(2):
            able = (
                jnp.logical_and(q <= atom, atom < n_atom - 1)
                if way == 0
                else jnp.logical_and(q >= atom, atom > 0)
            )

            @pl.when(able)
            def _():
                remote(
                    basis.at[slot, q], basis.at[slot, q], z_sent.at[stream, way, q],
                    v_got.at[slot, q], (grid, atom + 1 - 2 * way),
                )

    def spread_outer(t):
        q = visit(t)

        @pl.when(has_outer)
        def _():
            wait_bytes(basis.at[outer, q], v_got.at[outer, q])
            along(1, outer, q)

    def spread_own(t):
        q = visit(t)
        wait_bytes(basis.at[1, q], v_got.at[1, q])
        along(0, 1, q)
        remote(
            basis.at[1, q], basis.at[outer, q], chip_sent.at[q], v_got.at[outer, q], (ig, atom)
        )

    def product_outer(q):
        @pl.when(has_outer)
        def _():
            for i in range(nb):
                b = q * nb + i

                def keep(at, value):
                    part_out[0, b, :, at] = value.astype(jnp.bfloat16)

                product(outer, q, i, keep)
                outward(
                    0, q, i, part_out.at[0, b], part_in.at[0, b], part_sent.at[0],
                    part_got.at[0, q],
                )

    def products_here(q):
        wait_bytes(basis.at[inner, q], v_got.at[inner, q])
        for i in range(nb):
            b = q * nb + i

            def keep(at, value):
                part_out[1, b, :, at] = value.astype(jnp.bfloat16)

            product(inner, q, i, keep)
            remote(
                part_out.at[1, b], part_in.at[1, b], part_sent.at[1], part_got.at[1, q],
                (ig, atom),
            )

        for i in range(nb):
            b = q * nb + i

            def keep(at, value):
                acc[b, :, at] = value

            product(1, q, i, keep)
            for slot in range(3):
                basis_t[slot, b] = jnp.transpose(basis[slot, q, i])

    spread_outer(0)

    @pl.loop(0, n_atom)
    def _(t):
        q = visit(t)
        paired = jnp.logical_and(lax.rem(t, 2) == 1, t < 2 * reach)
        fresh = jnp.logical_and(
            t > 0, jnp.logical_or(lax.rem(t, 2) == 1, t > 2 * reach)
        )

        @pl.when(fresh)
        def _():
            spread_outer(t)

        @pl.when(paired)
        def _():
            spread_outer(t + 1)

        product_outer(q)

        @pl.when(t > 0)
        def _():
            products_here(visit(t - 1))

        @pl.when(fresh)
        def _():
            spread_own(t)

        @pl.when(paired)
        def _():
            spread_own(t + 1)

        @pl.when(t >= 1)
        def _():
            forward(0, t - 1)

        @pl.when(t >= 2)
        def _():
            finish(visit(t - 2))

    stops = layers + 2

    def rounds(s, act):
        for r in range(n_atom):
            if r * stops // n_atom == s:
                act(r)

    rounds(0, psi_round)
    products_here(visit(n_atom - 1))
    finish(visit(n_atom - 2))
    weight = to_columns(weights[...])[:, 0:1]
    spot = to_columns(place)
    hot = (spot == lax.broadcasted_iota(jnp.int32, spot.shape, 1).astype(jnp.float32)).astype(
        jnp.bfloat16
    )
    deep = lax.broadcasted_iota(jnp.int32, (LANES, LANES), 0).astype(jnp.float32)
    hot_t = jnp.concatenate([place[i : i + 1, :] == deep for i in range(nb)], axis=1).astype(
        jnp.bfloat16
    )
    for copy in loads[5:]:
        copy.wait()
    halves = scale.shape[1] // LANES
    wait_all(info_buf, got.at[1], n - 1)
    facts = info_buf[...].reshape(n * RUN, LANES)
    same = (facts[:, 0:1] == mine).astype(jnp.float32)
    mass = jnp.sum(same * facts[:, LANES // 2 : LANES // 2 + 1], axis=0, keepdims=True)
    share = 1.0 / (1.0 + to_columns(mass)[:, 0:1])
    same = same.reshape(n, RUN, LANES)
    none = jnp.zeros_like(same)
    selects = []
    for h in range(halves):
        full = jnp.concatenate(
            [same if k == h else none for k in range(halves)], axis=1
        ).reshape(n * RUN * halves, LANES)
        selects.append(jnp.transpose(full).astype(jnp.bfloat16))

    forward(0, n_atom - 1)
    finish(visit(n_atom - 1))
    dens_buf[atom] = dens[atom]

    wait_all(dens_buf, got.at[0], n_atom - 1)
    density = to_columns(2.0 * jnp.sum(dens_buf[...], axis=0))
    safe = jnp.where(density > 0.0, density, 1.0)
    radius = jnp.where(density > 0.0, jnp.exp(jnp.log(safe) * (1.0 / 3.0)), 0.0)[:, 0:1]
    hidden = jax.nn.silu(radius * scale[...] + shift[...])
    for layer in range(layers):
        message = jax.nn.silu(
            jnp.dot(hidden.astype(jnp.bfloat16), mw[layer], preferred_element_type=jnp.float32)
        )
        weighted = (weight * message).astype(jnp.bfloat16)
        part = jnp.dot(hot_t, weighted, preferred_element_type=jnp.float32)
        rows_out[layer] = jnp.concatenate(
            [part[0:RUN, h * LANES : (h + 1) * LANES] for h in range(halves)], axis=0
        ).astype(jnp.bfloat16)
        to_all(rows_out.at[layer], rows_buf.at[layer], 2 + layer)
        rounds(1 + layer, psi_round)
        rows_buf[layer, me] = rows_out[layer]
        wait_all(rows_buf.at[layer], got.at[2 + layer], n - 1)
        held = rows_buf[layer].reshape(n * RUN * halves, LANES)
        summed = jnp.concatenate(
            [jnp.dot(pick, held, preferred_element_type=jnp.float32) for pick in selects], axis=1
        )
        update = jax.nn.silu(
            jnp.dot(
                (summed * share).astype(jnp.bfloat16), aw[layer],
                preferred_element_type=jnp.float32,
            )
        ).astype(jnp.bfloat16)
        picked = jnp.dot(hot, update, preferred_element_type=jnp.float32)
        hidden = hidden + message * picked
    score = jnp.sum(hidden * head[...], axis=1, keepdims=True)
    potential = radius * (1.0 + jnp.tanh(score))
    pot[...] = to_rows(potential)
    final = 2 + layers
    scaled_out[...] = to_rows(weight * potential)

    @pl.loop(1, n_atom)
    def _(d):
        remote(
            scaled_out, near.at[n_atom + atom], sent.at[final], got.at[final],
            (grid, lax.rem(atom + d, n_atom)),
        )

    @pl.when(has_outer)
    def _():
        @pl.loop(0, n_atom)
        def _(d):
            remote(
                scaled_out, near.at[inner * n_atom + atom], sent.at[final + 1],
                got.at[final + 1 + side], (og, d),
            )

    @pl.loop(0, n_atom)
    def _(d):
        remote(
            scaled_out, near.at[outer * n_atom + atom], sent.at[final + 2],
            got.at[final + 2 - side], (ig, d),
        )

    rounds(layers + 1, psi_round)
    near[n_atom + atom] = scaled_out[...]
    wait_all(near, got.at[final], n_atom - 1)

    @pl.when(has_outer)
    def _():
        wait_all(near, got.at[final + 2 - side], n_atom)

    wait_all(near, got.at[final + 1 + side], n_atom)

    @pl.loop(0, n_atom)
    def _(q):
        at = pl.ds(q * nb, nb)
        wait_bytes(psi.at[inner, at], psi_got.at[inner, q])

        @pl.when(has_outer)
        def _():
            wait_bytes(psi.at[outer, at], psi_got.at[outer, q])

        @pl.when(q != atom)
        def _():
            wait_bytes(basis.at[1, q], chip_sent.at[q])

        for way in range(2):
            able = (
                jnp.logical_and(q <= atom, atom < n_atom - 1)
                if way == 0
                else jnp.logical_and(q >= atom, atom > 0)
            )

            @pl.when(able)
            def _():
                wait_bytes(basis.at[1, q], z_sent.at[0, way, q])

            @pl.when(jnp.logical_and(able, has_outer))
            def _():
                wait_bytes(basis.at[1, q], z_sent.at[1, way, q])

    @pl.when(has_outer)
    def _():
        wait_bytes(names, name_sent.at[0])
        wait_bytes(piece, v_sent.at[0])
        wait_bytes(part_out.at[0], part_sent.at[0])
        wait_bytes(psi.at[1], psi_sent.at[0])

    wait_bytes(names, name_sent.at[1])
    wait_bytes(piece, v_sent.at[1])
    wait_bytes(part_out.at[1], part_sent.at[1])
    wait_bytes(psi.at[1], psi_sent.at[1])

    @pl.when(relays)
    def _():
        for phase in range(2):
            wait_bytes(relay.at[phase], relay_sent.at[phase])

    wait_all(dens_buf, sent.at[0], n_atom - 1)
    wait_all(info_buf, sent.at[1], n - 1)
    for layer in range(layers):
        wait_all(rows_buf.at[layer], sent.at[2 + layer], n - 1)
    wait_all(near, sent.at[final], n_atom - 1)
    wait_all(near, sent.at[final + 2], n_atom)

    @pl.when(has_outer)
    def _():
        wait_all(near, sent.at[final + 1], n_atom)


def exchange_of(shape, own, piece, names, atoms, weights, scale, shift, mw, aw, head):
    n_grid, n_atom = shape
    n = n_grid * n_atom
    nb, points, depth = piece.shape
    count = nb * n_atom
    width, columns = own.shape[1:]
    layers, features, _ = mw.shape
    packed = RUN * (features // LANES)
    bf16, f32 = jnp.bfloat16, jnp.float32
    dma = pltpu.SemaphoreType.DMA
    grant = 2 * own.size + 14 * count * points * columns + 6 * count * depth * points
    grant += n * (packed * LANES * (2 * layers + 8) + 12 * RUN * LANES) + (6 << 20)
    given = 6 * count * points * (columns + depth)
    if grant + given > 48 << 20:
        grant = 60 << 20
    return pl.pallas_call(
        functools.partial(exchange_kernel, shape, layers),
        out_shape=(
            jax.ShapeDtypeStruct((nb, points), f32),
            jax.ShapeDtypeStruct((3 * n_atom, nb, points), f32),
            jax.ShapeDtypeStruct((3, count, points, columns), bf16),
            jax.ShapeDtypeStruct((3, count, depth, points), bf16),
            jax.ShapeDtypeStruct((3, *names.shape), names.dtype),
        ),
        in_specs=[HBM] * 10,
        out_specs=(VMEM,) * 5,
        scratch_shapes=[
            pltpu.VMEM(a.shape, a.dtype) for a in (atoms, weights, scale, shift, mw, aw, head)
        ]
        + [
            pltpu.VMEM((own.shape[0] + 2, width, columns), bf16),
            pltpu.VMEM((3, n_atom, nb, points, depth), bf16),
            pltpu.SMEM((3, *names.shape), names.dtype),
            pltpu.VMEM((count, points, columns), f32),
            pltpu.VMEM((2, count, points, columns), bf16),
            pltpu.VMEM((2, count, points, columns), bf16),
            pltpu.VMEM((2, n_atom, nb // 2, points, columns), bf16),
            pltpu.VMEM((n_atom, nb, points), f32),
            pltpu.VMEM((n_atom, nb, points), f32),
            pltpu.VMEM((RUN, LANES), f32),
            pltpu.VMEM((n, RUN, LANES), f32),
            pltpu.VMEM((layers, packed, LANES), bf16),
            pltpu.VMEM((layers, n, packed, LANES), bf16),
            pltpu.VMEM((nb, points), f32),
            dma((10,)),
            dma((1,)),
            dma((2,)),
            dma((3,)),
            dma((2,)),
            dma((3, n_atom)),
            dma((2, 2, n_atom)),
            dma((n_atom,)),
            dma((2,)),
            dma((2, n_atom)),
            dma((2,)),
            dma((3, n_atom)),
            dma((2, n_atom)),
            dma((2,)),
            dma((5 + layers,)),
            dma((5 + layers,)),
        ],
        compiler_params=pltpu.CompilerParams(
            collective_id=0, has_side_effects=True, vmem_limit_bytes=grant
        ),
        name="exchange_of",
    )(
        *(
            pltpu.with_memory_space_constraint(a, pltpu.HBM)
            for a in (own, piece, names, atoms, weights, scale, shift, mw, aw, head)
        )
    )


QUAD = 4


def fock_kernel(names, basis_t, near, psi, pot, out, pot_out, filled, table, held, done):
    groups, count, depth, points = basis_t.shape
    owned, width, columns = out.shape
    picks = depth // width
    most = groups * count * picks
    tile = min(columns, TILE)
    first = lax.axis_index("grid") * owned
    last = pltpu.make_async_copy(pot, pot_out, done.at[owned])
    last.start()

    @pl.loop(0, owned + 2)
    def _(r):
        filled[r] = 0

    for k in range(groups):

        @pl.loop(0, count)
        def _(b):
            for j in range(picks):
                row = jnp.minimum(jnp.maximum(names[k, j, b] - first + 1, 0), owned + 1)
                n = filled[row]
                table[row * most + n] = (k * count + b) * picks + j
                filled[row] = n + 1

    @pl.loop(0, owned)
    def _(r):
        n = filled[r + 1]

        @pl.when(n == 0)
        def _():
            held[r] = jnp.zeros((width, columns), jnp.float32)

        @pl.loop(0, (n + QUAD - 1) // QUAD)
        def _(m):
            parts, values = [], []
            for i in range(QUAD):
                at = m * QUAD + i
                entry = table[(r + 1) * most + jnp.minimum(at, n - 1)]
                s, j = entry // picks, lax.rem(entry, picks)
                k, b = s // count, lax.rem(s, count)
                taken = jnp.where(at < n, 1.0, 0.0)
                part = basis_t[k, b, pl.ds(pl.multiple_of(j * width, width), width), :]
                parts.append(
                    (part.astype(jnp.float32) * (near[pl.ds(s, 1), :] * taken)).astype(
                        jnp.bfloat16
                    )
                )
                values.append((k, b))
            left = jnp.concatenate(parts, axis=1)

            def multiply(first_time):
                for c in range(columns // tile):
                    at = pl.ds(c * tile, tile)
                    right = jnp.concatenate([psi[k, b, :, at] for k, b in values], axis=0)
                    value = jnp.dot(left, right, preferred_element_type=jnp.float32)
                    if first_time:
                        held[r, :, at] = value
                    else:
                        held[r, :, at] += value

            @pl.when(m == 0)
            def _():
                multiply(True)

            @pl.when(m > 0)
            def _():
                multiply(False)

        pltpu.make_async_copy(held.at[r], out.at[r], done.at[r]).start()

    for r in range(owned):
        pltpu.make_async_copy(held.at[r], out.at[r], done.at[r]).wait()
    last.wait()


def fock_of(names, basis_t, near, psi, pot, owned):
    groups, count, depth, points = basis_t.shape
    columns = psi.shape[3]
    width = depth // names.shape[1]
    most = groups * depth // width * count
    return pl.pallas_call(
        fock_kernel,
        out_shape=(
            jax.ShapeDtypeStruct((owned, width, columns), jnp.float32),
            jax.ShapeDtypeStruct(pot.shape, pot.dtype),
        ),
        in_specs=[pl.BlockSpec(memory_space=pltpu.SMEM), VMEM, VMEM, VMEM, VMEM],
        out_specs=(HBM, HBM),
        scratch_shapes=[
            pltpu.SMEM((owned + 2,), jnp.int32),
            pltpu.SMEM(((owned + 2) * most,), jnp.int32),
            pltpu.VMEM((owned, width, columns), jnp.float32),
            pltpu.SemaphoreType.DMA((owned + 1,)),
        ],
        compiler_params=pltpu.CompilerParams(
            vmem_limit_bytes=4 * owned * width * columns + (8 << 20)
        ),
        name="fock_of",
    )(names, basis_t, near, psi, pot)


def local(
    basis_values,
    block_lists,
    orbitals,
    point_weights,
    point_atoms,
    embed_scale,
    embed_shift,
    message_weight,
    atom_weight,
    head_weight,
):
    n_grid, n_atom = lax.axis_size("grid"), lax.axis_size("atom")
    own_rows = orbitals.shape[0]
    batches, points, depth = basis_values.shape
    picks = block_lists.shape[1]
    owned = own_rows // (depth // picks)
    potential, near, psi, basis_t, names = exchange_of(
        (n_grid, n_atom),
        orbitals.reshape(owned, own_rows // owned, -1),
        basis_values,
        block_lists.T,
        point_atoms.reshape(batches, points),
        point_weights.reshape(batches, points),
        embed_scale[None, :],
        embed_shift[None, :],
        message_weight,
        atom_weight,
        head_weight[None, :],
    )
    fock, potential = fock_of(names, basis_t, near.reshape(-1, points), psi, potential, owned)
    return (fock.reshape(own_rows, -1), potential.reshape(-1))


def solution(mesh):
    return jax.shard_map(
        local,
        mesh=mesh,
        in_specs=(
            P(("grid", "atom"), None, None),
            P("grid", None),
            P("grid", "atom"),
            P(("grid", "atom")),
            P(("grid", "atom")),
            P(),
            P(),
            P(),
            P(),
            P(),
        ),
        out_specs=(P("grid", "atom"), P(("grid", "atom"))),
        check_vma=False,
    )
```

```python
import functools
import jax
import jax.numpy as jnp
from jax import lax
from jax.experimental import pallas as pl
from jax.experimental.pallas import tpu as pltpu
from jax.sharding import PartitionSpec as P

ATOM_DEV = 32
RUN = max(ATOM_DEV // 4, 1)
LANES = 128
VMEM = pl.BlockSpec(memory_space=pltpu.VMEM)
HBM = pl.BlockSpec(memory_space=pltpu.HBM)
MESH = pl.DeviceIdType.MESH
TILE = 256


def wait_bytes(ref, sem):
    pltpu.make_async_copy(ref, ref, sem).wait()


def meet_all(shape):
    n_grid, n_atom = shape
    n = n_grid * n_atom
    me = lax.axis_index("grid") * n_atom + lax.axis_index("atom")
    barrier = pltpu.get_barrier_semaphore()

    @pl.loop(1, n)
    def _(d):
        t = lax.rem(me + d, n)
        pl.semaphore_signal(
            barrier, inc=1, device_id=(t // n_atom, lax.rem(t, n_atom)), device_id_type=MESH
        )

    pl.semaphore_wait(barrier, n - 1)


def to_columns(rows):
    parts = [
        jnp.transpose(jnp.broadcast_to(rows[i : i + 1, :], (LANES, LANES)))
        for i in range(rows.shape[0])
    ]
    return jnp.concatenate(parts, axis=0)


def to_rows(columns):
    parts = []
    for i in range(columns.shape[0] // LANES):
        piece = jnp.broadcast_to(columns[i * LANES : (i + 1) * LANES, :], (LANES, LANES))
        parts.append(jnp.transpose(piece)[0:1, :])
    return jnp.concatenate(parts, axis=0)


def wrapped(values, total):
    values = jnp.where(values < 0.0, values + total, values)
    return jnp.where(values >= total, values - total, values)


def exchange_kernel(
    shape, layers, own, piece, names, *rest,
):
    given, rest = rest[:7], rest[7:]
    pot, near, psi, basis_t, all_names = rest[:5]
    atoms, weights, scale, shift, mw, aw, head = rest[5:12]
    (
        rows, basis, lists, acc, part_out, part_in, relay, dens, dens_buf,
        info, info_buf, rows_out, rows_buf, scaled_out,
        load, list_sem, name_sent, name_got, v_sent, v_got, z_sent, chip_sent,
        part_sent, part_got, psi_sent, psi_got, passed, relay_sent, sent, got,
        relay_v, v_passed, pair_sent, pair_got,
    ) = rest[12:]
    n_grid, n_atom = shape
    n = n_grid * n_atom
    grid, atom = lax.axis_index("grid"), lax.axis_index("atom")
    last, middle = n_grid - 1, n_grid // 2
    side = lax.rem(grid, 2)
    outer, inner = 2 * side, 2 - 2 * side
    og, ig = grid - 1 + 2 * side, grid + 1 - 2 * side
    has_outer = jnp.logical_and(og >= 0, og < n_grid)
    at_split = jnp.logical_or(grid == middle - 1, grid == middle)
    whole = jnp.logical_and(has_outer, jnp.logical_not(at_split))
    relays = jnp.logical_or(grid == 0, grid == last)
    relay_to = jnp.where(grid == middle, 0, last)
    forward_to = jnp.where(grid == 0, middle - 1, middle)

    nb, points, depth = piece.shape
    owned, width, columns = own.shape
    picks = depth // width
    tile = min(columns, TILE)
    relayed = nb // 2
    direct = nb - relayed

    def remote(source, target, send_sem, recv_sem, to):
        pltpu.make_async_remote_copy(
            src_ref=source,
            dst_ref=target,
            send_sem=send_sem,
            recv_sem=recv_sem,
            device_id=to,
            device_id_type=MESH,
        ).start()

    half = n // 2
    place_here = (grid // 2) * n_atom + atom
    slot_here = side * half + place_here

    def to_chips(source, held, k):
        @pl.loop(1, half)
        def _(d):
            t = lax.rem(place_here + d, half)
            remote(
                source, held.at[slot_here], sent.at[k], got.at[k],
                ((t // n_atom) * 2 + side, lax.rem(t, n_atom)),
            )

    def hand_over(held, k):
        wait_bytes(held.at[pl.ds(0, half - 1)], got.at[k])
        slab = held.at[pl.ds(side * half, half)]
        remote(slab, slab, pair_sent.at[k], pair_got.at[k], (ig, atom))
        wait_bytes(held.at[pl.ds(0, half)], pair_got.at[k])

    def wait_all(held, sem, count):
        wait_bytes(held.at[pl.ds(0, count)], sem)

    def visit(t):
        reach = jnp.minimum(atom, n_atom - 1 - atom)
        close = jnp.where(lax.rem(t, 2) == 1, atom - (t + 1) // 2, atom + t // 2)
        far = jnp.where(reach == atom, t, n_atom - 1 - t)
        return jnp.where(t <= 2 * reach, close, far)

    held_here = (
        rows.at[pl.ds(1, owned)], basis.at[1, atom], all_names.at[1],
        atoms, weights, scale, shift, mw, aw, head,
    )
    loads = [
        pltpu.make_async_copy(source, target, load.at[i])
        for i, (source, target) in enumerate(zip((own, piece, names, *given), held_here))
    ]
    for copy in loads:
        copy.start()
    meet_all(shape)

    @pl.when(has_outer)
    def _():
        remote(names, all_names.at[inner], name_sent.at[0], name_got.at[inner], (og, atom))

    @pl.when(whole if relayed else has_outer)
    def _():
        remote(piece, basis.at[inner, atom], v_sent.at[0], v_got.at[inner, atom], (og, atom))

    if relayed:

        @pl.when(at_split)
        def _():
            part = pl.ds(direct, relayed)
            remote(piece.at[part], relay_v, v_sent.at[0], v_passed.at[0], (relay_to, atom))
            part = pl.ds(0, direct)
            remote(
                piece.at[part], basis.at[inner, atom, part], v_sent.at[0],
                v_got.at[inner, atom], (og, atom),
            )

    remote(names, all_names.at[outer], name_sent.at[1], name_got.at[outer], (ig, atom))
    remote(piece, basis.at[outer, atom], v_sent.at[1], v_got.at[outer, atom], (ig, atom))

    @pl.when(atom < n_atom - 1)
    def _():
        remote(
            piece, basis.at[1, atom], z_sent.at[0, 0, atom], v_got.at[1, atom], (grid, atom + 1)
        )

    @pl.when(atom > 0)
    def _():
        remote(
            piece, basis.at[1, atom], z_sent.at[0, 1, atom], v_got.at[1, atom], (grid, atom - 1)
        )

    for copy in loads[1:5]:
        copy.wait()
    total = float(ATOM_DEV * n_atom)
    named = atoms[...].astype(jnp.float32)
    lead = named[0:1, 0:1]
    shifted = wrapped(named - lead + total / 2, total) - total / 2
    least = jnp.min(jnp.min(shifted, axis=1, keepdims=True), axis=0, keepdims=True)
    start = wrapped(lead + least, total)
    place = shifted - least
    lane = lax.broadcasted_iota(jnp.int32, (1, LANES), 1)
    mine = jnp.where(lane < RUN, wrapped(start + lane.astype(jnp.float32), total), -1.0)
    run = lax.broadcasted_iota(jnp.int32, (RUN, LANES), 0).astype(jnp.float32)
    mass = jnp.zeros((RUN, 1), jnp.float32)
    for i in range(nb):
        here = jnp.where(place[i : i + 1, :] == run, weights[i : i + 1, :], 0.0)
        mass = mass + jnp.sum(here, axis=1, keepdims=True)
    info[...] = jnp.where(
        lax.broadcasted_iota(jnp.int32, (RUN, LANES), 1) < LANES // 2,
        wrapped(start + run, total),
        mass,
    )
    to_chips(info, info_buf, 1)
    info_buf[slot_here] = info[...]

    if relayed:

        @pl.when(relays)
        def _():
            wait_bytes(relay_v, v_passed.at[0])
            remote(
                relay_v, basis.at[inner, atom, pl.ds(direct, relayed)], v_passed.at[1],
                v_got.at[inner, atom], (forward_to, atom),
            )


    for edge in (0, owned + 1):
        rows[edge] = jnp.zeros((width, columns), rows.dtype)

    @pl.when(jnp.logical_not(has_outer))
    def _():
        all_names[outer] = jnp.full(names.shape, -1, names.dtype)
        part_in[0] = jnp.zeros(part_in.shape[1:], part_in.dtype)

    @pl.when(has_outer)
    def _():
        wait_bytes(names, name_got.at[outer])

    wait_bytes(names, name_got.at[inner])
    copy = pltpu.make_async_copy(all_names, lists, list_sem.at[0])
    copy.start()
    copy.wait()
    loads[0].wait()
    first = grid * owned

    def product(slot, q, i, keep):
        chosen = []
        for j in range(picks):
            block = lists[slot, j, q * nb + i] - first + 1
            chosen.append(jnp.minimum(jnp.maximum(block, 0), owned + 1))
        values = basis[slot, q, i]
        for c in range(columns // tile):
            at = pl.ds(c * tile, tile)
            held = jnp.concatenate(
                [rows[k, :, at] for k in chosen], axis=0
            )
            keep(at, jnp.dot(values, held, preferred_element_type=jnp.float32))

    def outward(phase, q, i, source, target, sent_sem, got_sem, near_by=True, far=True):
        if near_by:

            @pl.when(whole if i >= direct else has_outer)
            def _():
                remote(source, target, sent_sem, got_sem, (og, atom))

        if far and i >= direct:

            @pl.when(at_split)
            def _():
                remote(
                    source, relay.at[phase, q, i - direct], sent_sem, passed.at[phase, q],
                    (relay_to, atom),
                )

    def forward(phase, r):
        q = visit(r)

        @pl.when(relays)
        def _():
            held = relay.at[phase, q]
            wait_bytes(held, passed.at[phase, q])
            at = pl.ds(q * nb + direct, relayed)
            if phase == 0:
                target, got_sem = part_in.at[0, at], part_got.at[0, q]
            else:
                target, got_sem = psi.at[inner, at], psi_got.at[inner, q]
            remote(held, target, relay_sent.at[phase], got_sem, (forward_to, atom))

    def finish(q):
        wait_bytes(part_in.at[1, pl.ds(q * nb, nb)], part_got.at[1, q])

        @pl.when(has_outer)
        def _():
            wait_bytes(part_in.at[0, pl.ds(q * nb, nb)], part_got.at[0, q])

        for i in range(nb):
            b = q * nb + i
            sums = jnp.zeros((points, LANES), jnp.float32)
            for c in range(columns // LANES):
                at = pl.ds(c * LANES, LANES)
                value = (
                    acc[b, :, at]
                    + part_in[0, b, :, at].astype(jnp.float32)
                    + part_in[1, b, :, at].astype(jnp.float32)
                )
                rounded = value.astype(jnp.bfloat16)
                psi[1, b, :, at] = rounded
                sums = sums + jnp.square(rounded.astype(jnp.float32))
            dens[q, i : i + 1, :] = jnp.sum(jnp.transpose(sums), axis=0, keepdims=True)

        @pl.when(q != atom)
        def _():
            remote(dens.at[q], dens_buf.at[atom], sent.at[0], got.at[0], (grid, q))

        at = pl.ds(q * nb, nb)
        remote(psi.at[1, at], psi.at[outer, at], psi_sent.at[1], psi_got.at[outer, q], (ig, atom))
        psi_outward(q, near_by=False)

    def psi_outward(q, **which):
        for i in range(nb):
            b = q * nb + i
            outward(
                1, q, i, psi.at[1, b], psi.at[inner, b], psi_sent.at[0], psi_got.at[inner, q],
                **which,
            )

    def psi_round(r):
        psi_outward(visit(r), far=False)
        forward(1, r)

    reach = jnp.minimum(atom, n_atom - 1 - atom)

    def along(stream, slot, q):
        for way in range(2):
            able = (
                jnp.logical_and(q <= atom, atom < n_atom - 1)
                if way == 0
                else jnp.logical_and(q >= atom, atom > 0)
            )

            @pl.when(able)
            def _():
                remote(
                    basis.at[slot, q], basis.at[slot, q], z_sent.at[stream, way, q],
                    v_got.at[slot, q], (grid, atom + 1 - 2 * way),
                )

    def spread_outer(t):
        q = visit(t)

        @pl.when(has_outer)
        def _():
            wait_bytes(basis.at[outer, q], v_got.at[outer, q])
            along(1, outer, q)

    def spread_own(t):
        q = visit(t)
        wait_bytes(basis.at[1, q], v_got.at[1, q])
        along(0, 1, q)
        remote(
            basis.at[1, q], basis.at[outer, q], chip_sent.at[q], v_got.at[outer, q], (ig, atom)
        )

    def product_outer(q):
        @pl.when(has_outer)
        def _():
            for i in range(nb):
                b = q * nb + i

                def keep(at, value):
                    part_out[0, b, :, at] = value.astype(jnp.bfloat16)

                product(outer, q, i, keep)
                outward(
                    0, q, i, part_out.at[0, b], part_in.at[0, b], part_sent.at[0],
                    part_got.at[0, q],
                )

    def products_here(q):
        wait_bytes(basis.at[inner, q], v_got.at[inner, q])
        for i in range(nb):
            b = q * nb + i

            def keep(at, value):
                part_out[1, b, :, at] = value.astype(jnp.bfloat16)

            product(inner, q, i, keep)
            remote(
                part_out.at[1, b], part_in.at[1, b], part_sent.at[1], part_got.at[1, q],
                (ig, atom),
            )

        for i in range(nb):
            b = q * nb + i

            def keep(at, value):
                acc[b, :, at] = value

            product(1, q, i, keep)
            for slot in range(3):
                basis_t[slot, b] = jnp.transpose(basis[slot, q, i])

    spread_outer(0)

    @pl.loop(0, n_atom)
    def _(t):
        q = visit(t)
        paired = jnp.logical_and(lax.rem(t, 2) == 1, t < 2 * reach)
        fresh = jnp.logical_and(
            t > 0, jnp.logical_or(lax.rem(t, 2) == 1, t > 2 * reach)
        )

        @pl.when(fresh)
        def _():
            spread_outer(t)

        @pl.when(paired)
        def _():
            spread_outer(t + 1)

        product_outer(q)

        @pl.when(t > 0)
        def _():
            products_here(visit(t - 1))

        @pl.when(fresh)
        def _():
            spread_own(t)

        @pl.when(paired)
        def _():
            spread_own(t + 1)

        @pl.when(t >= 1)
        def _():
            forward(0, t - 1)

        @pl.when(t >= 2)
        def _():
            finish(visit(t - 2))

    stops = layers + 2

    def rounds(s, act):
        for r in range(n_atom):
            if r * stops // n_atom == s:
                act(r)

    rounds(0, psi_round)
    products_here(visit(n_atom - 1))
    finish(visit(n_atom - 2))
    weight = to_columns(weights[...])[:, 0:1]
    spot = to_columns(place)
    hot = (spot == lax.broadcasted_iota(jnp.int32, spot.shape, 1).astype(jnp.float32)).astype(
        jnp.bfloat16
    )
    deep = lax.broadcasted_iota(jnp.int32, (LANES, LANES), 0).astype(jnp.float32)
    hot_t = jnp.concatenate([place[i : i + 1, :] == deep for i in range(nb)], axis=1).astype(
        jnp.bfloat16
    )
    for copy in loads[5:]:
        copy.wait()
    halves = scale.shape[1] // LANES
    hand_over(info_buf, 1)
    facts = info_buf[...].reshape(n * RUN, LANES)
    same = (facts[:, 0:1] == mine).astype(jnp.float32)
    mass = jnp.sum(same * facts[:, LANES // 2 : LANES // 2 + 1], axis=0, keepdims=True)
    share = 1.0 / (1.0 + to_columns(mass)[:, 0:1])
    same = same.reshape(n, RUN, LANES)
    none = jnp.zeros_like(same)
    selects = []
    for h in range(halves):
        full = jnp.concatenate(
            [same if k == h else none for k in range(halves)], axis=1
        ).reshape(n * RUN * halves, LANES)
        selects.append(jnp.transpose(full).astype(jnp.bfloat16))

    forward(0, n_atom - 1)
    finish(visit(n_atom - 1))
    dens_buf[atom] = dens[atom]

    wait_all(dens_buf, got.at[0], n_atom - 1)
    density = to_columns(2.0 * jnp.sum(dens_buf[...], axis=0))
    safe = jnp.where(density > 0.0, density, 1.0)
    radius = jnp.where(density > 0.0, jnp.exp(jnp.log(safe) * (1.0 / 3.0)), 0.0)[:, 0:1]
    hidden = jax.nn.silu(radius * scale[...] + shift[...])
    for layer in range(layers):
        message = jax.nn.silu(
            jnp.dot(hidden.astype(jnp.bfloat16), mw[layer], preferred_element_type=jnp.float32)
        )
        weighted = (weight * message).astype(jnp.bfloat16)
        part = jnp.dot(hot_t, weighted, preferred_element_type=jnp.float32)
        rows_out[layer] = jnp.concatenate(
            [part[0:RUN, h * LANES : (h + 1) * LANES] for h in range(halves)], axis=0
        ).astype(jnp.bfloat16)
        to_chips(rows_out.at[layer], rows_buf.at[layer], 2 + layer)
        rows_buf[layer, slot_here] = rows_out[layer]
        rounds(1 + layer, psi_round)
        hand_over(rows_buf.at[layer], 2 + layer)
        held = rows_buf[layer].reshape(n * RUN * halves, LANES)
        summed = jnp.concatenate(
            [jnp.dot(pick, held, preferred_element_type=jnp.float32) for pick in selects], axis=1
        )
        update = jax.nn.silu(
            jnp.dot(
                (summed * share).astype(jnp.bfloat16), aw[layer],
                preferred_element_type=jnp.float32,
            )
        ).astype(jnp.bfloat16)
        picked = jnp.dot(hot, update, preferred_element_type=jnp.float32)
        hidden = hidden + message * picked
    score = jnp.sum(hidden * head[...], axis=1, keepdims=True)
    potential = radius * (1.0 + jnp.tanh(score))
    pot[...] = to_rows(potential)
    final = 2 + layers
    scaled_out[...] = to_rows(weight * potential)

    @pl.loop(1, n_atom)
    def _(d):
        remote(
            scaled_out, near.at[n_atom + atom], sent.at[final], got.at[final],
            (grid, lax.rem(atom + d, n_atom)),
        )

    @pl.when(has_outer)
    def _():
        @pl.loop(0, n_atom)
        def _(d):
            remote(
                scaled_out, near.at[inner * n_atom + atom], sent.at[final + 1],
                got.at[final + 1 + side], (og, d),
            )

    @pl.loop(0, n_atom)
    def _(d):
        remote(
            scaled_out, near.at[outer * n_atom + atom], sent.at[final + 2],
            got.at[final + 2 - side], (ig, d),
        )

    rounds(layers + 1, psi_round)
    near[n_atom + atom] = scaled_out[...]
    wait_all(near, got.at[final], n_atom - 1)

    @pl.when(has_outer)
    def _():
        wait_all(near, got.at[final + 2 - side], n_atom)

    wait_all(near, got.at[final + 1 + side], n_atom)

    @pl.loop(0, n_atom)
    def _(q):
        at = pl.ds(q * nb, nb)
        wait_bytes(psi.at[inner, at], psi_got.at[inner, q])

        @pl.when(has_outer)
        def _():
            wait_bytes(psi.at[outer, at], psi_got.at[outer, q])

        @pl.when(q != atom)
        def _():
            wait_bytes(basis.at[1, q], chip_sent.at[q])

        for way in range(2):
            able = (
                jnp.logical_and(q <= atom, atom < n_atom - 1)
                if way == 0
                else jnp.logical_and(q >= atom, atom > 0)
            )

            @pl.when(able)
            def _():
                wait_bytes(basis.at[1, q], z_sent.at[0, way, q])

            @pl.when(jnp.logical_and(able, has_outer))
            def _():
                wait_bytes(basis.at[1, q], z_sent.at[1, way, q])

    @pl.when(has_outer)
    def _():
        wait_bytes(names, name_sent.at[0])
        wait_bytes(piece, v_sent.at[0])
        wait_bytes(part_out.at[0], part_sent.at[0])
        wait_bytes(psi.at[1], psi_sent.at[0])

    wait_bytes(names, name_sent.at[1])
    wait_bytes(piece, v_sent.at[1])
    wait_bytes(part_out.at[1], part_sent.at[1])
    wait_bytes(psi.at[1], psi_sent.at[1])

    @pl.when(relays)
    def _():
        wait_bytes(relay_v, v_passed.at[1])
        for phase in range(2):
            wait_bytes(relay.at[phase], relay_sent.at[phase])

    wait_all(dens_buf, sent.at[0], n_atom - 1)
    for k, held in enumerate([info_buf] + [rows_buf.at[layer] for layer in range(layers)]):
        wait_all(held, sent.at[1 + k], half - 1)
        wait_all(held, pair_sent.at[1 + k], half)
    wait_all(near, sent.at[final], n_atom - 1)
    wait_all(near, sent.at[final + 2], n_atom)

    @pl.when(has_outer)
    def _():
        wait_all(near, sent.at[final + 1], n_atom)


def exchange_of(shape, own, piece, names, atoms, weights, scale, shift, mw, aw, head):
    n_grid, n_atom = shape
    n = n_grid * n_atom
    nb, points, depth = piece.shape
    count = nb * n_atom
    width, columns = own.shape[1:]
    layers, features, _ = mw.shape
    packed = RUN * (features // LANES)
    bf16, f32 = jnp.bfloat16, jnp.float32
    dma = pltpu.SemaphoreType.DMA
    grant = 2 * own.size + 14 * count * points * columns + 6 * count * depth * points
    grant += n * (packed * LANES * (2 * layers + 8) + 12 * RUN * LANES) + (6 << 20)
    given = 6 * count * points * (columns + depth)
    if grant + given > 48 << 20:
        grant = 60 << 20
    return pl.pallas_call(
        functools.partial(exchange_kernel, shape, layers),
        out_shape=(
            jax.ShapeDtypeStruct((nb, points), f32),
            jax.ShapeDtypeStruct((3 * n_atom, nb, points), f32),
            jax.ShapeDtypeStruct((3, count, points, columns), bf16),
            jax.ShapeDtypeStruct((3, count, depth, points), bf16),
            jax.ShapeDtypeStruct((3, *names.shape), names.dtype),
        ),
        in_specs=[HBM] * 10,
        out_specs=(VMEM,) * 5,
        scratch_shapes=[
            pltpu.VMEM(a.shape, a.dtype) for a in (atoms, weights, scale, shift, mw, aw, head)
        ]
        + [
            pltpu.VMEM((own.shape[0] + 2, width, columns), bf16),
            pltpu.VMEM((3, n_atom, nb, points, depth), bf16),
            pltpu.SMEM((3, *names.shape), names.dtype),
            pltpu.VMEM((count, points, columns), f32),
            pltpu.VMEM((2, count, points, columns), bf16),
            pltpu.VMEM((2, count, points, columns), bf16),
            pltpu.VMEM((2, n_atom, nb // 2, points, columns), bf16),
            pltpu.VMEM((n_atom, nb, points), f32),
            pltpu.VMEM((n_atom, nb, points), f32),
            pltpu.VMEM((RUN, LANES), f32),
            pltpu.VMEM((n, RUN, LANES), f32),
            pltpu.VMEM((layers, packed, LANES), bf16),
            pltpu.VMEM((layers, n, packed, LANES), bf16),
            pltpu.VMEM((nb, points), f32),
            dma((10,)),
            dma((1,)),
            dma((2,)),
            dma((3,)),
            dma((2,)),
            dma((3, n_atom)),
            dma((2, 2, n_atom)),
            dma((n_atom,)),
            dma((2,)),
            dma((2, n_atom)),
            dma((2,)),
            dma((3, n_atom)),
            dma((2, n_atom)),
            dma((2,)),
            dma((5 + layers,)),
            dma((5 + layers,)),
            pltpu.VMEM((max(nb // 2, 1), points, depth), bf16),
            dma((2,)),
            dma((2 + layers,)),
            dma((2 + layers,)),
        ],
        compiler_params=pltpu.CompilerParams(
            collective_id=0, has_side_effects=True, vmem_limit_bytes=grant
        ),
        name="exchange_of",
    )(
        *(
            pltpu.with_memory_space_constraint(a, pltpu.HBM)
            for a in (own, piece, names, atoms, weights, scale, shift, mw, aw, head)
        )
    )


QUAD = 4


def fock_kernel(names, basis_t, near, psi, pot, out, pot_out, filled, table, held, done):
    groups, count, depth, points = basis_t.shape
    owned, width, columns = out.shape
    picks = depth // width
    most = groups * count * picks
    tile = min(columns, TILE)
    first = lax.axis_index("grid") * owned
    last = pltpu.make_async_copy(pot, pot_out, done.at[owned])
    last.start()

    @pl.loop(0, owned + 2)
    def _(r):
        filled[r] = 0

    for k in range(groups):

        @pl.loop(0, count)
        def _(b):
            for j in range(picks):
                row = jnp.minimum(jnp.maximum(names[k, j, b] - first + 1, 0), owned + 1)
                n = filled[row]
                table[row * most + n] = (k * count + b) * picks + j
                filled[row] = n + 1

    @pl.loop(0, owned)
    def _(r):
        n = filled[r + 1]

        @pl.when(n == 0)
        def _():
            held[r] = jnp.zeros((width, columns), jnp.float32)

        @pl.loop(0, (n + QUAD - 1) // QUAD)
        def _(m):
            parts, values = [], []
            for i in range(QUAD):
                at = m * QUAD + i
                entry = table[(r + 1) * most + jnp.minimum(at, n - 1)]
                s, j = entry // picks, lax.rem(entry, picks)
                k, b = s // count, lax.rem(s, count)
                taken = jnp.where(at < n, 1.0, 0.0)
                part = basis_t[k, b, pl.ds(pl.multiple_of(j * width, width), width), :]
                parts.append(
                    (part.astype(jnp.float32) * (near[pl.ds(s, 1), :] * taken)).astype(
                        jnp.bfloat16
                    )
                )
                values.append((k, b))
            left = jnp.concatenate(parts, axis=1)

            def multiply(first_time):
                for c in range(columns // tile):
                    at = pl.ds(c * tile, tile)
                    right = jnp.concatenate([psi[k, b, :, at] for k, b in values], axis=0)
                    value = jnp.dot(left, right, preferred_element_type=jnp.float32)
                    if first_time:
                        held[r, :, at] = value
                    else:
                        held[r, :, at] += value

            @pl.when(m == 0)
            def _():
                multiply(True)

            @pl.when(m > 0)
            def _():
                multiply(False)

        pltpu.make_async_copy(held.at[r], out.at[r], done.at[r]).start()

    for r in range(owned):
        pltpu.make_async_copy(held.at[r], out.at[r], done.at[r]).wait()
    last.wait()


def fock_of(names, basis_t, near, psi, pot, owned):
    groups, count, depth, points = basis_t.shape
    columns = psi.shape[3]
    width = depth // names.shape[1]
    most = groups * depth // width * count
    return pl.pallas_call(
        fock_kernel,
        out_shape=(
            jax.ShapeDtypeStruct((owned, width, columns), jnp.float32),
            jax.ShapeDtypeStruct(pot.shape, pot.dtype),
        ),
        in_specs=[pl.BlockSpec(memory_space=pltpu.SMEM), VMEM, VMEM, VMEM, VMEM],
        out_specs=(HBM, HBM),
        scratch_shapes=[
            pltpu.SMEM((owned + 2,), jnp.int32),
            pltpu.SMEM(((owned + 2) * most,), jnp.int32),
            pltpu.VMEM((owned, width, columns), jnp.float32),
            pltpu.SemaphoreType.DMA((owned + 1,)),
        ],
        compiler_params=pltpu.CompilerParams(
            vmem_limit_bytes=4 * owned * width * columns + (8 << 20)
        ),
        name="fock_of",
    )(names, basis_t, near, psi, pot)


def local(
    basis_values,
    block_lists,
    orbitals,
    point_weights,
    point_atoms,
    embed_scale,
    embed_shift,
    message_weight,
    atom_weight,
    head_weight,
):
    n_grid, n_atom = lax.axis_size("grid"), lax.axis_size("atom")
    own_rows = orbitals.shape[0]
    batches, points, depth = basis_values.shape
    picks = block_lists.shape[1]
    owned = own_rows // (depth // picks)
    potential, near, psi, basis_t, names = exchange_of(
        (n_grid, n_atom),
        orbitals.reshape(owned, own_rows // owned, -1),
        basis_values,
        block_lists.T,
        point_atoms.reshape(batches, points),
        point_weights.reshape(batches, points),
        embed_scale[None, :],
        embed_shift[None, :],
        message_weight,
        atom_weight,
        head_weight[None, :],
    )
    fock, potential = fock_of(names, basis_t, near.reshape(-1, points), psi, potential, owned)
    return (fock.reshape(own_rows, -1), potential.reshape(-1))


def solution(mesh):
    return jax.shard_map(
        local,
        mesh=mesh,
        in_specs=(
            P(("grid", "atom"), None, None),
            P("grid", None),
            P("grid", "atom"),
            P(("grid", "atom")),
            P(("grid", "atom")),
            P(),
            P(),
            P(),
            P(),
            P(),
        ),
        out_specs=(P("grid", "atom"), P(("grid", "atom"))),
        check_vma=False,
    )
```

```python
import functools
import jax
import jax.numpy as jnp
from jax import lax
from jax.experimental import pallas as pl
from jax.experimental.pallas import tpu as pltpu
from jax.sharding import PartitionSpec as P

ATOM_DEV = 32
RUN = max(ATOM_DEV // 4, 1)
LANES = 128
VMEM = pl.BlockSpec(memory_space=pltpu.VMEM)
HBM = pl.BlockSpec(memory_space=pltpu.HBM)
MESH = pl.DeviceIdType.MESH
TILE = 256
PARTS = (2, 2, 2, 2)


def wait_bytes(ref, sem):
    pltpu.make_async_copy(ref, ref, sem).wait()


def meet_all(shape):
    n_grid, n_atom = shape
    n = n_grid * n_atom
    me = lax.axis_index("grid") * n_atom + lax.axis_index("atom")
    barrier = pltpu.get_barrier_semaphore()

    @pl.loop(1, n)
    def _(d):
        t = lax.rem(me + d, n)
        pl.semaphore_signal(
            barrier, inc=1, device_id=(t // n_atom, lax.rem(t, n_atom)), device_id_type=MESH
        )

    pl.semaphore_wait(barrier, n - 1)


def to_columns(rows):
    parts = [
        jnp.transpose(jnp.broadcast_to(rows[i : i + 1, :], (LANES, LANES)))
        for i in range(rows.shape[0])
    ]
    return jnp.concatenate(parts, axis=0)


def to_rows(columns):
    parts = []
    for i in range(columns.shape[0] // LANES):
        piece = jnp.broadcast_to(columns[i * LANES : (i + 1) * LANES, :], (LANES, LANES))
        parts.append(jnp.transpose(piece)[0:1, :])
    return jnp.concatenate(parts, axis=0)


def wrapped(values, total):
    values = jnp.where(values < 0.0, values + total, values)
    return jnp.where(values >= total, values - total, values)


def exchange_kernel(
    shape, layers, own, piece, names, *rest,
):
    given, rest = rest[:7], rest[7:]
    pot, near, psi, basis_t, all_names = rest[:5]
    atoms, weights, scale, shift, mw, aw, head = rest[5:12]
    (
        rows, basis, lists, acc, part_out, part_in, relay, dens, dens_buf,
        info, info_buf, rows_out, rows_buf, scaled_out,
        load, list_sem, name_sent, name_got, v_sent, v_got, z_sent, chip_sent,
        part_sent, part_got, psi_sent, psi_got, passed, relay_sent, sent, got,
        relay_v, v_passed, pair_sent, pair_got, v_first,
    ) = rest[12:]
    n_grid, n_atom = shape
    n = n_grid * n_atom
    grid, atom = lax.axis_index("grid"), lax.axis_index("atom")
    last, middle = n_grid - 1, n_grid // 2
    side = lax.rem(grid, 2)
    outer, inner = 2 * side, 2 - 2 * side
    og, ig = grid - 1 + 2 * side, grid + 1 - 2 * side
    has_outer = jnp.logical_and(og >= 0, og < n_grid)
    at_split = jnp.logical_or(grid == middle - 1, grid == middle)
    whole = jnp.logical_and(has_outer, jnp.logical_not(at_split))
    relays = jnp.logical_or(grid == 0, grid == last)
    relay_to = jnp.where(grid == middle, 0, last)
    forward_to = jnp.where(grid == 0, middle - 1, middle)

    nb, points, depth = piece.shape
    owned, width, columns = own.shape
    picks = depth // width
    tile = min(columns, TILE)
    relayed = nb // 2
    direct = nb - relayed

    def remote(source, target, send_sem, recv_sem, to):
        pltpu.make_async_remote_copy(
            src_ref=source,
            dst_ref=target,
            send_sem=send_sem,
            recv_sem=recv_sem,
            device_id=to,
            device_id_type=MESH,
        ).start()

    half = n // 2
    place_here = (grid // 2) * n_atom + atom
    slot_here = side * half + place_here

    def to_chips(source, held, k):
        @pl.loop(1, half)
        def _(d):
            t = lax.rem(place_here + d, half)
            remote(
                source, held.at[slot_here], sent.at[k], got.at[k],
                ((t // n_atom) * 2 + side, lax.rem(t, n_atom)),
            )

    def hand_over(held, k):
        wait_bytes(held.at[pl.ds(0, half - 1)], got.at[k])
        slab = held.at[pl.ds(side * half, half)]
        remote(slab, slab, pair_sent.at[k], pair_got.at[k], (ig, atom))
        wait_bytes(held.at[pl.ds(0, half)], pair_got.at[k])

    def wait_all(held, sem, count):
        wait_bytes(held.at[pl.ds(0, count)], sem)

    def visit(t):
        reach = jnp.minimum(atom, n_atom - 1 - atom)
        close = jnp.where(lax.rem(t, 2) == 1, atom - (t + 1) // 2, atom + t // 2)
        far = jnp.where(reach == atom, t, n_atom - 1 - t)
        return jnp.where(t <= 2 * reach, close, far)

    held_here = (
        rows.at[pl.ds(1, owned)], basis.at[1, atom], all_names.at[1],
        atoms, weights, scale, shift, mw, aw, head,
    )
    loads = [
        pltpu.make_async_copy(source, target, load.at[i])
        for i, (source, target) in enumerate(zip((own, piece, names, *given), held_here))
    ]
    for copy in loads:
        copy.start()
    meet_all(shape)

    @pl.when(has_outer)
    def _():
        remote(names, all_names.at[inner], name_sent.at[0], name_got.at[inner], (og, atom))

    for i in range(nb):
        target = basis.at[inner, atom, i]

        @pl.when(has_outer if i < direct else whole)
        def _():
            remote(piece.at[i], target, v_sent.at[0], v_first.at[i], (og, atom))

        if i >= direct:

            @pl.when(at_split)
            def _():
                remote(
                    piece.at[i], relay_v.at[i - direct], v_sent.at[0], v_passed.at[0],
                    (relay_to, atom),
                )

    remote(names, all_names.at[outer], name_sent.at[1], name_got.at[outer], (ig, atom))
    remote(piece, basis.at[outer, atom], v_sent.at[1], v_got.at[outer, atom], (ig, atom))

    @pl.when(atom < n_atom - 1)
    def _():
        remote(
            piece, basis.at[1, atom], z_sent.at[0, 0, atom], v_got.at[1, atom], (grid, atom + 1)
        )

    @pl.when(atom > 0)
    def _():
        remote(
            piece, basis.at[1, atom], z_sent.at[0, 1, atom], v_got.at[1, atom], (grid, atom - 1)
        )

    for copy in loads[1:5]:
        copy.wait()
    total = float(ATOM_DEV * n_atom)
    named = atoms[...].astype(jnp.float32)
    lead = named[0:1, 0:1]
    shifted = wrapped(named - lead + total / 2, total) - total / 2
    least = jnp.min(jnp.min(shifted, axis=1, keepdims=True), axis=0, keepdims=True)
    start = wrapped(lead + least, total)
    place = shifted - least
    lane = lax.broadcasted_iota(jnp.int32, (1, LANES), 1)
    mine = jnp.where(lane < RUN, wrapped(start + lane.astype(jnp.float32), total), -1.0)
    run = lax.broadcasted_iota(jnp.int32, (RUN, LANES), 0).astype(jnp.float32)
    mass = jnp.zeros((RUN, 1), jnp.float32)
    for i in range(nb):
        here = jnp.where(place[i : i + 1, :] == run, weights[i : i + 1, :], 0.0)
        mass = mass + jnp.sum(here, axis=1, keepdims=True)
    info[...] = jnp.where(
        lax.broadcasted_iota(jnp.int32, (RUN, LANES), 1) < LANES // 2,
        wrapped(start + run, total),
        mass,
    )
    to_chips(info, info_buf, 1)
    info_buf[slot_here] = info[...]

    if relayed:

        @pl.when(relays)
        def _():
            wait_bytes(relay_v, v_passed.at[0])
            for i in range(direct, nb):
                remote(
                    relay_v.at[i - direct], basis.at[inner, atom, i], v_passed.at[1],
                    v_first.at[i], (forward_to, atom),
                )

    for edge in (0, owned + 1):
        rows[edge] = jnp.zeros((width, columns), rows.dtype)

    @pl.when(jnp.logical_not(has_outer))
    def _():
        all_names[outer] = jnp.full(names.shape, -1, names.dtype)
        part_in[0] = jnp.zeros(part_in.shape[1:], part_in.dtype)

    @pl.when(has_outer)
    def _():
        wait_bytes(names, name_got.at[outer])

    wait_bytes(names, name_got.at[inner])
    copy = pltpu.make_async_copy(all_names, lists, list_sem.at[0])
    copy.start()
    copy.wait()
    loads[0].wait()
    first = grid * owned

    def product(slot, q, i, keep):
        chosen = []
        for j in range(picks):
            block = lists[slot, j, q * nb + i] - first + 1
            chosen.append(jnp.minimum(jnp.maximum(block, 0), owned + 1))
        values = basis[slot, q, i]
        for c in range(columns // tile):
            at = pl.ds(c * tile, tile)
            held = jnp.concatenate(
                [rows[k, :, at] for k in chosen], axis=0
            )
            keep(at, jnp.dot(values, held, preferred_element_type=jnp.float32))

    def outward(phase, q, i, source, target, sent_sem, got_sem, near_by=True, far=True):
        if near_by:

            @pl.when(whole if i >= direct else has_outer)
            def _():
                remote(source, target, sent_sem, got_sem, (og, atom))

        if far and i >= direct:

            @pl.when(at_split)
            def _():
                remote(
                    source, relay.at[phase, q, i - direct], sent_sem, passed.at[phase, q],
                    (relay_to, atom),
                )

    def forward(phase, r):
        q = visit(r)

        @pl.when(relays)
        def _():
            held = relay.at[phase, q]
            wait_bytes(held, passed.at[phase, q])
            at = pl.ds(q * nb + direct, relayed)
            if phase == 0:
                target, got_sem = part_in.at[0, at], part_got.at[0, q]
            else:
                target, got_sem = psi.at[inner, at], psi_got.at[inner, q]
            remote(held, target, relay_sent.at[phase], got_sem, (forward_to, atom))

    def finish(t):
        q = visit(t)
        wait_bytes(part_in.at[1, pl.ds(q * nb, nb)], part_got.at[1, q])

        @pl.when(has_outer)
        def _():
            wait_bytes(part_in.at[0, pl.ds(q * nb, nb)], part_got.at[0, q])

        for i in range(nb):
            b = q * nb + i
            sums = jnp.zeros((points, LANES), jnp.float32)
            for c in range(columns // LANES):
                at = pl.ds(c * LANES, LANES)
                value = (
                    acc[b, :, at]
                    + part_in[0, b, :, at].astype(jnp.float32)
                    + part_in[1, b, :, at].astype(jnp.float32)
                )
                rounded = value.astype(jnp.bfloat16)
                psi[1, b, :, at] = rounded
                sums = sums + jnp.square(rounded.astype(jnp.float32))
            dens[q, i : i + 1, :] = jnp.sum(jnp.transpose(sums), axis=0, keepdims=True)

        @pl.when(q != atom)
        def _():
            remote(dens.at[q], dens_buf.at[atom], sent.at[0], got.at[0], (grid, q))

        at = pl.ds(q * nb, nb)
        remote(psi.at[1, at], psi.at[outer, at], psi_sent.at[1], psi_got.at[outer, q], (ig, atom))
        for i in range(nb):
            psi_outward(t, i, near_by=False)

    def psi_outward(r, i, **which):
        q = visit(r)
        b = q * nb + i
        outward(
            1, q, i, psi.at[1, b], psi.at[inner, b], psi_sent.at[0], psi_got.at[inner, q],
            **which,
        )

    def psi_unit(r, i):
        psi_outward(r, i, far=False)
        if i == nb - 1:
            forward(1, r)

    reach = jnp.minimum(atom, n_atom - 1 - atom)

    def along(stream, slot, q):
        for way in range(2):
            able = (
                jnp.logical_and(q <= atom, atom < n_atom - 1)
                if way == 0
                else jnp.logical_and(q >= atom, atom > 0)
            )

            @pl.when(able)
            def _():
                remote(
                    basis.at[slot, q], basis.at[slot, q], z_sent.at[stream, way, q],
                    v_got.at[slot, q], (grid, atom + 1 - 2 * way),
                )

    def spread_outer(t):
        q = visit(t)

        @pl.when(has_outer)
        def _():
            wait_bytes(basis.at[outer, q], v_got.at[outer, q])
            along(1, outer, q)

    def send_first():
        for i in range(nb):
            mine_first = basis.at[outer, atom, i]
            wait_bytes(mine_first, v_first.at[i])
            for way in range(2):

                @pl.when(atom < n_atom - 1 if way == 0 else atom > 0)
                def _():
                    remote(
                        mine_first, mine_first, z_sent.at[1, way, atom], v_got.at[outer, atom],
                        (grid, atom + 1 - 2 * way),
                    )

            outer_part(atom, i)

    def spread_own(t):
        q = visit(t)
        wait_bytes(basis.at[1, q], v_got.at[1, q])
        along(0, 1, q)
        remote(
            basis.at[1, q], basis.at[outer, q], chip_sent.at[q], v_got.at[outer, q], (ig, atom)
        )

    def outer_part(q, i):
        b = q * nb + i

        def keep(at, value):
            part_out[0, b, :, at] = value.astype(jnp.bfloat16)

        product(outer, q, i, keep)
        outward(
            0, q, i, part_out.at[0, b], part_in.at[0, b], part_sent.at[0], part_got.at[0, q]
        )

    def product_outer(q):
        for i in range(nb):
            outer_part(q, i)

    def products_here(q):
        wait_bytes(basis.at[inner, q], v_got.at[inner, q])
        for i in range(nb):
            b = q * nb + i

            def keep(at, value):
                part_out[1, b, :, at] = value.astype(jnp.bfloat16)

            product(inner, q, i, keep)
            remote(
                part_out.at[1, b], part_in.at[1, b], part_sent.at[1], part_got.at[1, q],
                (ig, atom),
            )

        for i in range(nb):
            b = q * nb + i

            def keep(at, value):
                acc[b, :, at] = value

            product(1, q, i, keep)
            for slot in range(3):
                basis_t[slot, b] = jnp.transpose(basis[slot, q, i])

    @pl.when(has_outer)
    def _():
        send_first()

    @pl.loop(0, n_atom)
    def _(t):
        q = visit(t)
        paired = jnp.logical_and(lax.rem(t, 2) == 1, t < 2 * reach)
        fresh = jnp.logical_and(
            t > 0, jnp.logical_or(lax.rem(t, 2) == 1, t > 2 * reach)
        )

        @pl.when(fresh)
        def _():
            spread_outer(t)

        @pl.when(paired)
        def _():
            spread_outer(t + 1)

        @pl.when(jnp.logical_and(t > 0, has_outer))
        def _():
            product_outer(q)

        @pl.when(t > 0)
        def _():
            products_here(visit(t - 1))

        @pl.when(fresh)
        def _():
            spread_own(t)

        @pl.when(paired)
        def _():
            spread_own(t + 1)

        @pl.when(t >= 1)
        def _():
            forward(0, t - 1)

        @pl.when(t >= 2)
        def _():
            finish(t - 2)

    ends = [sum(PARTS[: s + 1]) for s in range(len(PARTS))]

    def send_psi(s):
        for u in range(n_atom * nb):
            if sum(u * ends[-1] >= end * n_atom * nb for end in ends) == s:
                psi_unit(u // nb, u % nb)

    send_psi(0)
    products_here(visit(n_atom - 1))
    finish(n_atom - 2)
    weight = to_columns(weights[...])[:, 0:1]
    spot = to_columns(place)
    hot = (spot == lax.broadcasted_iota(jnp.int32, spot.shape, 1).astype(jnp.float32)).astype(
        jnp.bfloat16
    )
    deep = lax.broadcasted_iota(jnp.int32, (LANES, LANES), 0).astype(jnp.float32)
    hot_t = jnp.concatenate([place[i : i + 1, :] == deep for i in range(nb)], axis=1).astype(
        jnp.bfloat16
    )
    for copy in loads[5:]:
        copy.wait()
    halves = scale.shape[1] // LANES
    hand_over(info_buf, 1)
    facts = info_buf[...].reshape(n * RUN, LANES)
    same = (facts[:, 0:1] == mine).astype(jnp.float32)
    mass = jnp.sum(same * facts[:, LANES // 2 : LANES // 2 + 1], axis=0, keepdims=True)
    share = 1.0 / (1.0 + to_columns(mass)[:, 0:1])
    same = same.reshape(n, RUN, LANES)
    none = jnp.zeros_like(same)
    selects = []
    for h in range(halves):
        full = jnp.concatenate(
            [same if k == h else none for k in range(halves)], axis=1
        ).reshape(n * RUN * halves, LANES)
        selects.append(jnp.transpose(full).astype(jnp.bfloat16))

    forward(0, n_atom - 1)
    finish(n_atom - 1)
    dens_buf[atom] = dens[atom]

    wait_all(dens_buf, got.at[0], n_atom - 1)
    density = to_columns(2.0 * jnp.sum(dens_buf[...], axis=0))
    safe = jnp.where(density > 0.0, density, 1.0)
    radius = jnp.where(density > 0.0, jnp.exp(jnp.log(safe) * (1.0 / 3.0)), 0.0)[:, 0:1]
    hidden = jax.nn.silu(radius * scale[...] + shift[...])
    for layer in range(layers):
        message = jax.nn.silu(
            jnp.dot(hidden.astype(jnp.bfloat16), mw[layer], preferred_element_type=jnp.float32)
        )
        weighted = (weight * message).astype(jnp.bfloat16)
        part = jnp.dot(hot_t, weighted, preferred_element_type=jnp.float32)
        rows_out[layer] = jnp.concatenate(
            [part[0:RUN, h * LANES : (h + 1) * LANES] for h in range(halves)], axis=0
        ).astype(jnp.bfloat16)
        to_chips(rows_out.at[layer], rows_buf.at[layer], 2 + layer)
        rows_buf[layer, slot_here] = rows_out[layer]
        send_psi(1 + layer)
        hand_over(rows_buf.at[layer], 2 + layer)
        held = rows_buf[layer].reshape(n * RUN * halves, LANES)
        summed = jnp.concatenate(
            [jnp.dot(pick, held, preferred_element_type=jnp.float32) for pick in selects], axis=1
        )
        update = jax.nn.silu(
            jnp.dot(
                (summed * share).astype(jnp.bfloat16), aw[layer],
                preferred_element_type=jnp.float32,
            )
        ).astype(jnp.bfloat16)
        picked = jnp.dot(hot, update, preferred_element_type=jnp.float32)
        hidden = hidden + message * picked
    score = jnp.sum(hidden * head[...], axis=1, keepdims=True)
    potential = radius * (1.0 + jnp.tanh(score))
    pot[...] = to_rows(potential)
    final = 2 + layers
    scaled_out[...] = to_rows(weight * potential)

    @pl.loop(1, n_atom)
    def _(d):
        remote(
            scaled_out, near.at[n_atom + atom], sent.at[final], got.at[final],
            (grid, lax.rem(atom + d, n_atom)),
        )

    @pl.when(has_outer)
    def _():
        @pl.loop(0, n_atom)
        def _(d):
            remote(
                scaled_out, near.at[inner * n_atom + atom], sent.at[final + 1],
                got.at[final + 1 + side], (og, d),
            )

    @pl.loop(0, n_atom)
    def _(d):
        remote(
            scaled_out, near.at[outer * n_atom + atom], sent.at[final + 2],
            got.at[final + 2 - side], (ig, d),
        )

    send_psi(layers + 1)
    near[n_atom + atom] = scaled_out[...]
    wait_all(near, got.at[final], n_atom - 1)

    @pl.when(has_outer)
    def _():
        wait_all(near, got.at[final + 2 - side], n_atom)

    wait_all(near, got.at[final + 1 + side], n_atom)

    @pl.loop(0, n_atom)
    def _(q):
        at = pl.ds(q * nb, nb)
        wait_bytes(psi.at[inner, at], psi_got.at[inner, q])

        @pl.when(has_outer)
        def _():
            wait_bytes(psi.at[outer, at], psi_got.at[outer, q])

        @pl.when(q != atom)
        def _():
            wait_bytes(basis.at[1, q], chip_sent.at[q])

        for way in range(2):
            able = (
                jnp.logical_and(q <= atom, atom < n_atom - 1)
                if way == 0
                else jnp.logical_and(q >= atom, atom > 0)
            )

            @pl.when(able)
            def _():
                wait_bytes(basis.at[1, q], z_sent.at[0, way, q])

            @pl.when(jnp.logical_and(able, has_outer))
            def _():
                wait_bytes(basis.at[1, q], z_sent.at[1, way, q])

    @pl.when(has_outer)
    def _():
        wait_bytes(names, name_sent.at[0])
        wait_bytes(piece, v_sent.at[0])
        wait_bytes(part_out.at[0], part_sent.at[0])
        wait_bytes(psi.at[1], psi_sent.at[0])

    wait_bytes(names, name_sent.at[1])
    wait_bytes(piece, v_sent.at[1])
    wait_bytes(part_out.at[1], part_sent.at[1])
    wait_bytes(psi.at[1], psi_sent.at[1])

    @pl.when(relays)
    def _():
        wait_bytes(relay_v, v_passed.at[1])
        for phase in range(2):
            wait_bytes(relay.at[phase], relay_sent.at[phase])

    wait_all(dens_buf, sent.at[0], n_atom - 1)
    for k, held in enumerate([info_buf] + [rows_buf.at[layer] for layer in range(layers)]):
        wait_all(held, sent.at[1 + k], half - 1)
        wait_all(held, pair_sent.at[1 + k], half)
    wait_all(near, sent.at[final], n_atom - 1)
    wait_all(near, sent.at[final + 2], n_atom)

    @pl.when(has_outer)
    def _():
        wait_all(near, sent.at[final + 1], n_atom)


def exchange_of(shape, own, piece, names, atoms, weights, scale, shift, mw, aw, head):
    n_grid, n_atom = shape
    n = n_grid * n_atom
    nb, points, depth = piece.shape
    count = nb * n_atom
    width, columns = own.shape[1:]
    layers, features, _ = mw.shape
    packed = RUN * (features // LANES)
    bf16, f32 = jnp.bfloat16, jnp.float32
    dma = pltpu.SemaphoreType.DMA
    grant = 2 * own.size + 14 * count * points * columns + 6 * count * depth * points
    grant += n * (packed * LANES * (2 * layers + 8) + 12 * RUN * LANES) + (6 << 20)
    given = 6 * count * points * (columns + depth)
    if grant + given > 48 << 20:
        grant = 60 << 20
    return pl.pallas_call(
        functools.partial(exchange_kernel, shape, layers),
        out_shape=(
            jax.ShapeDtypeStruct((nb, points), f32),
            jax.ShapeDtypeStruct((3 * n_atom, nb, points), f32),
            jax.ShapeDtypeStruct((3, count, points, columns), bf16),
            jax.ShapeDtypeStruct((3, count, depth, points), bf16),
            jax.ShapeDtypeStruct((3, *names.shape), names.dtype),
        ),
        in_specs=[HBM] * 10,
        out_specs=(VMEM,) * 5,
        scratch_shapes=[
            pltpu.VMEM(a.shape, a.dtype) for a in (atoms, weights, scale, shift, mw, aw, head)
        ]
        + [
            pltpu.VMEM((own.shape[0] + 2, width, columns), bf16),
            pltpu.VMEM((3, n_atom, nb, points, depth), bf16),
            pltpu.SMEM((3, *names.shape), names.dtype),
            pltpu.VMEM((count, points, columns), f32),
            pltpu.VMEM((2, count, points, columns), bf16),
            pltpu.VMEM((2, count, points, columns), bf16),
            pltpu.VMEM((2, n_atom, nb // 2, points, columns), bf16),
            pltpu.VMEM((n_atom, nb, points), f32),
            pltpu.VMEM((n_atom, nb, points), f32),
            pltpu.VMEM((RUN, LANES), f32),
            pltpu.VMEM((n, RUN, LANES), f32),
            pltpu.VMEM((layers, packed, LANES), bf16),
            pltpu.VMEM((layers, n, packed, LANES), bf16),
            pltpu.VMEM((nb, points), f32),
            dma((10,)),
            dma((1,)),
            dma((2,)),
            dma((3,)),
            dma((2,)),
            dma((3, n_atom)),
            dma((2, 2, n_atom)),
            dma((n_atom,)),
            dma((2,)),
            dma((2, n_atom)),
            dma((2,)),
            dma((3, n_atom)),
            dma((2, n_atom)),
            dma((2,)),
            dma((5 + layers,)),
            dma((5 + layers,)),
            pltpu.VMEM((max(nb // 2, 1), points, depth), bf16),
            dma((2,)),
            dma((2 + layers,)),
            dma((2 + layers,)),
            dma((nb,)),
        ],
        compiler_params=pltpu.CompilerParams(
            collective_id=0, has_side_effects=True, vmem_limit_bytes=grant
        ),
        name="exchange_of",
    )(
        *(
            pltpu.with_memory_space_constraint(a, pltpu.HBM)
            for a in (own, piece, names, atoms, weights, scale, shift, mw, aw, head)
        )
    )


MANY = 6


def fock_kernel(names, basis_t, near, psi, pot, out, pot_out, filled, table, held, done):
    groups, count, depth, points = basis_t.shape
    owned, width, columns = out.shape
    picks = depth // width
    most = groups * count * picks
    tile = min(columns, TILE)
    first = lax.axis_index("grid") * owned
    last = pltpu.make_async_copy(pot, pot_out, done.at[owned])
    last.start()

    @pl.loop(0, owned + 2)
    def _(r):
        filled[r] = 0

    for k in range(groups):

        @pl.loop(0, count)
        def _(b):
            for j in range(picks):
                row = jnp.minimum(jnp.maximum(names[k, j, b] - first + 1, 0), owned + 1)
                n = filled[row]
                table[row * most + n] = (k * count + b) * picks + j
                filled[row] = n + 1

    @pl.loop(0, owned)
    def _(r):
        n = filled[r + 1]

        @pl.when(n == 0)
        def _():
            held[r] = jnp.zeros((width, columns), jnp.float32)

        def multiply(begin, many, first_time):
            parts, values = [], []
            for i in range(many):
                entry = table[(r + 1) * most + begin + i]
                s, j = entry // picks, lax.rem(entry, picks)
                k, b = s // count, lax.rem(s, count)
                part = basis_t[k, b, pl.ds(pl.multiple_of(j * width, width), width), :]
                parts.append(
                    (part.astype(jnp.float32) * near[pl.ds(s, 1), :]).astype(jnp.bfloat16)
                )
                values.append((k, b))
            left = jnp.concatenate(parts, axis=1)
            for c in range(columns // tile):
                at = pl.ds(c * tile, tile)
                right = jnp.concatenate([psi[k, b, :, at] for k, b in values], axis=0)
                value = jnp.dot(left, right, preferred_element_type=jnp.float32)
                if first_time:
                    held[r, :, at] = value
                else:
                    held[r, :, at] += value

        for many in range(1, MANY + 1):

            @pl.when(n == many if many < MANY else n >= many)
            def _():
                multiply(0, many, True)

        @pl.loop(MANY, jnp.maximum(n, MANY))
        def _(m):
            multiply(m, 1, False)

        pltpu.make_async_copy(held.at[r], out.at[r], done.at[r]).start()

    for r in range(owned):
        pltpu.make_async_copy(held.at[r], out.at[r], done.at[r]).wait()
    last.wait()


def fock_of(names, basis_t, near, psi, pot, owned):
    groups, count, depth, points = basis_t.shape
    columns = psi.shape[3]
    width = depth // names.shape[1]
    most = groups * depth // width * count
    return pl.pallas_call(
        fock_kernel,
        out_shape=(
            jax.ShapeDtypeStruct((owned, width, columns), jnp.float32),
            jax.ShapeDtypeStruct(pot.shape, pot.dtype),
        ),
        in_specs=[pl.BlockSpec(memory_space=pltpu.SMEM), VMEM, VMEM, VMEM, VMEM],
        out_specs=(HBM, HBM),
        scratch_shapes=[
            pltpu.SMEM((owned + 2,), jnp.int32),
            pltpu.SMEM(((owned + 2) * most,), jnp.int32),
            pltpu.VMEM((owned, width, columns), jnp.float32),
            pltpu.SemaphoreType.DMA((owned + 1,)),
        ],
        compiler_params=pltpu.CompilerParams(
            vmem_limit_bytes=4 * owned * width * columns + (8 << 20)
        ),
        name="fock_of",
    )(names, basis_t, near, psi, pot)


def local(
    basis_values,
    block_lists,
    orbitals,
    point_weights,
    point_atoms,
    embed_scale,
    embed_shift,
    message_weight,
    atom_weight,
    head_weight,
):
    n_grid, n_atom = lax.axis_size("grid"), lax.axis_size("atom")
    own_rows = orbitals.shape[0]
    batches, points, depth = basis_values.shape
    picks = block_lists.shape[1]
    owned = own_rows // (depth // picks)
    potential, near, psi, basis_t, names = exchange_of(
        (n_grid, n_atom),
        orbitals.reshape(owned, own_rows // owned, -1),
        basis_values,
        block_lists.T,
        point_atoms.reshape(batches, points),
        point_weights.reshape(batches, points),
        embed_scale[None, :],
        embed_shift[None, :],
        message_weight,
        atom_weight,
        head_weight[None, :],
    )
    fock, potential = fock_of(names, basis_t, near.reshape(-1, points), psi, potential, owned)
    return (fock.reshape(own_rows, -1), potential.reshape(-1))


def solution(mesh):
    return jax.shard_map(
        local,
        mesh=mesh,
        in_specs=(
            P(("grid", "atom"), None, None),
            P("grid", None),
            P("grid", "atom"),
            P(("grid", "atom")),
            P(("grid", "atom")),
            P(),
            P(),
            P(),
            P(),
            P(),
        ),
        out_specs=(P("grid", "atom"), P(("grid", "atom"))),
        check_vma=False,
    )
```

```python
import functools
import jax
import jax.numpy as jnp
from jax import lax
from jax.experimental import pallas as pl
from jax.experimental.pallas import tpu as pltpu
from jax.sharding import PartitionSpec as P

ATOM_DEV = 32
RUN = max(ATOM_DEV // 4, 1)
LANES = 128
VMEM = pl.BlockSpec(memory_space=pltpu.VMEM)
HBM = pl.BlockSpec(memory_space=pltpu.HBM)
MESH = pl.DeviceIdType.MESH
TILE = 256
PARTS = (2, 2, 2, 2)


def wait_bytes(ref, sem):
    pltpu.make_async_copy(ref, ref, sem).wait()


def meet_all(shape):
    n_grid, n_atom = shape
    n = n_grid * n_atom
    me = lax.axis_index("grid") * n_atom + lax.axis_index("atom")
    barrier = pltpu.get_barrier_semaphore()

    @pl.loop(1, n)
    def _(d):
        t = lax.rem(me + d, n)
        pl.semaphore_signal(
            barrier, inc=1, device_id=(t // n_atom, lax.rem(t, n_atom)), device_id_type=MESH
        )

    pl.semaphore_wait(barrier, n - 1)


def to_columns(rows):
    parts = [
        jnp.transpose(jnp.broadcast_to(rows[i : i + 1, :], (LANES, LANES)))
        for i in range(rows.shape[0])
    ]
    return jnp.concatenate(parts, axis=0)


def to_rows(columns):
    parts = []
    for i in range(columns.shape[0] // LANES):
        piece = jnp.broadcast_to(columns[i * LANES : (i + 1) * LANES, :], (LANES, LANES))
        parts.append(jnp.transpose(piece)[0:1, :])
    return jnp.concatenate(parts, axis=0)


def wrapped(values, total):
    values = jnp.where(values < 0.0, values + total, values)
    return jnp.where(values >= total, values - total, values)


def exchange_kernel(
    shape, layers, own, piece, names, *rest,
):
    given, rest = rest[:7], rest[7:]
    pot, near, psi, basis_t, all_names = rest[:5]
    atoms, weights, scale, shift, mw, aw, head = rest[5:12]
    (
        rows, basis, lists, acc, part_out, part_in, relay, dens, dens_buf,
        info, info_buf, rows_out, rows_buf, scaled_out,
        load, list_sem, name_sent, name_got, v_sent, v_got, z_sent, chip_sent,
        part_sent, part_got, psi_sent, psi_got, passed, relay_sent, sent, got,
        relay_v, v_passed, pair_sent, pair_got, v_first, word,
    ) = rest[12:]
    n_grid, n_atom = shape
    n = n_grid * n_atom
    grid, atom = lax.axis_index("grid"), lax.axis_index("atom")
    last, middle = n_grid - 1, n_grid // 2
    side = lax.rem(grid, 2)
    outer, inner = 2 * side, 2 - 2 * side
    og, ig = grid - 1 + 2 * side, grid + 1 - 2 * side
    has_outer = jnp.logical_and(og >= 0, og < n_grid)
    at_split = jnp.logical_or(grid == middle - 1, grid == middle)
    whole = jnp.logical_and(has_outer, jnp.logical_not(at_split))
    relays = jnp.logical_or(grid == 0, grid == last)
    relay_to = jnp.where(grid == middle, 0, last)
    forward_to = jnp.where(grid == 0, middle - 1, middle)

    nb, points, depth = piece.shape
    owned, width, columns = own.shape
    picks = depth // width
    tile = min(columns, TILE)
    relayed = nb // 2
    direct = nb - relayed

    def remote(source, target, send_sem, recv_sem, to):
        pltpu.make_async_remote_copy(
            src_ref=source,
            dst_ref=target,
            send_sem=send_sem,
            recv_sem=recv_sem,
            device_id=to,
            device_id_type=MESH,
        ).start()

    half = n // 2
    place_here = (grid // 2) * n_atom + atom
    slot_here = side * half + place_here

    def to_chips(source, held, k):
        @pl.loop(1, half)
        def _(d):
            t = lax.rem(place_here + d, half)
            remote(
                source, held.at[slot_here], sent.at[k], got.at[k],
                ((t // n_atom) * 2 + side, lax.rem(t, n_atom)),
            )

    def hand_over(held, k):
        wait_bytes(held.at[pl.ds(0, half - 1)], got.at[k])
        slab = held.at[pl.ds(side * half, half)]
        remote(slab, slab, pair_sent.at[k], pair_got.at[k], (ig, atom))
        wait_bytes(held.at[pl.ds(0, half)], pair_got.at[k])

    def wait_all(held, sem, count):
        wait_bytes(held.at[pl.ds(0, count)], sem)

    def visit(t):
        reach = jnp.minimum(atom, n_atom - 1 - atom)
        close = jnp.where(lax.rem(t, 2) == 1, atom - (t + 1) // 2, atom + t // 2)
        far = jnp.where(reach == atom, t, n_atom - 1 - t)
        return jnp.where(t <= 2 * reach, close, far)

    held_here = (
        rows.at[pl.ds(1, owned)], basis.at[1, atom], all_names.at[1],
        atoms, weights, scale, shift, mw, aw, head,
    )
    loads = [
        pltpu.make_async_copy(source, target, load.at[i])
        for i, (source, target) in enumerate(zip((own, piece, names, *given), held_here))
    ]
    for copy in loads:
        copy.start()
    early = n_atom <= 4

    def greet_near():
        barrier = pltpu.get_barrier_semaphore()

        def greet(able, g, a):
            @pl.when(able)
            def _():
                pl.semaphore_signal(barrier, inc=1, device_id=(g, a), device_id_type=MESH)

        greet(grid >= 0, ig, atom)
        greet(has_outer, og, atom)
        greet(atom > 0, grid, atom - 1)
        greet(atom < n_atom - 1, grid, atom + 1)
        for g in (0, last):
            greet(at_split, g, atom)
        for g in (middle - 1, middle):
            greet(relays, g, atom)
        met = 1 + has_outer.astype(jnp.int32) + (atom > 0).astype(jnp.int32)
        met = met + (atom < n_atom - 1).astype(jnp.int32)
        met = met + 2 * jnp.logical_or(at_split, relays).astype(jnp.int32)
        pl.semaphore_wait(barrier, met)

    def pass_word(t):
        for way, (step, when) in enumerate(((1, grid), (-1, last - grid))):
            behind = grid > 0 if way == 0 else grid < last
            ahead = grid < last if way == 0 else grid > 0
            now = t == when * n_atom // n_grid

            @pl.when(jnp.logical_and(now, behind))
            def _():
                pl.semaphore_wait(word.at[way], 1)

            @pl.when(jnp.logical_and(now, ahead))
            def _():
                pl.semaphore_signal(
                    word.at[way], inc=1, device_id=(grid + step, atom), device_id_type=MESH
                )

    if early:
        greet_near()
    else:
        meet_all(shape)

    @pl.when(has_outer)
    def _():
        remote(names, all_names.at[inner], name_sent.at[0], name_got.at[inner], (og, atom))

    for i in range(nb):
        target = basis.at[inner, atom, i]

        @pl.when(has_outer if i < direct else whole)
        def _():
            remote(piece.at[i], target, v_sent.at[0], v_first.at[i], (og, atom))

        if i >= direct:

            @pl.when(at_split)
            def _():
                remote(
                    piece.at[i], relay_v.at[i - direct], v_sent.at[0], v_passed.at[0],
                    (relay_to, atom),
                )

    remote(names, all_names.at[outer], name_sent.at[1], name_got.at[outer], (ig, atom))
    remote(piece, basis.at[outer, atom], v_sent.at[1], v_got.at[outer, atom], (ig, atom))

    @pl.when(atom < n_atom - 1)
    def _():
        remote(
            piece, basis.at[1, atom], z_sent.at[0, 0, atom], v_got.at[1, atom], (grid, atom + 1)
        )

    @pl.when(atom > 0)
    def _():
        remote(
            piece, basis.at[1, atom], z_sent.at[0, 1, atom], v_got.at[1, atom], (grid, atom - 1)
        )

    for copy in loads[1:5]:
        copy.wait()
    total = float(ATOM_DEV * n_atom)
    named = atoms[...].astype(jnp.float32)
    lead = named[0:1, 0:1]
    shifted = wrapped(named - lead + total / 2, total) - total / 2
    least = jnp.min(jnp.min(shifted, axis=1, keepdims=True), axis=0, keepdims=True)
    start = wrapped(lead + least, total)
    place = shifted - least
    lane = lax.broadcasted_iota(jnp.int32, (1, LANES), 1)
    mine = jnp.where(lane < RUN, wrapped(start + lane.astype(jnp.float32), total), -1.0)
    run = lax.broadcasted_iota(jnp.int32, (RUN, LANES), 0).astype(jnp.float32)
    mass = jnp.zeros((RUN, 1), jnp.float32)
    for i in range(nb):
        here = jnp.where(place[i : i + 1, :] == run, weights[i : i + 1, :], 0.0)
        mass = mass + jnp.sum(here, axis=1, keepdims=True)
    info[...] = jnp.where(
        lax.broadcasted_iota(jnp.int32, (RUN, LANES), 1) < LANES // 2,
        wrapped(start + run, total),
        mass,
    )
    info_buf[slot_here] = info[...]

    if relayed:

        @pl.when(relays)
        def _():
            wait_bytes(relay_v, v_passed.at[0])
            for i in range(direct, nb):
                remote(
                    relay_v.at[i - direct], basis.at[inner, atom, i], v_passed.at[1],
                    v_first.at[i], (forward_to, atom),
                )

    for edge in (0, owned + 1):
        rows[edge] = jnp.zeros((width, columns), rows.dtype)

    @pl.when(jnp.logical_not(has_outer))
    def _():
        all_names[outer] = jnp.full(names.shape, -1, names.dtype)
        part_in[0] = jnp.zeros(part_in.shape[1:], part_in.dtype)

    @pl.when(has_outer)
    def _():
        wait_bytes(names, name_got.at[outer])

    wait_bytes(names, name_got.at[inner])
    copy = pltpu.make_async_copy(all_names, lists, list_sem.at[0])
    copy.start()
    copy.wait()
    loads[0].wait()
    first = grid * owned

    def product(slot, q, i, keep):
        chosen = []
        for j in range(picks):
            block = lists[slot, j, q * nb + i] - first + 1
            chosen.append(jnp.minimum(jnp.maximum(block, 0), owned + 1))
        values = basis[slot, q, i]
        for c in range(columns // tile):
            at = pl.ds(c * tile, tile)
            held = jnp.concatenate(
                [rows[k, :, at] for k in chosen], axis=0
            )
            keep(at, jnp.dot(values, held, preferred_element_type=jnp.float32))

    def outward(phase, q, i, source, target, sent_sem, got_sem, near_by=True, far=True):
        if near_by:

            @pl.when(whole if i >= direct else has_outer)
            def _():
                remote(source, target, sent_sem, got_sem, (og, atom))

        if far and i >= direct:

            @pl.when(at_split)
            def _():
                remote(
                    source, relay.at[phase, q, i - direct], sent_sem, passed.at[phase, q],
                    (relay_to, atom),
                )

    def forward(phase, r):
        q = visit(r)

        @pl.when(relays)
        def _():
            held = relay.at[phase, q]
            wait_bytes(held, passed.at[phase, q])
            at = pl.ds(q * nb + direct, relayed)
            if phase == 0:
                target, got_sem = part_in.at[0, at], part_got.at[0, q]
            else:
                target, got_sem = psi.at[inner, at], psi_got.at[inner, q]
            remote(held, target, relay_sent.at[phase], got_sem, (forward_to, atom))

    def finish(t):
        q = visit(t)
        wait_bytes(part_in.at[1, pl.ds(q * nb, nb)], part_got.at[1, q])

        @pl.when(has_outer)
        def _():
            wait_bytes(part_in.at[0, pl.ds(q * nb, nb)], part_got.at[0, q])

        for i in range(nb):
            b = q * nb + i
            sums = jnp.zeros((points, LANES), jnp.float32)
            for c in range(columns // LANES):
                at = pl.ds(c * LANES, LANES)
                value = (
                    acc[b, :, at]
                    + part_in[0, b, :, at].astype(jnp.float32)
                    + part_in[1, b, :, at].astype(jnp.float32)
                )
                rounded = value.astype(jnp.bfloat16)
                psi[1, b, :, at] = rounded
                sums = sums + jnp.square(rounded.astype(jnp.float32))
            dens[q, i : i + 1, :] = jnp.sum(jnp.transpose(sums), axis=0, keepdims=True)

        @pl.when(q != atom)
        def _():
            remote(dens.at[q], dens_buf.at[atom], sent.at[0], got.at[0], (grid, q))

        at = pl.ds(q * nb, nb)
        remote(psi.at[1, at], psi.at[outer, at], psi_sent.at[1], psi_got.at[outer, q], (ig, atom))
        for i in range(nb):
            psi_outward(t, i, near_by=False)

    def psi_outward(r, i, **which):
        q = visit(r)
        b = q * nb + i
        outward(
            1, q, i, psi.at[1, b], psi.at[inner, b], psi_sent.at[0], psi_got.at[inner, q],
            **which,
        )

    def psi_unit(r, i):
        psi_outward(r, i, far=False)
        if i == nb - 1:
            forward(1, r)

    reach = jnp.minimum(atom, n_atom - 1 - atom)

    def along(stream, slot, q):
        for way in range(2):
            able = (
                jnp.logical_and(q <= atom, atom < n_atom - 1)
                if way == 0
                else jnp.logical_and(q >= atom, atom > 0)
            )

            @pl.when(able)
            def _():
                remote(
                    basis.at[slot, q], basis.at[slot, q], z_sent.at[stream, way, q],
                    v_got.at[slot, q], (grid, atom + 1 - 2 * way),
                )

    def spread_outer(t):
        q = visit(t)

        @pl.when(has_outer)
        def _():
            wait_bytes(basis.at[outer, q], v_got.at[outer, q])
            along(1, outer, q)

    def send_first():
        for i in range(nb):
            mine_first = basis.at[outer, atom, i]
            wait_bytes(mine_first, v_first.at[i])
            for way in range(2):

                @pl.when(atom < n_atom - 1 if way == 0 else atom > 0)
                def _():
                    remote(
                        mine_first, mine_first, z_sent.at[1, way, atom], v_got.at[outer, atom],
                        (grid, atom + 1 - 2 * way),
                    )

            outer_part(atom, i)

    def spread_own(t):
        q = visit(t)
        wait_bytes(basis.at[1, q], v_got.at[1, q])
        along(0, 1, q)
        remote(
            basis.at[1, q], basis.at[outer, q], chip_sent.at[q], v_got.at[outer, q], (ig, atom)
        )

    def outer_part(q, i):
        b = q * nb + i

        def keep(at, value):
            part_out[0, b, :, at] = value.astype(jnp.bfloat16)

        product(outer, q, i, keep)
        outward(
            0, q, i, part_out.at[0, b], part_in.at[0, b], part_sent.at[0], part_got.at[0, q]
        )

    def product_outer(q):
        for i in range(nb):
            outer_part(q, i)

    def products_here(q):
        wait_bytes(basis.at[inner, q], v_got.at[inner, q])
        for i in range(nb):
            b = q * nb + i

            def keep(at, value):
                part_out[1, b, :, at] = value.astype(jnp.bfloat16)

            product(inner, q, i, keep)
            remote(
                part_out.at[1, b], part_in.at[1, b], part_sent.at[1], part_got.at[1, q],
                (ig, atom),
            )

        for i in range(nb):
            b = q * nb + i

            def keep(at, value):
                acc[b, :, at] = value

            product(1, q, i, keep)
            for slot in range(3):
                basis_t[slot, b] = jnp.transpose(basis[slot, q, i])

    @pl.when(has_outer)
    def _():
        send_first()

    @pl.loop(0, n_atom)
    def _(t):
        q = visit(t)
        paired = jnp.logical_and(lax.rem(t, 2) == 1, t < 2 * reach)
        fresh = jnp.logical_and(
            t > 0, jnp.logical_or(lax.rem(t, 2) == 1, t > 2 * reach)
        )

        @pl.when(fresh)
        def _():
            spread_outer(t)

        @pl.when(paired)
        def _():
            spread_outer(t + 1)

        @pl.when(jnp.logical_and(t > 0, has_outer))
        def _():
            product_outer(q)

        @pl.when(t > 0)
        def _():
            products_here(visit(t - 1))

        @pl.when(fresh)
        def _():
            spread_own(t)

        @pl.when(paired)
        def _():
            spread_own(t + 1)

        @pl.when(t >= 1)
        def _():
            forward(0, t - 1)

        if early:
            pass_word(t)

        @pl.when(t >= 2)
        def _():
            finish(t - 2)

    ends = [sum(PARTS[: s + 1]) for s in range(len(PARTS))]

    def send_psi(s):
        for u in range(n_atom * nb):
            if sum(u * ends[-1] >= end * n_atom * nb for end in ends) == s:
                psi_unit(u // nb, u % nb)

    send_psi(0)
    products_here(visit(n_atom - 1))
    finish(n_atom - 2)
    weight = to_columns(weights[...])[:, 0:1]
    spot = to_columns(place)
    hot = (spot == lax.broadcasted_iota(jnp.int32, spot.shape, 1).astype(jnp.float32)).astype(
        jnp.bfloat16
    )
    deep = lax.broadcasted_iota(jnp.int32, (LANES, LANES), 0).astype(jnp.float32)
    hot_t = jnp.concatenate([place[i : i + 1, :] == deep for i in range(nb)], axis=1).astype(
        jnp.bfloat16
    )
    for copy in loads[5:]:
        copy.wait()
    halves = scale.shape[1] // LANES
    forward(0, n_atom - 1)
    finish(n_atom - 1)
    dens_buf[atom] = dens[atom]

    wait_all(dens_buf, got.at[0], n_atom - 1)
    to_chips(info, info_buf, 1)
    density = to_columns(2.0 * jnp.sum(dens_buf[...], axis=0))
    safe = jnp.where(density > 0.0, density, 1.0)
    radius = jnp.where(density > 0.0, jnp.exp(jnp.log(safe) * (1.0 / 3.0)), 0.0)[:, 0:1]
    hidden = jax.nn.silu(radius * scale[...] + shift[...])
    for layer in range(layers):
        message = jax.nn.silu(
            jnp.dot(hidden.astype(jnp.bfloat16), mw[layer], preferred_element_type=jnp.float32)
        )
        weighted = (weight * message).astype(jnp.bfloat16)
        part = jnp.dot(hot_t, weighted, preferred_element_type=jnp.float32)
        rows_out[layer] = jnp.concatenate(
            [part[0:RUN, h * LANES : (h + 1) * LANES] for h in range(halves)], axis=0
        ).astype(jnp.bfloat16)
        to_chips(rows_out.at[layer], rows_buf.at[layer], 2 + layer)
        rows_buf[layer, slot_here] = rows_out[layer]
        send_psi(1 + layer)
        if layer == 0:
            hand_over(info_buf, 1)
            facts = info_buf[...].reshape(n * RUN, LANES)
            same = (facts[:, 0:1] == mine).astype(jnp.float32)
            mass = jnp.sum(same * facts[:, LANES // 2 : LANES // 2 + 1], axis=0, keepdims=True)
            share = 1.0 / (1.0 + to_columns(mass)[:, 0:1])
            same = same.reshape(n, RUN, LANES)
            none = jnp.zeros_like(same)
            selects = []
            for h in range(halves):
                full = jnp.concatenate(
                    [same if k == h else none for k in range(halves)], axis=1
                ).reshape(n * RUN * halves, LANES)
                selects.append(jnp.transpose(full).astype(jnp.bfloat16))

        hand_over(rows_buf.at[layer], 2 + layer)
        held = rows_buf[layer].reshape(n * RUN * halves, LANES)
        summed = jnp.concatenate(
            [jnp.dot(pick, held, preferred_element_type=jnp.float32) for pick in selects], axis=1
        )
        update = jax.nn.silu(
            jnp.dot(
                (summed * share).astype(jnp.bfloat16), aw[layer],
                preferred_element_type=jnp.float32,
            )
        ).astype(jnp.bfloat16)
        picked = jnp.dot(hot, update, preferred_element_type=jnp.float32)
        hidden = hidden + message * picked
    score = jnp.sum(hidden * head[...], axis=1, keepdims=True)
    potential = radius * (1.0 + jnp.tanh(score))
    pot[...] = to_rows(potential)
    final = 2 + layers
    scaled_out[...] = to_rows(weight * potential)

    @pl.loop(1, n_atom)
    def _(d):
        remote(
            scaled_out, near.at[n_atom + atom], sent.at[final], got.at[final],
            (grid, lax.rem(atom + d, n_atom)),
        )

    @pl.when(has_outer)
    def _():
        @pl.loop(0, n_atom)
        def _(d):
            remote(
                scaled_out, near.at[inner * n_atom + atom], sent.at[final + 1],
                got.at[final + 1 + side], (og, d),
            )

    @pl.loop(0, n_atom)
    def _(d):
        remote(
            scaled_out, near.at[outer * n_atom + atom], sent.at[final + 2],
            got.at[final + 2 - side], (ig, d),
        )

    send_psi(layers + 1)
    near[n_atom + atom] = scaled_out[...]
    wait_all(near, got.at[final], n_atom - 1)

    @pl.when(has_outer)
    def _():
        wait_all(near, got.at[final + 2 - side], n_atom)

    wait_all(near, got.at[final + 1 + side], n_atom)

    @pl.loop(0, n_atom)
    def _(q):
        at = pl.ds(q * nb, nb)
        wait_bytes(psi.at[inner, at], psi_got.at[inner, q])

        @pl.when(has_outer)
        def _():
            wait_bytes(psi.at[outer, at], psi_got.at[outer, q])

        @pl.when(q != atom)
        def _():
            wait_bytes(basis.at[1, q], chip_sent.at[q])

        for way in range(2):
            able = (
                jnp.logical_and(q <= atom, atom < n_atom - 1)
                if way == 0
                else jnp.logical_and(q >= atom, atom > 0)
            )

            @pl.when(able)
            def _():
                wait_bytes(basis.at[1, q], z_sent.at[0, way, q])

            @pl.when(jnp.logical_and(able, has_outer))
            def _():
                wait_bytes(basis.at[1, q], z_sent.at[1, way, q])

    @pl.when(has_outer)
    def _():
        wait_bytes(names, name_sent.at[0])
        wait_bytes(piece, v_sent.at[0])
        wait_bytes(part_out.at[0], part_sent.at[0])
        wait_bytes(psi.at[1], psi_sent.at[0])

    wait_bytes(names, name_sent.at[1])
    wait_bytes(piece, v_sent.at[1])
    wait_bytes(part_out.at[1], part_sent.at[1])
    wait_bytes(psi.at[1], psi_sent.at[1])

    @pl.when(relays)
    def _():
        wait_bytes(relay_v, v_passed.at[1])
        for phase in range(2):
            wait_bytes(relay.at[phase], relay_sent.at[phase])

    wait_all(dens_buf, sent.at[0], n_atom - 1)
    for k, held in enumerate([info_buf] + [rows_buf.at[layer] for layer in range(layers)]):
        wait_all(held, sent.at[1 + k], half - 1)
        wait_all(held, pair_sent.at[1 + k], half)
    wait_all(near, sent.at[final], n_atom - 1)
    wait_all(near, sent.at[final + 2], n_atom)

    @pl.when(has_outer)
    def _():
        wait_all(near, sent.at[final + 1], n_atom)


def exchange_of(shape, own, piece, names, atoms, weights, scale, shift, mw, aw, head):
    n_grid, n_atom = shape
    n = n_grid * n_atom
    nb, points, depth = piece.shape
    count = nb * n_atom
    width, columns = own.shape[1:]
    layers, features, _ = mw.shape
    packed = RUN * (features // LANES)
    bf16, f32 = jnp.bfloat16, jnp.float32
    dma = pltpu.SemaphoreType.DMA
    grant = 2 * own.size + 14 * count * points * columns + 6 * count * depth * points
    grant += n * (packed * LANES * (2 * layers + 8) + 12 * RUN * LANES) + (6 << 20)
    given = 6 * count * points * (columns + depth)
    if grant + given > 48 << 20:
        grant = 60 << 20
    return pl.pallas_call(
        functools.partial(exchange_kernel, shape, layers),
        out_shape=(
            jax.ShapeDtypeStruct((nb, points), f32),
            jax.ShapeDtypeStruct((3 * n_atom, nb, points), f32),
            jax.ShapeDtypeStruct((3, count, points, columns), bf16),
            jax.ShapeDtypeStruct((3, count, depth, points), bf16),
            jax.ShapeDtypeStruct((3, *names.shape), names.dtype),
        ),
        in_specs=[HBM] * 10,
        out_specs=(VMEM,) * 5,
        scratch_shapes=[
            pltpu.VMEM(a.shape, a.dtype) for a in (atoms, weights, scale, shift, mw, aw, head)
        ]
        + [
            pltpu.VMEM((own.shape[0] + 2, width, columns), bf16),
            pltpu.VMEM((3, n_atom, nb, points, depth), bf16),
            pltpu.SMEM((3, *names.shape), names.dtype),
            pltpu.VMEM((count, points, columns), f32),
            pltpu.VMEM((2, count, points, columns), bf16),
            pltpu.VMEM((2, count, points, columns), bf16),
            pltpu.VMEM((2, n_atom, nb // 2, points, columns), bf16),
            pltpu.VMEM((n_atom, nb, points), f32),
            pltpu.VMEM((n_atom, nb, points), f32),
            pltpu.VMEM((RUN, LANES), f32),
            pltpu.VMEM((n, RUN, LANES), f32),
            pltpu.VMEM((layers, packed, LANES), bf16),
            pltpu.VMEM((layers, n, packed, LANES), bf16),
            pltpu.VMEM((nb, points), f32),
            dma((10,)),
            dma((1,)),
            dma((2,)),
            dma((3,)),
            dma((2,)),
            dma((3, n_atom)),
            dma((2, 2, n_atom)),
            dma((n_atom,)),
            dma((2,)),
            dma((2, n_atom)),
            dma((2,)),
            dma((3, n_atom)),
            dma((2, n_atom)),
            dma((2,)),
            dma((5 + layers,)),
            dma((5 + layers,)),
            pltpu.VMEM((max(nb // 2, 1), points, depth), bf16),
            dma((2,)),
            dma((2 + layers,)),
            dma((2 + layers,)),
            dma((nb,)),
            pltpu.SemaphoreType.REGULAR((2,)),
        ],
        compiler_params=pltpu.CompilerParams(
            collective_id=0, has_side_effects=True, vmem_limit_bytes=grant
        ),
        name="exchange_of",
    )(
        *(
            pltpu.with_memory_space_constraint(a, pltpu.HBM)
            for a in (own, piece, names, atoms, weights, scale, shift, mw, aw, head)
        )
    )


MANY = 6


def fock_kernel(names, basis_t, near, psi, pot, out, pot_out, filled, table, held, done):
    groups, count, depth, points = basis_t.shape
    owned, width, columns = out.shape
    picks = depth // width
    most = groups * count * picks
    tile = min(columns, TILE)
    first = lax.axis_index("grid") * owned
    last = pltpu.make_async_copy(pot, pot_out, done.at[owned])
    last.start()

    @pl.loop(0, owned + 2)
    def _(r):
        filled[r] = 0

    for k in range(groups):

        @pl.loop(0, count)
        def _(b):
            for j in range(picks):
                row = jnp.minimum(jnp.maximum(names[k, j, b] - first + 1, 0), owned + 1)
                n = filled[row]
                table[row * most + n] = (k * count + b) * picks + j
                filled[row] = n + 1

    @pl.loop(0, owned)
    def _(r):
        n = filled[r + 1]

        @pl.when(n == 0)
        def _():
            held[r] = jnp.zeros((width, columns), jnp.float32)

        def multiply(begin, many, first_time):
            parts, values = [], []
            for i in range(many):
                entry = table[(r + 1) * most + begin + i]
                s, j = entry // picks, lax.rem(entry, picks)
                k, b = s // count, lax.rem(s, count)
                part = basis_t[k, b, pl.ds(pl.multiple_of(j * width, width), width), :]
                parts.append(
                    (part.astype(jnp.float32) * near[pl.ds(s, 1), :]).astype(jnp.bfloat16)
                )
                values.append((k, b))
            left = jnp.concatenate(parts, axis=1)
            for c in range(columns // tile):
                at = pl.ds(c * tile, tile)
                right = jnp.concatenate([psi[k, b, :, at] for k, b in values], axis=0)
                value = jnp.dot(left, right, preferred_element_type=jnp.float32)
                if first_time:
                    held[r, :, at] = value
                else:
                    held[r, :, at] += value

        for many in range(1, MANY + 1):

            @pl.when(n == many if many < MANY else n >= many)
            def _():
                multiply(0, many, True)

        @pl.loop(MANY, jnp.maximum(n, MANY))
        def _(m):
            multiply(m, 1, False)

        pltpu.make_async_copy(held.at[r], out.at[r], done.at[r]).start()

    for r in range(owned):
        pltpu.make_async_copy(held.at[r], out.at[r], done.at[r]).wait()
    last.wait()


def fock_of(names, basis_t, near, psi, pot, owned):
    groups, count, depth, points = basis_t.shape
    columns = psi.shape[3]
    width = depth // names.shape[1]
    most = groups * depth // width * count
    return pl.pallas_call(
        fock_kernel,
        out_shape=(
            jax.ShapeDtypeStruct((owned, width, columns), jnp.float32),
            jax.ShapeDtypeStruct(pot.shape, pot.dtype),
        ),
        in_specs=[pl.BlockSpec(memory_space=pltpu.SMEM), VMEM, VMEM, VMEM, VMEM],
        out_specs=(HBM, HBM),
        scratch_shapes=[
            pltpu.SMEM((owned + 2,), jnp.int32),
            pltpu.SMEM(((owned + 2) * most,), jnp.int32),
            pltpu.VMEM((owned, width, columns), jnp.float32),
            pltpu.SemaphoreType.DMA((owned + 1,)),
        ],
        compiler_params=pltpu.CompilerParams(
            vmem_limit_bytes=4 * owned * width * columns + (8 << 20)
        ),
        name="fock_of",
    )(names, basis_t, near, psi, pot)


def local(
    basis_values,
    block_lists,
    orbitals,
    point_weights,
    point_atoms,
    embed_scale,
    embed_shift,
    message_weight,
    atom_weight,
    head_weight,
):
    n_grid, n_atom = lax.axis_size("grid"), lax.axis_size("atom")
    own_rows = orbitals.shape[0]
    batches, points, depth = basis_values.shape
    picks = block_lists.shape[1]
    owned = own_rows // (depth // picks)
    potential, near, psi, basis_t, names = exchange_of(
        (n_grid, n_atom),
        orbitals.reshape(owned, own_rows // owned, -1),
        basis_values,
        block_lists.T,
        point_atoms.reshape(batches, points),
        point_weights.reshape(batches, points),
        embed_scale[None, :],
        embed_shift[None, :],
        message_weight,
        atom_weight,
        head_weight[None, :],
    )
    fock, potential = fock_of(names, basis_t, near.reshape(-1, points), psi, potential, owned)
    return (fock.reshape(own_rows, -1), potential.reshape(-1))


def solution(mesh):
    return jax.shard_map(
        local,
        mesh=mesh,
        in_specs=(
            P(("grid", "atom"), None, None),
            P("grid", None),
            P("grid", "atom"),
            P(("grid", "atom")),
            P(("grid", "atom")),
            P(),
            P(),
            P(),
            P(),
            P(),
        ),
        out_specs=(P("grid", "atom"), P(("grid", "atom"))),
        check_vma=False,
    )
```

```python
import functools
import jax
import jax.numpy as jnp
from jax import lax
from jax.experimental import pallas as pl
from jax.experimental.pallas import tpu as pltpu
from jax.sharding import PartitionSpec as P

ATOM_DEV = 32
RUN = max(ATOM_DEV // 4, 1)
LANES = 128
VMEM = pl.BlockSpec(memory_space=pltpu.VMEM)
HBM = pl.BlockSpec(memory_space=pltpu.HBM)
MESH = pl.DeviceIdType.MESH
TILE = 256
PARTS = (2, 2, 2, 2)


def wait_bytes(ref, sem):
    pltpu.make_async_copy(ref, ref, sem).wait()


def meet_all(shape):
    n_grid, n_atom = shape
    n = n_grid * n_atom
    me = lax.axis_index("grid") * n_atom + lax.axis_index("atom")
    barrier = pltpu.get_barrier_semaphore()

    @pl.loop(1, n)
    def _(d):
        t = lax.rem(me + d, n)
        pl.semaphore_signal(
            barrier, inc=1, device_id=(t // n_atom, lax.rem(t, n_atom)), device_id_type=MESH
        )

    pl.semaphore_wait(barrier, n - 1)


def to_columns(rows):
    parts = [
        jnp.transpose(jnp.broadcast_to(rows[i : i + 1, :], (LANES, LANES)))
        for i in range(rows.shape[0])
    ]
    return jnp.concatenate(parts, axis=0)


def to_rows(columns):
    parts = []
    for i in range(columns.shape[0] // LANES):
        piece = jnp.broadcast_to(columns[i * LANES : (i + 1) * LANES, :], (LANES, LANES))
        parts.append(jnp.transpose(piece)[0:1, :])
    return jnp.concatenate(parts, axis=0)


def wrapped(values, total):
    values = jnp.where(values < 0.0, values + total, values)
    return jnp.where(values >= total, values - total, values)


def exchange_kernel(
    shape, layers, own, piece, names, *rest,
):
    given, rest = rest[:7], rest[7:]
    pot, near, psi, basis_t, all_names = rest[:5]
    atoms, weights, scale, shift, mw, aw, head = rest[5:12]
    (
        rows, basis, lists, acc, part_out, part_in, relay, dens, dens_buf,
        info, info_buf, rows_out, rows_buf, scaled_out,
        load, list_sem, name_sent, name_got, v_sent, v_got, z_sent, chip_sent,
        part_sent, part_got, psi_sent, psi_got, passed, relay_sent, sent, got,
        relay_v, v_passed, pair_sent, pair_got, v_first, word,
    ) = rest[12:]
    n_grid, n_atom = shape
    n = n_grid * n_atom
    grid, atom = lax.axis_index("grid"), lax.axis_index("atom")
    last, middle = n_grid - 1, n_grid // 2
    side = lax.rem(grid, 2)
    outer, inner = 2 * side, 2 - 2 * side
    og, ig = grid - 1 + 2 * side, grid + 1 - 2 * side
    has_outer = jnp.logical_and(og >= 0, og < n_grid)
    at_split = jnp.logical_or(grid == middle - 1, grid == middle)
    whole = jnp.logical_and(has_outer, jnp.logical_not(at_split))
    relays = jnp.logical_or(grid == 0, grid == last)
    relay_to = jnp.where(grid == middle, 0, last)
    forward_to = jnp.where(grid == 0, middle - 1, middle)

    nb, points, depth = piece.shape
    owned, width, columns = own.shape
    picks = depth // width
    tile = min(columns, TILE)
    relayed = nb // 2
    direct = nb - relayed

    def remote(source, target, send_sem, recv_sem, to):
        pltpu.make_async_remote_copy(
            src_ref=source,
            dst_ref=target,
            send_sem=send_sem,
            recv_sem=recv_sem,
            device_id=to,
            device_id_type=MESH,
        ).start()

    half = n // 2
    place_here = (grid // 2) * n_atom + atom
    slot_here = side * half + place_here

    def to_chips(source, held, k):
        @pl.loop(1, half)
        def _(d):
            t = lax.rem(place_here + d, half)
            remote(
                source, held.at[slot_here], sent.at[k], got.at[k],
                ((t // n_atom) * 2 + side, lax.rem(t, n_atom)),
            )

    def hand_over(held, k):
        wait_bytes(held.at[pl.ds(0, half - 1)], got.at[k])
        slab = held.at[pl.ds(side * half, half)]
        remote(slab, slab, pair_sent.at[k], pair_got.at[k], (ig, atom))
        wait_bytes(held.at[pl.ds(0, half)], pair_got.at[k])

    def wait_all(held, sem, count):
        wait_bytes(held.at[pl.ds(0, count)], sem)

    def visit(t):
        reach = jnp.minimum(atom, n_atom - 1 - atom)
        close = jnp.where(lax.rem(t, 2) == 1, atom - (t + 1) // 2, atom + t // 2)
        far = jnp.where(reach == atom, t, n_atom - 1 - t)
        return jnp.where(t <= 2 * reach, close, far)

    held_here = (
        rows.at[pl.ds(1, owned)], basis.at[1, atom], all_names.at[1],
        atoms, weights, scale, shift, mw, aw, head,
    )
    loads = [
        pltpu.make_async_copy(source, target, load.at[i])
        for i, (source, target) in enumerate(zip((own, piece, names, *given), held_here))
    ]
    for copy in loads:
        copy.start()
    early = n_atom <= 4

    def greet_near():
        barrier = pltpu.get_barrier_semaphore()

        def greet(able, g, a):
            @pl.when(able)
            def _():
                pl.semaphore_signal(barrier, inc=1, device_id=(g, a), device_id_type=MESH)

        greet(grid >= 0, ig, atom)
        greet(has_outer, og, atom)
        greet(atom > 0, grid, atom - 1)
        greet(atom < n_atom - 1, grid, atom + 1)
        for g in (0, last):
            greet(at_split, g, atom)
        for g in (middle - 1, middle):
            greet(relays, g, atom)
        met = 1 + has_outer.astype(jnp.int32) + (atom > 0).astype(jnp.int32)
        met = met + (atom < n_atom - 1).astype(jnp.int32)
        met = met + 2 * jnp.logical_or(at_split, relays).astype(jnp.int32)
        pl.semaphore_wait(barrier, met)

    def pass_word(t):
        for way, (step, when) in enumerate(((1, grid), (-1, last - grid))):
            behind = grid > 0 if way == 0 else grid < last
            ahead = grid < last if way == 0 else grid > 0
            now = t == when * n_atom // n_grid

            @pl.when(jnp.logical_and(now, behind))
            def _():
                pl.semaphore_wait(word.at[way], 1)

            @pl.when(jnp.logical_and(now, ahead))
            def _():
                pl.semaphore_signal(
                    word.at[way], inc=1, device_id=(grid + step, atom), device_id_type=MESH
                )

    if early:
        greet_near()
    else:
        meet_all(shape)

    @pl.when(has_outer)
    def _():
        remote(names, all_names.at[inner], name_sent.at[0], name_got.at[inner], (og, atom))

    for i in range(nb):
        target = basis.at[inner, atom, i]

        @pl.when(has_outer if i < direct else whole)
        def _():
            remote(piece.at[i], target, v_sent.at[0], v_first.at[i], (og, atom))

        if i >= direct:

            @pl.when(at_split)
            def _():
                remote(
                    piece.at[i], relay_v.at[i - direct], v_sent.at[0], v_passed.at[0],
                    (relay_to, atom),
                )

    remote(names, all_names.at[outer], name_sent.at[1], name_got.at[outer], (ig, atom))
    remote(piece, basis.at[outer, atom], v_sent.at[1], v_got.at[outer, atom], (ig, atom))

    @pl.when(atom < n_atom - 1)
    def _():
        remote(
            piece, basis.at[1, atom], z_sent.at[0, 0, atom], v_got.at[1, atom], (grid, atom + 1)
        )

    @pl.when(atom > 0)
    def _():
        remote(
            piece, basis.at[1, atom], z_sent.at[0, 1, atom], v_got.at[1, atom], (grid, atom - 1)
        )

    for copy in loads[1:5]:
        copy.wait()
    total = float(ATOM_DEV * n_atom)
    named = atoms[...].astype(jnp.float32)
    lead = named[0:1, 0:1]
    shifted = wrapped(named - lead + total / 2, total) - total / 2
    least = jnp.min(jnp.min(shifted, axis=1, keepdims=True), axis=0, keepdims=True)
    start = wrapped(lead + least, total)
    place = shifted - least
    lane = lax.broadcasted_iota(jnp.int32, (1, LANES), 1)
    mine = jnp.where(lane < RUN, wrapped(start + lane.astype(jnp.float32), total), -1.0)
    run = lax.broadcasted_iota(jnp.int32, (RUN, LANES), 0).astype(jnp.float32)
    mass = jnp.zeros((RUN, 1), jnp.float32)
    for i in range(nb):
        here = jnp.where(place[i : i + 1, :] == run, weights[i : i + 1, :], 0.0)
        mass = mass + jnp.sum(here, axis=1, keepdims=True)
    own_lane = lax.broadcasted_iota(jnp.int32, (RUN, LANES), 1).astype(jnp.float32)
    masses = jnp.sum(jnp.where(own_lane == run + LANES // 2, mass, 0.0), axis=0, keepdims=True)
    info[...] = jnp.where(lane < LANES // 2, mine, masses)
    info_buf[slot_here] = info[...]

    if relayed:

        @pl.when(relays)
        def _():
            wait_bytes(relay_v, v_passed.at[0])
            for i in range(direct, nb):
                remote(
                    relay_v.at[i - direct], basis.at[inner, atom, i], v_passed.at[1],
                    v_first.at[i], (forward_to, atom),
                )

    for edge in (0, owned + 1):
        rows[edge] = jnp.zeros((width, columns), rows.dtype)

    @pl.when(jnp.logical_not(has_outer))
    def _():
        all_names[outer] = jnp.full(names.shape, -1, names.dtype)
        part_in[0] = jnp.zeros(part_in.shape[1:], part_in.dtype)

    @pl.when(has_outer)
    def _():
        wait_bytes(names, name_got.at[outer])

    wait_bytes(names, name_got.at[inner])
    copy = pltpu.make_async_copy(all_names, lists, list_sem.at[0])
    copy.start()
    copy.wait()
    loads[0].wait()
    first = grid * owned

    def product(slot, q, i, keep):
        chosen = []
        for j in range(picks):
            block = lists[slot, j, q * nb + i] - first + 1
            chosen.append(jnp.minimum(jnp.maximum(block, 0), owned + 1))
        values = basis[slot, q, i]
        for c in range(columns // tile):
            at = pl.ds(c * tile, tile)
            held = jnp.concatenate(
                [rows[k, :, at] for k in chosen], axis=0
            )
            keep(at, jnp.dot(values, held, preferred_element_type=jnp.float32))

    def outward(phase, q, i, source, target, sent_sem, got_sem, near_by=True, far=True):
        if near_by:

            @pl.when(whole if i >= direct else has_outer)
            def _():
                remote(source, target, sent_sem, got_sem, (og, atom))

        if far and i >= direct:

            @pl.when(at_split)
            def _():
                remote(
                    source, relay.at[phase, q, i - direct], sent_sem, passed.at[phase, q],
                    (relay_to, atom),
                )

    def forward(phase, r):
        q = visit(r)

        @pl.when(relays)
        def _():
            held = relay.at[phase, q]
            wait_bytes(held, passed.at[phase, q])
            at = pl.ds(q * nb + direct, relayed)
            if phase == 0:
                target, got_sem = part_in.at[0, at], part_got.at[0, q]
            else:
                target, got_sem = psi.at[inner, at], psi_got.at[inner, q]
            remote(held, target, relay_sent.at[phase], got_sem, (forward_to, atom))

    def finish(t):
        q = visit(t)
        wait_bytes(part_in.at[1, pl.ds(q * nb, nb)], part_got.at[1, q])

        @pl.when(has_outer)
        def _():
            wait_bytes(part_in.at[0, pl.ds(q * nb, nb)], part_got.at[0, q])

        for i in range(nb):
            b = q * nb + i
            sums = jnp.zeros((points, LANES), jnp.float32)
            for c in range(columns // LANES):
                at = pl.ds(c * LANES, LANES)
                value = (
                    acc[b, :, at]
                    + part_in[0, b, :, at].astype(jnp.float32)
                    + part_in[1, b, :, at].astype(jnp.float32)
                )
                rounded = value.astype(jnp.bfloat16)
                psi[1, b, :, at] = rounded
                sums = sums + jnp.square(rounded.astype(jnp.float32))
            dens[q, i : i + 1, :] = jnp.sum(jnp.transpose(sums), axis=0, keepdims=True)

        @pl.when(q != atom)
        def _():
            remote(dens.at[q], dens_buf.at[atom], sent.at[0], got.at[0], (grid, q))

        at = pl.ds(q * nb, nb)
        remote(psi.at[1, at], psi.at[outer, at], psi_sent.at[1], psi_got.at[outer, q], (ig, atom))
        for i in range(nb):
            psi_outward(t, i, near_by=False)

    def psi_outward(r, i, **which):
        q = visit(r)
        b = q * nb + i
        outward(
            1, q, i, psi.at[1, b], psi.at[inner, b], psi_sent.at[0], psi_got.at[inner, q],
            **which,
        )

    def psi_unit(r, i):
        psi_outward(r, i, far=False)
        if i == nb - 1:
            forward(1, r)

    reach = jnp.minimum(atom, n_atom - 1 - atom)

    def along(stream, slot, q):
        for way in range(2):
            able = (
                jnp.logical_and(q <= atom, atom < n_atom - 1)
                if way == 0
                else jnp.logical_and(q >= atom, atom > 0)
            )

            @pl.when(able)
            def _():
                remote(
                    basis.at[slot, q], basis.at[slot, q], z_sent.at[stream, way, q],
                    v_got.at[slot, q], (grid, atom + 1 - 2 * way),
                )

    def spread_outer(t):
        q = visit(t)

        @pl.when(has_outer)
        def _():
            wait_bytes(basis.at[outer, q], v_got.at[outer, q])
            along(1, outer, q)

    def send_first():
        for i in range(nb):
            mine_first = basis.at[outer, atom, i]
            wait_bytes(mine_first, v_first.at[i])
            for way in range(2):

                @pl.when(atom < n_atom - 1 if way == 0 else atom > 0)
                def _():
                    remote(
                        mine_first, mine_first, z_sent.at[1, way, atom], v_got.at[outer, atom],
                        (grid, atom + 1 - 2 * way),
                    )

            outer_part(atom, i)

    def spread_own(t):
        q = visit(t)
        wait_bytes(basis.at[1, q], v_got.at[1, q])
        along(0, 1, q)
        remote(
            basis.at[1, q], basis.at[outer, q], chip_sent.at[q], v_got.at[outer, q], (ig, atom)
        )

    def outer_part(q, i):
        b = q * nb + i

        def keep(at, value):
            part_out[0, b, :, at] = value.astype(jnp.bfloat16)

        product(outer, q, i, keep)
        outward(
            0, q, i, part_out.at[0, b], part_in.at[0, b], part_sent.at[0], part_got.at[0, q]
        )

    def product_outer(q):
        for i in range(nb):
            outer_part(q, i)

    def products_here(q):
        wait_bytes(basis.at[inner, q], v_got.at[inner, q])
        for i in range(nb):
            b = q * nb + i

            def keep(at, value):
                part_out[1, b, :, at] = value.astype(jnp.bfloat16)

            product(inner, q, i, keep)
            remote(
                part_out.at[1, b], part_in.at[1, b], part_sent.at[1], part_got.at[1, q],
                (ig, atom),
            )

        for i in range(nb):
            b = q * nb + i

            def keep(at, value):
                acc[b, :, at] = value

            product(1, q, i, keep)
            for slot in range(3):
                basis_t[slot, b] = jnp.transpose(basis[slot, q, i])

    @pl.when(has_outer)
    def _():
        send_first()

    @pl.loop(0, n_atom)
    def _(t):
        q = visit(t)
        paired = jnp.logical_and(lax.rem(t, 2) == 1, t < 2 * reach)
        fresh = jnp.logical_and(
            t > 0, jnp.logical_or(lax.rem(t, 2) == 1, t > 2 * reach)
        )

        @pl.when(fresh)
        def _():
            spread_outer(t)

        @pl.when(paired)
        def _():
            spread_outer(t + 1)

        @pl.when(jnp.logical_and(t > 0, has_outer))
        def _():
            product_outer(q)

        @pl.when(t > 0)
        def _():
            products_here(visit(t - 1))

        @pl.when(fresh)
        def _():
            spread_own(t)

        @pl.when(paired)
        def _():
            spread_own(t + 1)

        @pl.when(t >= 1)
        def _():
            forward(0, t - 1)

        if early:
            pass_word(t)

        @pl.when(t >= 2)
        def _():
            finish(t - 2)

    ends = [sum(PARTS[: s + 1]) for s in range(len(PARTS))]

    def send_psi(s):
        for u in range(n_atom * nb):
            if sum(u * ends[-1] >= end * n_atom * nb for end in ends) == s:
                psi_unit(u // nb, u % nb)

    send_psi(0)
    products_here(visit(n_atom - 1))
    finish(n_atom - 2)
    weight = to_columns(weights[...])[:, 0:1]
    spot = to_columns(place)
    hot = (spot == lax.broadcasted_iota(jnp.int32, spot.shape, 1).astype(jnp.float32)).astype(
        jnp.bfloat16
    )
    deep = lax.broadcasted_iota(jnp.int32, (LANES, LANES), 0).astype(jnp.float32)
    hot_t = jnp.concatenate([place[i : i + 1, :] == deep for i in range(nb)], axis=1).astype(
        jnp.bfloat16
    )
    for copy in loads[5:]:
        copy.wait()
    halves = scale.shape[1] // LANES
    forward(0, n_atom - 1)
    finish(n_atom - 1)
    dens_buf[atom] = dens[atom]

    wait_all(dens_buf, got.at[0], n_atom - 1)
    to_chips(info, info_buf, 1)
    density = to_columns(2.0 * jnp.sum(dens_buf[...], axis=0))
    safe = jnp.where(density > 0.0, density, 1.0)
    radius = jnp.where(density > 0.0, jnp.exp(jnp.log(safe) * (1.0 / 3.0)), 0.0)[:, 0:1]
    hidden = jax.nn.silu(radius * scale[...] + shift[...])
    for layer in range(layers):
        message = jax.nn.silu(
            jnp.dot(hidden.astype(jnp.bfloat16), mw[layer], preferred_element_type=jnp.float32)
        )
        weighted = (weight * message).astype(jnp.bfloat16)
        part = jnp.dot(hot_t, weighted, preferred_element_type=jnp.float32)
        rows_out[layer] = jnp.concatenate(
            [part[0:RUN, h * LANES : (h + 1) * LANES] for h in range(halves)], axis=0
        ).astype(jnp.bfloat16)
        to_chips(rows_out.at[layer], rows_buf.at[layer], 2 + layer)
        rows_buf[layer, slot_here] = rows_out[layer]
        send_psi(1 + layer)
        if layer == 0:
            hand_over(info_buf, 1)
            facts = jnp.broadcast_to(info_buf[...], (n, RUN, LANES)).reshape(n * RUN, LANES)
            row = lax.rem(lax.broadcasted_iota(jnp.int32, (n * RUN, LANES), 0), RUN)
            lanes = lax.broadcasted_iota(jnp.int32, (n * RUN, LANES), 1)
            named = jnp.sum(jnp.where(lanes == row, facts, 0.0), axis=1, keepdims=True)
            held_mass = jnp.where(lanes == row + LANES // 2, facts, 0.0)
            same = (named == mine).astype(jnp.float32)
            held_mass = jnp.sum(held_mass, axis=1, keepdims=True)
            mass = jnp.sum(same * held_mass, axis=0, keepdims=True)
            share = 1.0 / (1.0 + to_columns(mass)[:, 0:1])
            same = same.reshape(n, RUN, LANES)
            none = jnp.zeros_like(same)
            selects = []
            for h in range(halves):
                full = jnp.concatenate(
                    [same if k == h else none for k in range(halves)], axis=1
                ).reshape(n * RUN * halves, LANES)
                selects.append(jnp.transpose(full).astype(jnp.bfloat16))

        hand_over(rows_buf.at[layer], 2 + layer)
        held = rows_buf[layer].reshape(n * RUN * halves, LANES)
        summed = jnp.concatenate(
            [jnp.dot(pick, held, preferred_element_type=jnp.float32) for pick in selects], axis=1
        )
        update = jax.nn.silu(
            jnp.dot(
                (summed * share).astype(jnp.bfloat16), aw[layer],
                preferred_element_type=jnp.float32,
            )
        ).astype(jnp.bfloat16)
        picked = jnp.dot(hot, update, preferred_element_type=jnp.float32)
        hidden = hidden + message * picked
    score = jnp.sum(hidden * head[...], axis=1, keepdims=True)
    potential = radius * (1.0 + jnp.tanh(score))
    pot[...] = to_rows(potential)
    final = 2 + layers
    scaled_out[...] = to_rows(weight * potential)

    @pl.loop(1, n_atom)
    def _(d):
        remote(
            scaled_out, near.at[n_atom + atom], sent.at[final], got.at[final],
            (grid, lax.rem(atom + d, n_atom)),
        )

    @pl.when(has_outer)
    def _():
        @pl.loop(0, n_atom)
        def _(d):
            remote(
                scaled_out, near.at[inner * n_atom + atom], sent.at[final + 1],
                got.at[final + 1 + side], (og, d),
            )

    @pl.loop(0, n_atom)
    def _(d):
        remote(
            scaled_out, near.at[outer * n_atom + atom], sent.at[final + 2],
            got.at[final + 2 - side], (ig, d),
        )

    send_psi(layers + 1)
    near[n_atom + atom] = scaled_out[...]
    wait_all(near, got.at[final], n_atom - 1)

    @pl.when(has_outer)
    def _():
        wait_all(near, got.at[final + 2 - side], n_atom)

    wait_all(near, got.at[final + 1 + side], n_atom)

    @pl.loop(0, n_atom)
    def _(q):
        at = pl.ds(q * nb, nb)
        wait_bytes(psi.at[inner, at], psi_got.at[inner, q])

        @pl.when(has_outer)
        def _():
            wait_bytes(psi.at[outer, at], psi_got.at[outer, q])

        @pl.when(q != atom)
        def _():
            wait_bytes(basis.at[1, q], chip_sent.at[q])

        for way in range(2):
            able = (
                jnp.logical_and(q <= atom, atom < n_atom - 1)
                if way == 0
                else jnp.logical_and(q >= atom, atom > 0)
            )

            @pl.when(able)
            def _():
                wait_bytes(basis.at[1, q], z_sent.at[0, way, q])

            @pl.when(jnp.logical_and(able, has_outer))
            def _():
                wait_bytes(basis.at[1, q], z_sent.at[1, way, q])

    @pl.when(has_outer)
    def _():
        wait_bytes(names, name_sent.at[0])
        wait_bytes(piece, v_sent.at[0])
        wait_bytes(part_out.at[0], part_sent.at[0])
        wait_bytes(psi.at[1], psi_sent.at[0])

    wait_bytes(names, name_sent.at[1])
    wait_bytes(piece, v_sent.at[1])
    wait_bytes(part_out.at[1], part_sent.at[1])
    wait_bytes(psi.at[1], psi_sent.at[1])

    @pl.when(relays)
    def _():
        wait_bytes(relay_v, v_passed.at[1])
        for phase in range(2):
            wait_bytes(relay.at[phase], relay_sent.at[phase])

    wait_all(dens_buf, sent.at[0], n_atom - 1)
    for k, held in enumerate([info_buf] + [rows_buf.at[layer] for layer in range(layers)]):
        wait_all(held, sent.at[1 + k], half - 1)
        wait_all(held, pair_sent.at[1 + k], half)
    wait_all(near, sent.at[final], n_atom - 1)
    wait_all(near, sent.at[final + 2], n_atom)

    @pl.when(has_outer)
    def _():
        wait_all(near, sent.at[final + 1], n_atom)


def exchange_of(shape, own, piece, names, atoms, weights, scale, shift, mw, aw, head):
    n_grid, n_atom = shape
    n = n_grid * n_atom
    nb, points, depth = piece.shape
    count = nb * n_atom
    width, columns = own.shape[1:]
    layers, features, _ = mw.shape
    packed = RUN * (features // LANES)
    bf16, f32 = jnp.bfloat16, jnp.float32
    dma = pltpu.SemaphoreType.DMA
    grant = 2 * own.size + 14 * count * points * columns + 6 * count * depth * points
    grant += n * (packed * LANES * (2 * layers + 8) + 12 * RUN * LANES) + (6 << 20)
    given = 6 * count * points * (columns + depth)
    if grant + given > 48 << 20:
        grant = 60 << 20
    return pl.pallas_call(
        functools.partial(exchange_kernel, shape, layers),
        out_shape=(
            jax.ShapeDtypeStruct((nb, points), f32),
            jax.ShapeDtypeStruct((3 * n_atom, nb, points), f32),
            jax.ShapeDtypeStruct((3, count, points, columns), bf16),
            jax.ShapeDtypeStruct((3, count, depth, points), bf16),
            jax.ShapeDtypeStruct((3, *names.shape), names.dtype),
        ),
        in_specs=[HBM] * 10,
        out_specs=(VMEM,) * 5,
        scratch_shapes=[
            pltpu.VMEM(a.shape, a.dtype) for a in (atoms, weights, scale, shift, mw, aw, head)
        ]
        + [
            pltpu.VMEM((own.shape[0] + 2, width, columns), bf16),
            pltpu.VMEM((3, n_atom, nb, points, depth), bf16),
            pltpu.SMEM((3, *names.shape), names.dtype),
            pltpu.VMEM((count, points, columns), f32),
            pltpu.VMEM((2, count, points, columns), bf16),
            pltpu.VMEM((2, count, points, columns), bf16),
            pltpu.VMEM((2, n_atom, nb // 2, points, columns), bf16),
            pltpu.VMEM((n_atom, nb, points), f32),
            pltpu.VMEM((n_atom, nb, points), f32),
            pltpu.VMEM((1, LANES), f32),
            pltpu.VMEM((n, 1, LANES), f32),
            pltpu.VMEM((layers, packed, LANES), bf16),
            pltpu.VMEM((layers, n, packed, LANES), bf16),
            pltpu.VMEM((nb, points), f32),
            dma((10,)),
            dma((1,)),
            dma((2,)),
            dma((3,)),
            dma((2,)),
            dma((3, n_atom)),
            dma((2, 2, n_atom)),
            dma((n_atom,)),
            dma((2,)),
            dma((2, n_atom)),
            dma((2,)),
            dma((3, n_atom)),
            dma((2, n_atom)),
            dma((2,)),
            dma((5 + layers,)),
            dma((5 + layers,)),
            pltpu.VMEM((max(nb // 2, 1), points, depth), bf16),
            dma((2,)),
            dma((2 + layers,)),
            dma((2 + layers,)),
            dma((nb,)),
            pltpu.SemaphoreType.REGULAR((2,)),
        ],
        compiler_params=pltpu.CompilerParams(
            collective_id=0, has_side_effects=True, vmem_limit_bytes=grant
        ),
        name="exchange_of",
    )(
        *(
            pltpu.with_memory_space_constraint(a, pltpu.HBM)
            for a in (own, piece, names, atoms, weights, scale, shift, mw, aw, head)
        )
    )


MANY = 6


def fock_kernel(names, basis_t, near, psi, pot, out, pot_out, filled, table, held, done):
    groups, count, depth, points = basis_t.shape
    owned, width, columns = out.shape
    picks = depth // width
    most = groups * count * picks
    tile = min(columns, TILE)
    first = lax.axis_index("grid") * owned
    last = pltpu.make_async_copy(pot, pot_out, done.at[owned])
    last.start()

    @pl.loop(0, owned + 2)
    def _(r):
        filled[r] = 0

    for k in range(groups):

        @pl.loop(0, count)
        def _(b):
            for j in range(picks):
                row = jnp.minimum(jnp.maximum(names[k, j, b] - first + 1, 0), owned + 1)
                n = filled[row]
                table[row * most + n] = (k * count + b) * picks + j
                filled[row] = n + 1

    @pl.loop(0, owned)
    def _(r):
        n = filled[r + 1]

        @pl.when(n == 0)
        def _():
            held[r] = jnp.zeros((width, columns), jnp.float32)

        def multiply(begin, many, first_time):
            parts, values = [], []
            for i in range(many):
                entry = table[(r + 1) * most + begin + i]
                s, j = entry // picks, lax.rem(entry, picks)
                k, b = s // count, lax.rem(s, count)
                part = basis_t[k, b, pl.ds(pl.multiple_of(j * width, width), width), :]
                parts.append(
                    (part.astype(jnp.float32) * near[pl.ds(s, 1), :]).astype(jnp.bfloat16)
                )
                values.append((k, b))
            left = jnp.concatenate(parts, axis=1)
            for c in range(columns // tile):
                at = pl.ds(c * tile, tile)
                right = jnp.concatenate([psi[k, b, :, at] for k, b in values], axis=0)
                value = jnp.dot(left, right, preferred_element_type=jnp.float32)
                if first_time:
                    held[r, :, at] = value
                else:
                    held[r, :, at] += value

        for many in range(1, MANY + 1):

            @pl.when(n == many if many < MANY else n >= many)
            def _():
                multiply(0, many, True)

        @pl.loop(MANY, jnp.maximum(n, MANY))
        def _(m):
            multiply(m, 1, False)

        pltpu.make_async_copy(held.at[r], out.at[r], done.at[r]).start()

    for r in range(owned):
        pltpu.make_async_copy(held.at[r], out.at[r], done.at[r]).wait()
    last.wait()


def fock_of(names, basis_t, near, psi, pot, owned):
    groups, count, depth, points = basis_t.shape
    columns = psi.shape[3]
    width = depth // names.shape[1]
    most = groups * depth // width * count
    return pl.pallas_call(
        fock_kernel,
        out_shape=(
            jax.ShapeDtypeStruct((owned, width, columns), jnp.float32),
            jax.ShapeDtypeStruct(pot.shape, pot.dtype),
        ),
        in_specs=[pl.BlockSpec(memory_space=pltpu.SMEM), VMEM, VMEM, VMEM, VMEM],
        out_specs=(HBM, HBM),
        scratch_shapes=[
            pltpu.SMEM((owned + 2,), jnp.int32),
            pltpu.SMEM(((owned + 2) * most,), jnp.int32),
            pltpu.VMEM((owned, width, columns), jnp.float32),
            pltpu.SemaphoreType.DMA((owned + 1,)),
        ],
        compiler_params=pltpu.CompilerParams(
            vmem_limit_bytes=4 * owned * width * columns + (8 << 20)
        ),
        name="fock_of",
    )(names, basis_t, near, psi, pot)


def local(
    basis_values,
    block_lists,
    orbitals,
    point_weights,
    point_atoms,
    embed_scale,
    embed_shift,
    message_weight,
    atom_weight,
    head_weight,
):
    n_grid, n_atom = lax.axis_size("grid"), lax.axis_size("atom")
    own_rows = orbitals.shape[0]
    batches, points, depth = basis_values.shape
    picks = block_lists.shape[1]
    owned = own_rows // (depth // picks)
    potential, near, psi, basis_t, names = exchange_of(
        (n_grid, n_atom),
        orbitals.reshape(owned, own_rows // owned, -1),
        basis_values,
        block_lists.T,
        point_atoms.reshape(batches, points),
        point_weights.reshape(batches, points),
        embed_scale[None, :],
        embed_shift[None, :],
        message_weight,
        atom_weight,
        head_weight[None, :],
    )
    fock, potential = fock_of(names, basis_t, near.reshape(-1, points), psi, potential, owned)
    return (fock.reshape(own_rows, -1), potential.reshape(-1))


def solution(mesh):
    return jax.shard_map(
        local,
        mesh=mesh,
        in_specs=(
            P(("grid", "atom"), None, None),
            P("grid", None),
            P("grid", "atom"),
            P(("grid", "atom")),
            P(("grid", "atom")),
            P(),
            P(),
            P(),
            P(),
            P(),
        ),
        out_specs=(P("grid", "atom"), P(("grid", "atom"))),
        check_vma=False,
    )
```

```python
import functools
import jax
import jax.numpy as jnp
from jax import lax
from jax.experimental import pallas as pl
from jax.experimental.pallas import tpu as pltpu
from jax.sharding import PartitionSpec as P

ATOM_DEV = 32
RUN = max(ATOM_DEV // 4, 1)
LANES = 128
VMEM = pl.BlockSpec(memory_space=pltpu.VMEM)
HBM = pl.BlockSpec(memory_space=pltpu.HBM)
MESH = pl.DeviceIdType.MESH
TILE = 256
PARTS = (2, 2, 2, 2)


def wait_bytes(ref, sem):
    pltpu.make_async_copy(ref, ref, sem).wait()


def meet_all(shape):
    n_grid, n_atom = shape
    n = n_grid * n_atom
    me = lax.axis_index("grid") * n_atom + lax.axis_index("atom")
    barrier = pltpu.get_barrier_semaphore()

    @pl.loop(1, n)
    def _(d):
        t = lax.rem(me + d, n)
        pl.semaphore_signal(
            barrier, inc=1, device_id=(t // n_atom, lax.rem(t, n_atom)), device_id_type=MESH
        )

    pl.semaphore_wait(barrier, n - 1)


def to_columns(rows):
    parts = [
        jnp.transpose(jnp.broadcast_to(rows[i : i + 1, :], (LANES, LANES)))
        for i in range(rows.shape[0])
    ]
    return jnp.concatenate(parts, axis=0)


def to_rows(columns):
    parts = []
    for i in range(columns.shape[0] // LANES):
        piece = jnp.broadcast_to(columns[i * LANES : (i + 1) * LANES, :], (LANES, LANES))
        parts.append(jnp.transpose(piece)[0:1, :])
    return jnp.concatenate(parts, axis=0)


def wrapped(values, total):
    values = jnp.where(values < 0.0, values + total, values)
    return jnp.where(values >= total, values - total, values)


def exchange_kernel(
    shape, layers, own, piece, names, *rest,
):
    given, rest = rest[:7], rest[7:]
    pot, near, psi, basis_t, all_names = rest[:5]
    atoms, weights, scale, shift, mw, aw, head = rest[5:12]
    (
        rows, basis, lists, acc, part_out, part_in, relay, dens, dens_buf,
        info, info_buf, rows_out, rows_buf, scaled_out,
        load, list_sem, name_sent, name_got, v_sent, v_got, z_sent, chip_sent,
        part_sent, part_got, psi_sent, psi_got, passed, relay_sent, sent, got,
        relay_v, v_passed, pair_sent, pair_got, v_first, word,
    ) = rest[12:]
    n_grid, n_atom = shape
    n = n_grid * n_atom
    grid, atom = lax.axis_index("grid"), lax.axis_index("atom")
    last, middle = n_grid - 1, n_grid // 2
    side = lax.rem(grid, 2)
    outer, inner = 2 * side, 2 - 2 * side
    og, ig = grid - 1 + 2 * side, grid + 1 - 2 * side
    has_outer = jnp.logical_and(og >= 0, og < n_grid)
    at_split = jnp.logical_or(grid == middle - 1, grid == middle)
    whole = jnp.logical_and(has_outer, jnp.logical_not(at_split))
    relays = jnp.logical_or(grid == 0, grid == last)
    relay_to = jnp.where(grid == middle, 0, last)
    forward_to = jnp.where(grid == 0, middle - 1, middle)

    nb, points, depth = piece.shape
    owned, width, columns = own.shape
    picks = depth // width
    tile = min(columns, TILE)
    relayed = nb // 2
    direct = nb - relayed

    def remote(source, target, send_sem, recv_sem, to):
        pltpu.make_async_remote_copy(
            src_ref=source,
            dst_ref=target,
            send_sem=send_sem,
            recv_sem=recv_sem,
            device_id=to,
            device_id_type=MESH,
        ).start()

    half = n // 2
    place_here = (grid // 2) * n_atom + atom
    slot_here = side * half + place_here

    def to_chips(source, held, k):
        @pl.loop(1, half)
        def _(d):
            t = lax.rem(place_here + d, half)
            remote(
                source, held.at[slot_here], sent.at[k], got.at[k],
                ((t // n_atom) * 2 + side, lax.rem(t, n_atom)),
            )

    def hand_over(held, k):
        wait_bytes(held.at[pl.ds(0, half - 1)], got.at[k])
        slab = held.at[pl.ds(side * half, half)]
        remote(slab, slab, pair_sent.at[k], pair_got.at[k], (ig, atom))
        wait_bytes(held.at[pl.ds(0, half)], pair_got.at[k])

    def wait_all(held, sem, count):
        wait_bytes(held.at[pl.ds(0, count)], sem)

    def visit(t):
        reach = jnp.minimum(atom, n_atom - 1 - atom)
        close = jnp.where(lax.rem(t, 2) == 1, atom - (t + 1) // 2, atom + t // 2)
        far = jnp.where(reach == atom, t, n_atom - 1 - t)
        return jnp.where(t <= 2 * reach, close, far)

    held_here = (
        rows.at[pl.ds(1, owned)], basis.at[1, atom], all_names.at[1],
        atoms, weights, scale, shift, mw, aw, head,
    )
    loads = [
        pltpu.make_async_copy(source, target, load.at[i])
        for i, (source, target) in enumerate(zip((own, piece, names, *given), held_here))
    ]
    for copy in loads:
        copy.start()
    early = n_atom <= 4

    def greet_near():
        barrier = pltpu.get_barrier_semaphore()

        def greet(able, g, a):
            @pl.when(able)
            def _():
                pl.semaphore_signal(barrier, inc=1, device_id=(g, a), device_id_type=MESH)

        greet(grid >= 0, ig, atom)
        greet(has_outer, og, atom)
        greet(atom > 0, grid, atom - 1)
        greet(atom < n_atom - 1, grid, atom + 1)
        for g in (0, last):
            greet(at_split, g, atom)
        for g in (middle - 1, middle):
            greet(relays, g, atom)
        met = 1 + has_outer.astype(jnp.int32) + (atom > 0).astype(jnp.int32)
        met = met + (atom < n_atom - 1).astype(jnp.int32)
        met = met + 2 * jnp.logical_or(at_split, relays).astype(jnp.int32)
        pl.semaphore_wait(barrier, met)

    def pass_word(t):
        for way, (step, when) in enumerate(((1, grid), (-1, last - grid))):
            behind = grid > 0 if way == 0 else grid < last
            ahead = grid < last if way == 0 else grid > 0
            now = t == when * n_atom // n_grid

            @pl.when(jnp.logical_and(now, behind))
            def _():
                pl.semaphore_wait(word.at[way], 1)

            @pl.when(jnp.logical_and(now, ahead))
            def _():
                pl.semaphore_signal(
                    word.at[way], inc=1, device_id=(grid + step, atom), device_id_type=MESH
                )

    if early:
        greet_near()
    else:
        meet_all(shape)

    @pl.when(has_outer)
    def _():
        remote(names, all_names.at[inner], name_sent.at[0], name_got.at[inner], (og, atom))

    for i in range(nb):
        target = basis.at[inner, atom, i]

        @pl.when(has_outer if i < direct else whole)
        def _():
            remote(piece.at[i], target, v_sent.at[0], v_first.at[i], (og, atom))

        if i >= direct:

            @pl.when(at_split)
            def _():
                remote(
                    piece.at[i], relay_v.at[i - direct], v_sent.at[0], v_passed.at[0],
                    (relay_to, atom),
                )

    remote(names, all_names.at[outer], name_sent.at[1], name_got.at[outer], (ig, atom))
    remote(piece, basis.at[outer, atom], v_sent.at[1], v_got.at[outer, atom], (ig, atom))

    @pl.when(atom < n_atom - 1)
    def _():
        remote(
            piece, basis.at[1, atom], z_sent.at[0, 0, atom], v_got.at[1, atom], (grid, atom + 1)
        )

    @pl.when(atom > 0)
    def _():
        remote(
            piece, basis.at[1, atom], z_sent.at[0, 1, atom], v_got.at[1, atom], (grid, atom - 1)
        )

    for copy in loads[1:5]:
        copy.wait()
    total = float(ATOM_DEV * n_atom)
    named = atoms[...].astype(jnp.float32)
    lead = named[0:1, 0:1]
    shifted = wrapped(named - lead + total / 2, total) - total / 2
    least = jnp.min(jnp.min(shifted, axis=1, keepdims=True), axis=0, keepdims=True)
    start = wrapped(lead + least, total)
    place = shifted - least
    lane = lax.broadcasted_iota(jnp.int32, (1, LANES), 1)
    mine = jnp.where(lane < RUN, wrapped(start + lane.astype(jnp.float32), total), -1.0)
    run = lax.broadcasted_iota(jnp.int32, (RUN, LANES), 0).astype(jnp.float32)
    mass = jnp.zeros((RUN, 1), jnp.float32)
    for i in range(nb):
        here = jnp.where(place[i : i + 1, :] == run, weights[i : i + 1, :], 0.0)
        mass = mass + jnp.sum(here, axis=1, keepdims=True)
    own_lane = lax.broadcasted_iota(jnp.int32, (RUN, LANES), 1).astype(jnp.float32)
    masses = jnp.sum(jnp.where(own_lane == run + LANES // 2, mass, 0.0), axis=0, keepdims=True)
    info[...] = jnp.where(lane < LANES // 2, mine, masses)
    info_buf[slot_here] = info[...]

    if relayed:

        @pl.when(relays)
        def _():
            wait_bytes(relay_v, v_passed.at[0])
            for i in range(direct, nb):
                remote(
                    relay_v.at[i - direct], basis.at[inner, atom, i], v_passed.at[1],
                    v_first.at[i], (forward_to, atom),
                )

    for edge in (0, owned + 1):
        rows[edge] = jnp.zeros((width, columns), rows.dtype)

    @pl.when(jnp.logical_not(has_outer))
    def _():
        all_names[outer] = jnp.full(names.shape, -1, names.dtype)
        part_in[0] = jnp.zeros(part_in.shape[1:], part_in.dtype)

    @pl.when(has_outer)
    def _():
        wait_bytes(names, name_got.at[outer])

    wait_bytes(names, name_got.at[inner])
    copy = pltpu.make_async_copy(all_names, lists, list_sem.at[0])
    copy.start()
    copy.wait()
    loads[0].wait()
    first = grid * owned

    def product(slot, q, i, keep):
        chosen = []
        for j in range(picks):
            block = lists[slot, j, q * nb + i] - first + 1
            chosen.append(jnp.minimum(jnp.maximum(block, 0), owned + 1))
        values = basis[slot, q, i]
        for c in range(columns // tile):
            at = pl.ds(c * tile, tile)
            held = jnp.concatenate(
                [rows[k, :, at] for k in chosen], axis=0
            )
            keep(at, jnp.dot(values, held, preferred_element_type=jnp.float32))

    def outward(phase, q, i, source, target, sent_sem, got_sem, near_by=True, far=True):
        if near_by:

            @pl.when(whole if i >= direct else has_outer)
            def _():
                remote(source, target, sent_sem, got_sem, (og, atom))

        if far and i >= direct:

            @pl.when(at_split)
            def _():
                remote(
                    source, relay.at[phase, q, i - direct], sent_sem, passed.at[phase, q],
                    (relay_to, atom),
                )

    def forward(phase, r):
        q = visit(r)

        @pl.when(relays)
        def _():
            held = relay.at[phase, q]
            wait_bytes(held, passed.at[phase, q])
            at = pl.ds(q * nb + direct, relayed)
            if phase == 0:
                target, got_sem = part_in.at[0, at], part_got.at[0, q]
            else:
                target, got_sem = psi.at[inner, at], psi_got.at[inner, q]
            remote(held, target, relay_sent.at[phase], got_sem, (forward_to, atom))

    def finish(t):
        q = visit(t)
        wait_bytes(part_in.at[1, pl.ds(q * nb, nb)], part_got.at[1, q])

        @pl.when(has_outer)
        def _():
            wait_bytes(part_in.at[0, pl.ds(q * nb, nb)], part_got.at[0, q])

        for i in range(nb):
            b = q * nb + i
            sums = jnp.zeros((points, LANES), jnp.float32)
            for c in range(columns // LANES):
                at = pl.ds(c * LANES, LANES)
                value = (
                    acc[b, :, at]
                    + part_in[0, b, :, at].astype(jnp.float32)
                    + part_in[1, b, :, at].astype(jnp.float32)
                )
                rounded = value.astype(jnp.bfloat16)
                psi[1, b, :, at] = rounded
                sums = sums + jnp.square(rounded.astype(jnp.float32))
            dens[q, i : i + 1, :] = jnp.sum(jnp.transpose(sums), axis=0, keepdims=True)

        @pl.when(q != atom)
        def _():
            remote(dens.at[q], dens_buf.at[atom], sent.at[0], got.at[0], (grid, q))

        at = pl.ds(q * nb, nb)
        remote(psi.at[1, at], psi.at[outer, at], psi_sent.at[1], psi_got.at[outer, q], (ig, atom))
        for i in range(nb):
            psi_outward(t, i, near_by=False)

    def psi_outward(r, i, **which):
        q = visit(r)
        b = q * nb + i
        outward(
            1, q, i, psi.at[1, b], psi.at[inner, b], psi_sent.at[0], psi_got.at[inner, q],
            **which,
        )

    def psi_unit(r, i):
        psi_outward(r, i, far=False)
        if i == nb - 1:
            forward(1, r)

    reach = jnp.minimum(atom, n_atom - 1 - atom)

    def along(stream, slot, q):
        for way in range(2):
            able = (
                jnp.logical_and(q <= atom, atom < n_atom - 1)
                if way == 0
                else jnp.logical_and(q >= atom, atom > 0)
            )

            @pl.when(able)
            def _():
                remote(
                    basis.at[slot, q], basis.at[slot, q], z_sent.at[stream, way, q],
                    v_got.at[slot, q], (grid, atom + 1 - 2 * way),
                )

    def spread_outer(t):
        q = visit(t)

        @pl.when(has_outer)
        def _():
            wait_bytes(basis.at[outer, q], v_got.at[outer, q])
            along(1, outer, q)

    def send_first():
        for i in range(nb):
            mine_first = basis.at[outer, atom, i]
            wait_bytes(mine_first, v_first.at[i])
            for way in range(2):

                @pl.when(atom < n_atom - 1 if way == 0 else atom > 0)
                def _():
                    remote(
                        mine_first, mine_first, z_sent.at[1, way, atom], v_got.at[outer, atom],
                        (grid, atom + 1 - 2 * way),
                    )

            outer_part(atom, i)

    def spread_own(t):
        q = visit(t)
        wait_bytes(basis.at[1, q], v_got.at[1, q])
        along(0, 1, q)
        remote(
            basis.at[1, q], basis.at[outer, q], chip_sent.at[q], v_got.at[outer, q], (ig, atom)
        )

    def outer_part(q, i):
        b = q * nb + i

        def keep(at, value):
            part_out[0, b, :, at] = value.astype(jnp.bfloat16)

        product(outer, q, i, keep)
        outward(
            0, q, i, part_out.at[0, b], part_in.at[0, b], part_sent.at[0], part_got.at[0, q]
        )

    def product_outer(q):
        for i in range(nb):
            outer_part(q, i)

    def products_here(q):
        wait_bytes(basis.at[inner, q], v_got.at[inner, q])
        for i in range(nb):
            b = q * nb + i

            def keep(at, value):
                part_out[1, b, :, at] = value.astype(jnp.bfloat16)

            product(inner, q, i, keep)
            remote(
                part_out.at[1, b], part_in.at[1, b], part_sent.at[1], part_got.at[1, q],
                (ig, atom),
            )

        for i in range(nb):
            b = q * nb + i

            def keep(at, value):
                acc[b, :, at] = value

            product(1, q, i, keep)
            for slot in range(3):
                basis_t[slot, b] = jnp.transpose(basis[slot, q, i])

    @pl.when(has_outer)
    def _():
        send_first()

    @pl.loop(0, n_atom)
    def _(t):
        q = visit(t)
        paired = jnp.logical_and(lax.rem(t, 2) == 1, t < 2 * reach)
        fresh = jnp.logical_and(
            t > 0, jnp.logical_or(lax.rem(t, 2) == 1, t > 2 * reach)
        )

        @pl.when(fresh)
        def _():
            spread_outer(t)

        @pl.when(paired)
        def _():
            spread_outer(t + 1)

        @pl.when(jnp.logical_and(t > 0, has_outer))
        def _():
            product_outer(q)

        @pl.when(t > 0)
        def _():
            products_here(visit(t - 1))

        @pl.when(fresh)
        def _():
            spread_own(t)

        @pl.when(paired)
        def _():
            spread_own(t + 1)

        @pl.when(t >= 1)
        def _():
            forward(0, t - 1)

        if early:
            pass_word(t)

        @pl.when(t >= 2)
        def _():
            finish(t - 2)

    ends = [sum(PARTS[: s + 1]) for s in range(len(PARTS))]

    def send_psi(s):
        for u in range(n_atom * nb):
            if sum(u * ends[-1] >= end * n_atom * nb for end in ends) == s:
                psi_unit(u // nb, u % nb)

    send_psi(0)
    products_here(visit(n_atom - 1))
    finish(n_atom - 2)
    weight = to_columns(weights[...])[:, 0:1]
    spot = to_columns(place)
    hot = (spot == lax.broadcasted_iota(jnp.int32, spot.shape, 1).astype(jnp.float32)).astype(
        jnp.bfloat16
    )
    deep = lax.broadcasted_iota(jnp.int32, (LANES, LANES), 0).astype(jnp.float32)
    hot_t = jnp.concatenate([place[i : i + 1, :] == deep for i in range(nb)], axis=1).astype(
        jnp.bfloat16
    )
    for copy in loads[5:]:
        copy.wait()
    halves = scale.shape[1] // LANES
    forward(0, n_atom - 1)
    finish(n_atom - 1)
    dens_buf[atom] = dens[atom]

    wait_all(dens_buf, got.at[0], n_atom - 1)
    to_chips(info, info_buf, 1)
    density = to_columns(2.0 * jnp.sum(dens_buf[...], axis=0))
    safe = jnp.where(density > 0.0, density, 1.0)
    radius = jnp.where(density > 0.0, jnp.exp(jnp.log(safe) * (1.0 / 3.0)), 0.0)[:, 0:1]
    hidden = jax.nn.silu(radius * scale[...] + shift[...])
    for layer in range(layers):
        message = jax.nn.silu(
            jnp.dot(hidden.astype(jnp.bfloat16), mw[layer], preferred_element_type=jnp.float32)
        )
        weighted = (weight * message).astype(jnp.bfloat16)
        part = jnp.dot(hot_t, weighted, preferred_element_type=jnp.float32)
        rows_out[layer] = jnp.concatenate(
            [part[0:RUN, h * LANES : (h + 1) * LANES] for h in range(halves)], axis=0
        ).astype(jnp.bfloat16)
        to_chips(rows_out.at[layer], rows_buf.at[layer], 2 + layer)
        rows_buf[layer, slot_here] = rows_out[layer]
        send_psi(1 + layer)
        if layer == 0:
            hand_over(info_buf, 1)
            facts = jnp.broadcast_to(info_buf[...], (n, RUN, LANES)).reshape(n * RUN, LANES)
            row = lax.rem(lax.broadcasted_iota(jnp.int32, (n * RUN, LANES), 0), RUN)
            lanes = lax.broadcasted_iota(jnp.int32, (n * RUN, LANES), 1)
            named = jnp.sum(jnp.where(lanes == row, facts, 0.0), axis=1, keepdims=True)
            held_mass = jnp.where(lanes == row + LANES // 2, facts, 0.0)
            same = (named == mine).astype(jnp.float32)
            held_mass = jnp.sum(held_mass, axis=1, keepdims=True)
            mass = jnp.sum(same * held_mass, axis=0, keepdims=True)
            share = 1.0 / (1.0 + to_columns(mass)[:, 0:1])
            same = same.reshape(n, RUN, LANES)
            none = jnp.zeros_like(same)
            selects = []
            for h in range(halves):
                full = jnp.concatenate(
                    [same if k == h else none for k in range(halves)], axis=1
                ).reshape(n * RUN * halves, LANES)
                selects.append(jnp.transpose(full).astype(jnp.bfloat16))

        hand_over(rows_buf.at[layer], 2 + layer)
        held = rows_buf[layer].reshape(n * RUN * halves, LANES)
        summed = jnp.concatenate(
            [jnp.dot(pick, held, preferred_element_type=jnp.float32) for pick in selects], axis=1
        )
        update = jax.nn.silu(
            jnp.dot(
                (summed * share).astype(jnp.bfloat16), aw[layer],
                preferred_element_type=jnp.float32,
            )
        ).astype(jnp.bfloat16)
        picked = jnp.dot(hot, update, preferred_element_type=jnp.float32)
        hidden = hidden + message * picked
    score = jnp.sum(hidden * head[...], axis=1, keepdims=True)
    potential = radius * (1.0 + jnp.tanh(score))
    pot[...] = to_rows(potential)
    final = 2 + layers
    scaled_out[...] = to_rows(weight * potential)

    @pl.loop(1, n_atom)
    def _(d):
        remote(
            scaled_out, near.at[n_atom + atom], sent.at[final], got.at[final],
            (grid, lax.rem(atom + d, n_atom)),
        )

    @pl.when(has_outer)
    def _():
        @pl.loop(0, n_atom)
        def _(d):
            remote(
                scaled_out, near.at[inner * n_atom + atom], sent.at[final + 1],
                got.at[final + 1 + side], (og, d),
            )

    @pl.loop(0, n_atom)
    def _(d):
        remote(
            scaled_out, near.at[outer * n_atom + atom], sent.at[final + 2],
            got.at[final + 2 - side], (ig, d),
        )

    send_psi(layers + 1)
    near[n_atom + atom] = scaled_out[...]
    wait_all(near, got.at[final], n_atom - 1)

    @pl.when(has_outer)
    def _():
        wait_all(near, got.at[final + 2 - side], n_atom)

    wait_all(near, got.at[final + 1 + side], n_atom)

    all_names[...] = jnp.minimum(jnp.maximum(all_names[...] - first + 1, 0), owned + 1)

    @pl.loop(0, n_atom)
    def _(q):
        at = pl.ds(q * nb, nb)
        wait_bytes(psi.at[inner, at], psi_got.at[inner, q])

        @pl.when(has_outer)
        def _():
            wait_bytes(psi.at[outer, at], psi_got.at[outer, q])

        @pl.when(q != atom)
        def _():
            wait_bytes(basis.at[1, q], chip_sent.at[q])

        for way in range(2):
            able = (
                jnp.logical_and(q <= atom, atom < n_atom - 1)
                if way == 0
                else jnp.logical_and(q >= atom, atom > 0)
            )

            @pl.when(able)
            def _():
                wait_bytes(basis.at[1, q], z_sent.at[0, way, q])

            @pl.when(jnp.logical_and(able, has_outer))
            def _():
                wait_bytes(basis.at[1, q], z_sent.at[1, way, q])

    @pl.when(has_outer)
    def _():
        wait_bytes(names, name_sent.at[0])
        wait_bytes(piece, v_sent.at[0])
        wait_bytes(part_out.at[0], part_sent.at[0])
        wait_bytes(psi.at[1], psi_sent.at[0])

    wait_bytes(names, name_sent.at[1])
    wait_bytes(piece, v_sent.at[1])
    wait_bytes(part_out.at[1], part_sent.at[1])
    wait_bytes(psi.at[1], psi_sent.at[1])

    @pl.when(relays)
    def _():
        wait_bytes(relay_v, v_passed.at[1])
        for phase in range(2):
            wait_bytes(relay.at[phase], relay_sent.at[phase])

    wait_all(dens_buf, sent.at[0], n_atom - 1)
    for k, held in enumerate([info_buf] + [rows_buf.at[layer] for layer in range(layers)]):
        wait_all(held, sent.at[1 + k], half - 1)
        wait_all(held, pair_sent.at[1 + k], half)
    wait_all(near, sent.at[final], n_atom - 1)
    wait_all(near, sent.at[final + 2], n_atom)

    @pl.when(has_outer)
    def _():
        wait_all(near, sent.at[final + 1], n_atom)


def exchange_of(shape, own, piece, names, atoms, weights, scale, shift, mw, aw, head):
    n_grid, n_atom = shape
    n = n_grid * n_atom
    nb, points, depth = piece.shape
    count = nb * n_atom
    width, columns = own.shape[1:]
    layers, features, _ = mw.shape
    packed = RUN * (features // LANES)
    bf16, f32 = jnp.bfloat16, jnp.float32
    dma = pltpu.SemaphoreType.DMA
    grant = 2 * own.size + 14 * count * points * columns + 6 * count * depth * points
    grant += n * (packed * LANES * (2 * layers + 8) + 12 * RUN * LANES) + (6 << 20)
    given = 6 * count * points * (columns + depth)
    if grant + given > 48 << 20:
        grant = 60 << 20
    return pl.pallas_call(
        functools.partial(exchange_kernel, shape, layers),
        out_shape=(
            jax.ShapeDtypeStruct((nb, points), f32),
            jax.ShapeDtypeStruct((3 * n_atom, nb, points), f32),
            jax.ShapeDtypeStruct((3, count, points, columns), bf16),
            jax.ShapeDtypeStruct((3, count, depth, points), bf16),
            jax.ShapeDtypeStruct((3, *names.shape), names.dtype),
        ),
        in_specs=[HBM] * 10,
        out_specs=(VMEM,) * 5,
        scratch_shapes=[
            pltpu.VMEM(a.shape, a.dtype) for a in (atoms, weights, scale, shift, mw, aw, head)
        ]
        + [
            pltpu.VMEM((own.shape[0] + 2, width, columns), bf16),
            pltpu.VMEM((3, n_atom, nb, points, depth), bf16),
            pltpu.SMEM((3, *names.shape), names.dtype),
            pltpu.VMEM((count, points, columns), f32),
            pltpu.VMEM((2, count, points, columns), bf16),
            pltpu.VMEM((2, count, points, columns), bf16),
            pltpu.VMEM((2, n_atom, nb // 2, points, columns), bf16),
            pltpu.VMEM((n_atom, nb, points), f32),
            pltpu.VMEM((n_atom, nb, points), f32),
            pltpu.VMEM((1, LANES), f32),
            pltpu.VMEM((n, 1, LANES), f32),
            pltpu.VMEM((layers, packed, LANES), bf16),
            pltpu.VMEM((layers, n, packed, LANES), bf16),
            pltpu.VMEM((nb, points), f32),
            dma((10,)),
            dma((1,)),
            dma((2,)),
            dma((3,)),
            dma((2,)),
            dma((3, n_atom)),
            dma((2, 2, n_atom)),
            dma((n_atom,)),
            dma((2,)),
            dma((2, n_atom)),
            dma((2,)),
            dma((3, n_atom)),
            dma((2, n_atom)),
            dma((2,)),
            dma((5 + layers,)),
            dma((5 + layers,)),
            pltpu.VMEM((max(nb // 2, 1), points, depth), bf16),
            dma((2,)),
            dma((2 + layers,)),
            dma((2 + layers,)),
            dma((nb,)),
            pltpu.SemaphoreType.REGULAR((2,)),
        ],
        compiler_params=pltpu.CompilerParams(
            collective_id=0, has_side_effects=True, vmem_limit_bytes=grant
        ),
        name="exchange_of",
    )(
        *(
            pltpu.with_memory_space_constraint(a, pltpu.HBM)
            for a in (own, piece, names, atoms, weights, scale, shift, mw, aw, head)
        )
    )


MANY = 6


def fock_kernel(names, basis_t, near, psi, pot, out, pot_out, filled, table, held, done):
    groups, count, depth, points = basis_t.shape
    owned, width, columns = out.shape
    picks = depth // width
    most = groups * count * picks
    tile = min(columns, TILE)
    last = pltpu.make_async_copy(pot, pot_out, done.at[owned])
    last.start()

    @pl.loop(0, owned + 2)
    def _(r):
        filled[r] = 0

    for k in range(groups):

        @pl.loop(0, count)
        def _(b):
            for j in range(picks):
                row = names[k, j, b]
                n = filled[row]
                table[row * most + n] = (k * count + b) * picks + j
                filled[row] = n + 1

    @pl.loop(0, owned)
    def _(r):
        n = filled[r + 1]

        @pl.when(n == 0)
        def _():
            held[r] = jnp.zeros((width, columns), jnp.float32)

        def multiply(begin, many, first_time):
            parts, values = [], []
            for i in range(many):
                entry = table[(r + 1) * most + begin + i]
                s, j = entry // picks, lax.rem(entry, picks)
                k, b = s // count, lax.rem(s, count)
                part = basis_t[k, b, pl.ds(pl.multiple_of(j * width, width), width), :]
                parts.append(
                    (part.astype(jnp.float32) * near[pl.ds(s, 1), :]).astype(jnp.bfloat16)
                )
                values.append((k, b))
            left = jnp.concatenate(parts, axis=1)
            for c in range(columns // tile):
                at = pl.ds(c * tile, tile)
                right = jnp.concatenate([psi[k, b, :, at] for k, b in values], axis=0)
                value = jnp.dot(left, right, preferred_element_type=jnp.float32)
                if first_time:
                    held[r, :, at] = value
                else:
                    held[r, :, at] += value

        for many in range(1, MANY + 1):

            @pl.when(n == many if many < MANY else n >= many)
            def _():
                multiply(0, many, True)

        @pl.loop(MANY, jnp.maximum(n, MANY))
        def _(m):
            multiply(m, 1, False)

        pltpu.make_async_copy(held.at[r], out.at[r], done.at[r]).start()

    for r in range(owned):
        pltpu.make_async_copy(held.at[r], out.at[r], done.at[r]).wait()
    last.wait()


def fock_of(names, basis_t, near, psi, pot, owned):
    groups, count, depth, points = basis_t.shape
    columns = psi.shape[3]
    width = depth // names.shape[1]
    most = groups * depth // width * count
    return pl.pallas_call(
        fock_kernel,
        out_shape=(
            jax.ShapeDtypeStruct((owned, width, columns), jnp.float32),
            jax.ShapeDtypeStruct(pot.shape, pot.dtype),
        ),
        in_specs=[pl.BlockSpec(memory_space=pltpu.SMEM), VMEM, VMEM, VMEM, VMEM],
        out_specs=(HBM, HBM),
        scratch_shapes=[
            pltpu.SMEM((owned + 2,), jnp.int32),
            pltpu.SMEM(((owned + 2) * most,), jnp.int32),
            pltpu.VMEM((owned, width, columns), jnp.float32),
            pltpu.SemaphoreType.DMA((owned + 1,)),
        ],
        compiler_params=pltpu.CompilerParams(
            vmem_limit_bytes=4 * owned * width * columns + (8 << 20)
        ),
        name="fock_of",
    )(names, basis_t, near, psi, pot)


def local(
    basis_values,
    block_lists,
    orbitals,
    point_weights,
    point_atoms,
    embed_scale,
    embed_shift,
    message_weight,
    atom_weight,
    head_weight,
):
    n_grid, n_atom = lax.axis_size("grid"), lax.axis_size("atom")
    own_rows = orbitals.shape[0]
    batches, points, depth = basis_values.shape
    picks = block_lists.shape[1]
    owned = own_rows // (depth // picks)
    potential, near, psi, basis_t, names = exchange_of(
        (n_grid, n_atom),
        orbitals.reshape(owned, own_rows // owned, -1),
        basis_values,
        block_lists.T,
        point_atoms.reshape(batches, points),
        point_weights.reshape(batches, points),
        embed_scale[None, :],
        embed_shift[None, :],
        message_weight,
        atom_weight,
        head_weight[None, :],
    )
    fock, potential = fock_of(names, basis_t, near.reshape(-1, points), psi, potential, owned)
    return (fock.reshape(own_rows, -1), potential.reshape(-1))


def solution(mesh):
    return jax.shard_map(
        local,
        mesh=mesh,
        in_specs=(
            P(("grid", "atom"), None, None),
            P("grid", None),
            P("grid", "atom"),
            P(("grid", "atom")),
            P(("grid", "atom")),
            P(),
            P(),
            P(),
            P(),
            P(),
        ),
        out_specs=(P("grid", "atom"), P(("grid", "atom"))),
        check_vma=False,
    )
```
